32 devices in a mesh: dp: 1 (over z), tp: 32 (over y, x, core).
Axes of the slice: x: 4, y: 4, z: 1, core: 2. Of those that a mesh axis runs over, the one named last changes fastest.
The devices are a block of a 4x4x8 slice.
Arguments:
- x_tokens: bfloat16 [1, 4096, 2048], P('dp', 'tp')
- ln1_gain: float32 [2, 2048], replicated
- ln1_bias: float32 [2, 2048], replicated
- ln2_gain: float32 [2, 2048], replicated
- ln2_bias: float32 [2, 2048], replicated
- w_qkv: bfloat16 [2, 2048, 3, 32, 64], P(None, None, None, 'tp')
- w_out: bfloat16 [2, 32, 64, 2048], P(None, 'tp')
- b_out: float32 [2, 2048], replicated
- w_up: bfloat16 [2, 2048, 8192], P(None, None, 'tp')
- b_up: float32 [2, 8192], P(None, 'tp')
- w_down: bfloat16 [2, 8192, 2048], P(None, 'tp')
- b_down: float32 [2, 2048], replicated
Outputs:
- output: bfloat16 [1, 4096, 2048], P('dp', 'tp')
All inputs are finite; a program needn't handle non-finite values.
Results may differ from the reference program's by a relative error of at most 0.011077.
Values are sent between devices in bfloat16 or wider.
A program may use at most 768 MiB of HBM per device.

```python
import math
import jax
import jax.numpy as jnp
from jax import lax

BATCH = 1
SEQ_LEN = 4096
D_MODEL = 2048
HEADS = 32
HEAD_DIM = 64
D_FF = 8192
LAYERS = 2


def setup_inputs(seed: int = 0, part: int = 0) -> dict:
    base_key = jax.random.key(seed)
    part_key = jax.random.fold_in(base_key, part)
    row_key, tok_key = jax.random.split(part_key)
    keys = jax.random.split(base_key, 11)
    row_scale = 0.5 + jax.random.uniform(row_key, (BATCH, SEQ_LEN, 1), jnp.float32)
    tokens = jax.random.normal(tok_key, (BATCH, SEQ_LEN, D_MODEL), jnp.float32) * row_scale
    qk_gain = (math.log(SEQ_LEN) / 2.0) ** 0.25
    attn_level = math.sqrt((1.0 + 0.5 * math.log(SEQ_LEN)) / math.sqrt(SEQ_LEN))
    out_gain = 0.5 / attn_level
    proj_gain = jnp.array([qk_gain, qk_gain, 1.0], jnp.float32).reshape(1, 1, 3, 1, 1)
    vec_shape = (LAYERS, D_MODEL)
    w_qkv = jax.random.normal(keys[4], (LAYERS, D_MODEL, 3, HEADS, HEAD_DIM), jnp.float32) * proj_gain * D_MODEL ** -0.5
    w_out = jax.random.normal(keys[5], (LAYERS, HEADS, HEAD_DIM, D_MODEL), jnp.float32) * (out_gain * D_MODEL ** -0.5)
    w_up = jax.random.normal(keys[7], (LAYERS, D_MODEL, D_FF), jnp.float32) * D_MODEL ** -0.5
    w_down = jax.random.normal(keys[9], (LAYERS, D_FF, D_MODEL), jnp.float32) * (0.8 * D_FF ** -0.5)
    return {
        "x_tokens": tokens.astype(jnp.bfloat16),
        "ln1_gain": 1.0 + 0.2 * jax.random.normal(keys[0], vec_shape, jnp.float32),
        "ln1_bias": 0.2 * jax.random.normal(keys[1], vec_shape, jnp.float32),
        "ln2_gain": 1.0 + 0.2 * jax.random.normal(keys[2], vec_shape, jnp.float32),
        "ln2_bias": 0.2 * jax.random.normal(keys[3], vec_shape, jnp.float32),
        "w_qkv": w_qkv.astype(jnp.bfloat16),
        "w_out": w_out.astype(jnp.bfloat16),
        "b_out": 0.2 * jax.random.normal(keys[6], vec_shape, jnp.float32),
        "w_up": w_up.astype(jnp.bfloat16),
        "b_up": 0.3 * jax.random.normal(keys[8], (LAYERS, D_FF), jnp.float32),
        "w_down": w_down.astype(jnp.bfloat16),
        "b_down": 0.2 * jax.random.normal(keys[10], vec_shape, jnp.float32),
    }


def layer_norm(resid, gain, shift):
    row_mean = jnp.mean(resid, axis=-1, keepdims=True)
    centered = resid - row_mean
    variance = jnp.mean(centered * centered, axis=-1, keepdims=True)
    return (centered * lax.rsqrt(variance + 1e-5) * gain + shift).astype(jnp.bfloat16)


def attention_head(head_parts):
    queries, keys_all, values_all = head_parts
    scores = jnp.einsum("bqe,bke->bqk", queries.astype(jnp.float32), keys_all.astype(jnp.float32)) / math.sqrt(HEAD_DIM)
    positions = jnp.arange(SEQ_LEN)
    causal = positions[:, None] >= positions[None, :]
    scores = jnp.where(causal, scores, -1e30)
    attn_probs = jax.nn.softmax(scores, axis=-1).astype(jnp.bfloat16)
    return jnp.einsum("bqk,bke->bqe", attn_probs.astype(jnp.float32), values_all.astype(jnp.float32)).astype(jnp.bfloat16)


def layer_step(resid, params):
    ln1_gain, ln1_bias, ln2_gain, ln2_bias, w_qkv, w_out, b_out, w_up, b_up, w_down, b_down = params
    normed = layer_norm(resid, ln1_gain, ln1_bias)
    qkv_proj = jnp.dot(normed.reshape(BATCH * SEQ_LEN, D_MODEL), w_qkv.reshape(D_MODEL, 3 * HEADS * HEAD_DIM), preferred_element_type=jnp.float32).astype(jnp.bfloat16)
    qkv_proj = qkv_proj.reshape(BATCH, SEQ_LEN, 3, HEADS, HEAD_DIM)
    heads_first = jnp.transpose(qkv_proj, (2, 3, 0, 1, 4))
    attn_heads = lax.map(attention_head, (heads_first[0], heads_first[1], heads_first[2]))
    attn_out = jnp.einsum("hbse,hed->bsd", attn_heads.astype(jnp.float32), w_out.astype(jnp.float32))
    resid = resid + (attn_out + b_out)
    normed_mlp = layer_norm(resid, ln2_gain, ln2_bias)
    pre_act = jnp.dot(normed_mlp.reshape(BATCH * SEQ_LEN, D_MODEL), w_up, preferred_element_type=jnp.float32) + b_up
    hidden = jax.nn.gelu(pre_act, approximate=True).astype(jnp.bfloat16)
    mlp_out = jnp.dot(hidden, w_down, preferred_element_type=jnp.float32).reshape(BATCH, SEQ_LEN, D_MODEL)
    resid = resid + (mlp_out + b_down)
    return resid, None


def reference(x_tokens, ln1_gain, ln1_bias, ln2_gain, ln2_bias, w_qkv, w_out, b_out, w_up, b_up, w_down, b_down):
    params = (ln1_gain, ln1_bias, ln2_gain, ln2_bias, w_qkv, w_out, b_out, w_up, b_up, w_down, b_down)
    resid, _ = lax.scan(layer_step, x_tokens.astype(jnp.float32), params)
    return resid.astype(jnp.bfloat16)
```

```python
import functools
import math
import jax
import jax.numpy as jnp
from jax import lax
from jax.experimental import pallas as pl
from jax.experimental.pallas import tpu as pltpu
from jax.sharding import PartitionSpec as P

F32 = jnp.float32
BF16 = jnp.bfloat16
CORES = 2
NT = (((1,), (1,)), ((), ()))


def layer_norm(resid, gain, shift):
    row_mean = jnp.mean(resid, axis=-1, keepdims=True)
    centered = resid - row_mean
    variance = jnp.mean(centered * centered, axis=-1, keepdims=True)
    return (centered * lax.rsqrt(variance + 1e-5) * gain + shift).astype(BF16)


def attention_kernel(scale, block, q_ref, k_ref, v_ref, o_ref):
    seq, dim = q_ref.shape
    rows = lax.broadcasted_iota(jnp.int32, (block, block), 0)
    cols = lax.broadcasted_iota(jnp.int32, (block, block), 1)

    def q_step(i, _):
        q = q_ref[pl.ds(pl.multiple_of(i * block, block), block), :]

        def scores(j):
            k = k_ref[pl.ds(pl.multiple_of(j * block, block), block), :]
            return lax.dot_general(q, k, NT, preferred_element_type=F32) * scale

        def update(s, j, carry):
            m, l, acc = carry
            m_new = jnp.maximum(m, jnp.max(s, axis=-1, keepdims=True))
            p = jnp.exp(s - m_new)
            alpha = jnp.exp(m - m_new)
            v = v_ref[pl.ds(pl.multiple_of(j * block, block), block), :]
            acc = acc * alpha + jnp.dot(p.astype(BF16), v, preferred_element_type=F32)
            return m_new, l * alpha + jnp.sum(p, axis=-1, keepdims=True), acc

        def k_step(j, carry):
            return update(scores(j), j, carry)

        init = (jnp.full((block, 1), -1e30, F32), jnp.zeros((block, 1), F32), jnp.zeros((block, dim), F32))
        carry = lax.fori_loop(0, i, k_step, init)
        _, l, acc = update(jnp.where(rows >= cols, scores(i), -1e30), i, carry)
        o_ref[pl.ds(pl.multiple_of(i * block, block), block), :] = (acc / l).astype(BF16)
        return 0

    lax.fori_loop(0, seq // block, q_step, 0)


def attention(q, k, v, scale):
    seq, dim = q.shape
    flops = 2 * seq * seq * dim
    return pl.pallas_call(
        functools.partial(attention_kernel, scale, 512),
        out_shape=jax.ShapeDtypeStruct((seq, dim), BF16),
        in_specs=[pl.BlockSpec(memory_space=pltpu.VMEM)] * 3,
        out_specs=pl.BlockSpec(memory_space=pltpu.VMEM),
        cost_estimate=pl.CostEstimate(flops=flops * 8, bytes_accessed=8 * seq * dim, transcendentals=seq * seq // 2),
        name="attention",
    )(q, k, v)


def solution(mesh):
    tp = mesh.shape["tp"]
    side = math.isqrt(tp // CORES)
    row_groups = [[(y * side + x) * CORES + c for x in range(side)] for y in range(side) for c in range(CORES)]
    col_groups = [[(y * side + x) * CORES + c for y in range(side) for c in range(CORES)] for x in range(side)]
    col = side * CORES

    def local_forward(x_local, ln1_gain, ln1_bias, ln2_gain, ln2_bias, w_qkv, w_out, b_out, w_up, b_up, w_down, b_down):
        _, share, width = x_local.shape
        layers, _, three, _, dim = w_qkv.shape
        scale = 1.0 / math.sqrt(dim)
        hidden = w_up.shape[2]
        wq_t = jnp.transpose(w_qkv, (0, 2, 3, 4, 1)).reshape(layers, three * dim, width)
        bup_all = lax.all_gather(b_up, "tp", axis=0, axis_index_groups=col_groups)
        gathered = []
        for layer in range(layers):
            gathered.append((
                lax.all_gather(wq_t[layer], "tp", axis=0, axis_index_groups=col_groups),
                lax.all_gather(w_out[layer].reshape(dim, width), "tp", axis=0),
                lax.all_gather(w_up[layer], "tp", axis=0, axis_index_groups=col_groups),
                lax.all_gather(w_down[layer], "tp", axis=0, axis_index_groups=col_groups),
            ))
        resid = x_local[0].astype(F32)
        for layer in range(layers):
            gq, go, gu, gd = gathered[layer]
            normed = layer_norm(resid, ln1_gain[layer], ln1_bias[layer])
            rows = lax.all_gather(normed, "tp", axis=0, axis_index_groups=row_groups, tiled=True)
            qkv = jnp.einsum("sd,ged->gse", rows, gq, preferred_element_type=F32).astype(BF16)
            qkv = lax.all_to_all(qkv, "tp", 0, 0, axis_index_groups=col_groups, tiled=True)
            qkv = qkv.reshape(side, CORES, side, share, three * dim).transpose(0, 2, 1, 3, 4).reshape(tp * share, three, dim)
            o = attention(qkv[:, 0], qkv[:, 1], qkv[:, 2], scale)
            o = lax.all_to_all(o.reshape(tp, share, dim), "tp", 0, 0, tiled=True)
            o = o.transpose(1, 0, 2).reshape(share, tp * dim)
            attn = jnp.dot(o, go.reshape(tp * dim, width), preferred_element_type=F32)
            resid = resid + (attn + b_out[layer])
            normed = layer_norm(resid, ln2_gain[layer], ln2_bias[layer])
            rows = lax.all_gather(normed, "tp", axis=0, axis_index_groups=row_groups, tiled=True)
            pre = jnp.einsum("sd,gdf->sgf", rows, gu, preferred_element_type=F32) + bup_all[:, layer]
            act = jax.nn.gelu(pre, approximate=True).astype(BF16)
            z = jnp.einsum("sgf,gfd->sd", act, gd, preferred_element_type=F32).astype(BF16)
            z = lax.all_to_all(z.reshape(side, share, width), "tp", 0, 0, axis_index_groups=row_groups, tiled=True)
            resid = resid + (jnp.sum(z.astype(F32), axis=0) + b_down[layer])
        return resid.astype(BF16)[None]

    rows_spec = P("dp", "tp", None)
    in_specs = (rows_spec, P(), P(), P(), P(), P(None, None, None, "tp", None), P(None, "tp", None, None), P(), P(None, None, "tp"), P(None, "tp"), P(None, "tp", None), P())
    return jax.shard_map(local_forward, mesh=mesh, in_specs=in_specs, out_specs=rows_spec, check_vma=False)
```

```python
import functools
import math
import jax
import jax.numpy as jnp
from jax import lax
from jax.experimental import pallas as pl
from jax.experimental.pallas import tpu as pltpu
from jax.sharding import PartitionSpec as P

F32 = jnp.float32
BF16 = jnp.bfloat16
CORES = 2
NN = (((1,), (0,)), ((), ()))
NT = (((1,), (1,)), ((), ()))
TN = (((0,), (0,)), ((), ()))
MESH = pl.DeviceIdType.MESH
VMEM = pl.BlockSpec(memory_space=pltpu.VMEM)
HBM = pl.BlockSpec(memory_space=pl.ANY)
DMA = pltpu.SemaphoreType.DMA


def place(side):
    me = lax.axis_index("tp")
    return me, me // (side * CORES), (me // CORES) % side, me % CORES


def index_of(side, y, x, c):
    return (y * side + x) * CORES + c


def dev(index):
    return {"tp": index}


def remote(src, dst, send_sem, recv_sem, index):
    return pltpu.make_async_remote_copy(src_ref=src, dst_ref=dst, send_sem=send_sem, recv_sem=recv_sem, device_id=dev(index), device_id_type=MESH)


def enter(indices):
    barrier = pltpu.get_barrier_semaphore()
    for index in indices:
        pl.semaphore_signal(barrier, inc=1, device_id=dev(index), device_id_type=MESH)
    pl.semaphore_wait(barrier, len(indices))


def norm(resid, gain, shift):
    row_mean = jnp.mean(resid, axis=-1, keepdims=True)
    centered = resid - row_mean
    variance = jnp.mean(centered * centered, axis=-1, keepdims=True)
    return (centered * lax.rsqrt(variance + 1e-5) * gain + shift).astype(BF16)


def ring_order(side):
    return sorted(range(1, side), key=lambda off: min(off, side - off))


def qkv_kernel(side, r_ref, gain_ref, shift_ref, w_hbm, out_ref, w_ref, hbuf, sbuf, w_sem, h_send, h_recv, q_send, q_recv):
    me, y, x, c = place(side)
    col = side * CORES
    mine = y * CORES + c
    offs = ring_order(side)

    def in_col(m):
        return index_of(side, m // CORES, x, m % CORES)

    load = pltpu.make_async_copy(w_hbm, w_ref, w_sem)
    load.start()
    row_peers = [index_of(side, y, (x + off) % side, c) for off in offs]
    enter(row_peers + [in_col((mine + d) % col) for d in range(1, col)])
    hbuf[x] = norm(r_ref[...].astype(F32), gain_ref[...], shift_ref[...])
    sends = [remote(hbuf.at[x], hbuf.at[x], h_send.at[n], h_recv.at[n], row_peers[n]) for n in range(len(offs))]
    for copy in sends:
        copy.start()
    load.wait()

    def slot_copy(k, d, xk):
        return remote(sbuf.at[k, d], out_ref.at[index_of(side, y, xk, c)], q_send.at[k, d], q_recv.at[k, d], in_col((mine + d) % col))

    for k in range(side):
        xk = (x - ([0] + offs)[k] + side) % side
        if k:
            remote(hbuf.at[xk], hbuf.at[xk], h_send.at[k - 1], h_recv.at[k - 1], row_peers[k - 1]).wait_recv()

        def step(n, _):
            d = (n + 1) % col
            g = (mine + d) % col
            part = lax.dot_general(w_ref[g], hbuf[xk], NT, preferred_element_type=F32).astype(BF16)

            @pl.when(d != 0)
            def _():
                sbuf[k, d] = part
                slot_copy(k, d, xk).start()

            @pl.when(d == 0)
            def _():
                out_ref[index_of(side, y, xk, c)] = part

            return 0

        lax.fori_loop(0, col, step, 0)
    for copy in sends:
        copy.wait_send()
    for k in range(side):
        for d in range(1, col):
            slot_copy(k, d, x).wait()


def attention_kernel(side, scale, block, qkv_ref, o_ref, sbuf, send_sem, recv_sem):
    tp, three_dim, share = qkv_ref.shape
    dim = three_dim // 3
    me, _, _, _ = place(side)
    per = block // share
    c2 = scale * math.log2(math.e)
    rows = lax.broadcasted_iota(jnp.int32, (block, block), 0)
    cols = lax.broadcasted_iota(jnp.int32, (block, block), 1)
    enter([(me + d) % tp for d in range(1, tp)])

    def part(i, which):
        return jnp.concatenate([qkv_ref[i * per + n, which * dim : (which + 1) * dim, :] for n in range(per)], axis=1)

    def o_copy(d):
        return remote(sbuf.at[d], o_ref.at[me], send_sem.at[d], recv_sem.at[d], (me + d) % tp)

    def q_step(i, _):
        q = part(i, 0).T

        def scores(j):
            return lax.dot_general(q, part(j, 1), NN, preferred_element_type=F32)

        def update(s, j, carry):
            m, l, acc = carry
            m_new = jnp.maximum(m, jnp.max(s, axis=-1, keepdims=True))
            p = jnp.exp2(s * c2 - m_new * c2)
            alpha = jnp.exp2((m - m_new) * c2)
            acc = acc * alpha + lax.dot_general(p.astype(BF16), part(j, 2), NT, preferred_element_type=F32)
            return m_new, l * alpha + jnp.sum(p, axis=-1, keepdims=True), acc

        init = (jnp.full((block, 1), -1e30, F32), jnp.zeros((block, 1), F32), jnp.zeros((block, dim), F32))
        carry = lax.fori_loop(0, i, lambda j, carry: update(scores(j), j, carry), init)
        _, l, acc = update(jnp.where(rows >= cols, scores(i), -1e30), i, carry)
        o_t = (acc / l).T.astype(BF16)
        for n in range(per):
            d = (i * per + n - me + tp) % tp
            piece = o_t[:, n * share : (n + 1) * share]

            @pl.when(d != 0)
            def _():
                sbuf[d] = piece
                o_copy(d).start()

            @pl.when(d == 0)
            def _():
                o_ref[me] = piece

        return 0

    lax.fori_loop(0, tp * share // block, q_step, 0)

    def drain(d, _):
        o_copy(d).wait()
        return 0

    lax.fori_loop(1, tp, drain, 0)


def mlp_kernel(side, r_ref, o_ref, bo_ref, gain_ref, shift_ref, bu_ref, bd_ref, wo_hbm, wu_hbm, wd_hbm, out_ref,
               wo, wu, wd, hbuf, ubuf, zsend, zrecv, resid, w_sem, h_send, h_recv, z_send, z_recv):
    me, y, x, c = place(side)
    offs = ring_order(side)
    width = r_ref.shape[1]
    share = r_ref.shape[0]
    tile = 256
    loads = [pltpu.make_async_copy(src, dst, w_sem.at[n]) for n, (src, dst) in enumerate(((wo_hbm, wo), (wu_hbm, wu), (wd_hbm, wd)))]
    for load in loads:
        load.start()
    fwd = [index_of(side, y, (x + off) % side, c) for off in offs]
    enter(fwd)
    o_t = o_ref[...].reshape(wo.shape[0], share)
    loads[0].wait()

    def out_step(n, _):
        cs = pl.ds(pl.multiple_of(n * tile, tile), tile)
        resid[:, cs] = r_ref[:, cs].astype(F32) + (lax.dot_general(o_t, wo[:, cs], TN, preferred_element_type=F32) + bo_ref[:, cs])
        return 0

    lax.fori_loop(0, width // tile, out_step, 0)
    hbuf[x] = norm(resid[...], gain_ref[...], shift_ref[...])
    sends = [remote(hbuf.at[x], hbuf.at[x], h_send.at[n], h_recv.at[n], fwd[n]) for n in range(len(offs))]
    for copy in sends:
        copy.start()
    loads[1].wait()
    loads[2].wait()
    back = [index_of(side, y, (x - off + side) % side, c) for off in offs]
    z_copies = [remote(zsend.at[n], zrecv.at[n], z_send.at[n], z_recv.at[n], back[n]) for n in range(len(offs))]
    for k in range(side):
        xk = (x - ([0] + offs)[k] + side) % side
        if k:
            sends[k - 1].wait_recv()

        def up_step(g, _):
            pre = lax.dot_general(hbuf[xk], wu[g], NN, preferred_element_type=F32) + bu_ref[g]
            ubuf[:, pl.ds(pl.multiple_of(g * wu.shape[2], 128), wu.shape[2])] = jax.nn.gelu(pre, approximate=True).astype(BF16)
            return 0

        lax.fori_loop(0, wu.shape[0], up_step, 0)

        def down_step(n, _):
            cs = pl.ds(pl.multiple_of(n * tile, tile), tile)
            z = lax.dot_general(ubuf[...], wd[:, cs], NN, preferred_element_type=F32)
            if k:
                zsend[k - 1, :, cs] = z.astype(BF16)
            else:
                resid[:, cs] = resid[:, cs] + (z + bd_ref[:, cs])
            return 0

        lax.fori_loop(0, width // tile, down_step, 0)
        if k:
            z_copies[k - 1].start()
    for copy in z_copies:
        copy.wait_recv()
    total = resid[...]
    for n in range(len(offs)):
        total = total + zrecv[n].astype(F32)
    out_ref[...] = total.astype(out_ref.dtype)
    for copy in sends + z_copies:
        copy.wait_send()


def params(collective_id):
    return pltpu.CompilerParams(collective_id=collective_id, has_side_effects=True, vmem_limit_bytes=60 * 1024 * 1024)


def solution(mesh):
    tp = mesh.shape["tp"]
    side = math.isqrt(tp // CORES)
    col_groups = [[(y * side + x) * CORES + c for y in range(side) for c in range(CORES)] for x in range(side)]
    col = side * CORES
    near = side - 1

    def local_forward(x_local, ln1_gain, ln1_bias, ln2_gain, ln2_bias, w_qkv, w_out, b_out, w_up, b_up, w_down, b_down):
        _, share, width = x_local.shape
        layers, _, three, _, dim = w_qkv.shape
        scale = 1.0 / math.sqrt(dim)
        hidden = w_up.shape[2]
        wq_t = jnp.transpose(w_qkv, (0, 2, 3, 4, 1)).reshape(layers, three * dim, width)
        bup_all = lax.all_gather(b_up, "tp", axis=0, axis_index_groups=col_groups)
        gathered = []
        for layer in range(layers):
            gathered.append((
                lax.all_gather(wq_t[layer], "tp", axis=0, axis_index_groups=col_groups),
                lax.all_gather(w_out[layer].reshape(dim, width), "tp", axis=0),
                lax.all_gather(w_up[layer], "tp", axis=0, axis_index_groups=col_groups),
                lax.all_gather(w_down[layer], "tp", axis=0, axis_index_groups=col_groups),
            ))
        resid = x_local[0]
        for layer in range(layers):
            gq, go, gu, gd = gathered[layer]
            qkv = pl.pallas_call(
                functools.partial(qkv_kernel, side),
                out_shape=jax.ShapeDtypeStruct((tp, three * dim, share), BF16),
                in_specs=[VMEM, VMEM, VMEM, HBM],
                out_specs=VMEM,
                scratch_shapes=[
                    pltpu.VMEM((col, three * dim, width), BF16),
                    pltpu.VMEM((side, share, width), BF16),
                    pltpu.VMEM((side, col, three * dim, share), BF16),
                    DMA, DMA((near,)), DMA((near,)), DMA((side, col)), DMA((side, col)),
                ],
                compiler_params=params(0),
                cost_estimate=pl.CostEstimate(flops=20_000_000_000, bytes_accessed=10_000_000, transcendentals=0),
                name=f"qkv{layer}",
            )(resid, ln1_gain[layer : layer + 1], ln1_bias[layer : layer + 1], gq)
            o = pl.pallas_call(
                functools.partial(attention_kernel, side, scale, 4 * share),
                out_shape=jax.ShapeDtypeStruct((tp, dim, share), BF16),
                in_specs=[VMEM],
                out_specs=VMEM,
                scratch_shapes=[pltpu.VMEM((tp, dim, share), BF16), DMA((tp,)), DMA((tp,))],
                compiler_params=params(1),
                cost_estimate=pl.CostEstimate(flops=20_000_000_000, bytes_accessed=10_000_000, transcendentals=0),
                name=f"attention{layer}",
            )(qkv)
            last = layer == layers - 1
            resid = pl.pallas_call(
                functools.partial(mlp_kernel, side),
                out_shape=jax.ShapeDtypeStruct((share, width), BF16 if last else F32),
                in_specs=[VMEM] * 7 + [HBM] * 3,
                out_specs=VMEM,
                scratch_shapes=[
                    pltpu.VMEM((tp * dim, width), BF16),
                    pltpu.VMEM((col, width, hidden), BF16),
                    pltpu.VMEM((col * hidden, width), BF16),
                    pltpu.VMEM((side, share, width), BF16),
                    pltpu.VMEM((share, col * hidden), BF16),
                    pltpu.VMEM((near, share, width), BF16),
                    pltpu.VMEM((near, share, width), BF16),
                    pltpu.VMEM((share, width), F32),
                    DMA((3,)), DMA((near,)), DMA((near,)), DMA((near,)), DMA((near,)),
                ],
                compiler_params=params(2),
                cost_estimate=pl.CostEstimate(flops=30_000_000_000, bytes_accessed=30_000_000, transcendentals=0),
                name=f"mlp{layer}",
            )(resid, o, b_out[layer : layer + 1], ln2_gain[layer : layer + 1], ln2_bias[layer : layer + 1],
              bup_all[:, layer][:, None], b_down[layer : layer + 1], go.reshape(tp * dim, width), gu, gd.reshape(col * hidden, width))
        return resid[None]

    rows_spec = P("dp", "tp", None)
    in_specs = (rows_spec, P(), P(), P(), P(), P(None, None, None, "tp", None), P(None, "tp", None, None), P(), P(None, None, "tp"), P(None, "tp"), P(None, "tp", None), P())
    return jax.shard_map(local_forward, mesh=mesh, in_specs=in_specs, out_specs=rows_spec, check_vma=False)
```

```python
import functools
import math
import jax
import jax.numpy as jnp
from jax import lax
from jax.experimental import pallas as pl
from jax.experimental.pallas import tpu as pltpu
from jax.sharding import PartitionSpec as P

F32 = jnp.float32
BF16 = jnp.bfloat16
CORES = 2
NN = (((1,), (0,)), ((), ()))
NT = (((1,), (1,)), ((), ()))
TN = (((0,), (0,)), ((), ()))
MESH = pl.DeviceIdType.MESH
VMEM = pl.BlockSpec(memory_space=pltpu.VMEM)
HBM = pl.BlockSpec(memory_space=pl.ANY)
DMA = pltpu.SemaphoreType.DMA


def place(side):
    me = lax.axis_index("tp")
    return me, me // (side * CORES), (me // CORES) % side, me % CORES


def index_of(side, y, x, c):
    return (y * side + x) * CORES + c


def dev(index):
    return {"tp": index}


def remote(src, dst, send_sem, recv_sem, index):
    return pltpu.make_async_remote_copy(src_ref=src, dst_ref=dst, send_sem=send_sem, recv_sem=recv_sem, device_id=dev(index), device_id_type=MESH)


def enter(indices):
    barrier = pltpu.get_barrier_semaphore()
    for index in indices:
        pl.semaphore_signal(barrier, inc=1, device_id=dev(index), device_id_type=MESH)
    pl.semaphore_wait(barrier, len(indices))


def norm(resid, gain, shift):
    row_mean = jnp.mean(resid, axis=-1, keepdims=True)
    centered = resid - row_mean
    variance = jnp.mean(centered * centered, axis=-1, keepdims=True)
    return (centered * lax.rsqrt(variance + 1e-5) * gain + shift).astype(BF16)


def ring_order(side):
    return sorted(range(1, side), key=lambda off: min(off, side - off))


class Gather:
    def __init__(self, ring, src, slot, half, recv, send, partner):
        self.prev, self.next, self.back, self.here, self.fwd, self.far = ring
        self.src, self.slot, self.half, self.recv, self.send, self.partner = src, slot, half, recv, send, partner

    def start(self):
        dst = self.slot(self.here, 0)
        remote(self.src, dst, self.send, self.recv.at[0], self.next).start()
        remote(self.src, dst, self.send, self.recv.at[1], self.prev).start()
        if self.partner is not None:
            remote(self.src, dst, self.send, self.recv.at[4], self.partner).start()

    def landed(self, ref, n):
        remote(ref, ref, self.send, self.recv.at[n], self.next).wait_recv()

    def share(self, pos, n):
        if self.partner is not None:
            ref = self.slot(pos, 0)
            remote(ref, ref, self.send, self.recv.at[n], self.partner).start()

    def relay(self):
        for n, pos, to in ((0, self.back, self.next), (1, self.fwd, self.prev)):
            self.landed(self.slot(pos, 0), n)
            ref = self.half(pos, n)
            remote(ref, ref, self.send, self.recv.at[2 + n], to).start()
            self.share(pos, 5 + n)

    def last(self):
        self.landed(self.half(self.far, 0), 2)
        self.landed(self.half(self.far, 1), 3)
        self.share(self.far, 7)

    def finish(self):
        if self.partner is not None:
            for n, pos in enumerate((self.here, self.back, self.fwd, self.far)):
                self.landed(self.slot(pos, 1), 4 + n)

    def drain(self, whole):
        ref = whole(7 if self.partner is not None else 3)
        remote(ref, ref, self.send, self.recv.at[0], self.next).wait_send()


def decoder_kernel(side, layers, x_ref, ln1g, ln1b, ln2g, ln2b, bo_ref, bu_ref, bd_ref, wq_in, wo_in, wu_in, wd_in,
                   out_ref, gq, go, gu, gd,
                   wq, wo, wu, wd, h1, h2, qkv, qsend, oall, osend, ubuf, zsend, zrecv, resid, bup,
                   g_recv, g_send, h_send, h_recv, q_sem, o_sem, z_send, z_recv, b_sem, l_sem):
    me, y, x, c = place(side)
    col = side * CORES
    tp = side * col
    near = side - 1
    mine = y * CORES + c
    offs = ring_order(side)
    share, width = x_ref.shape
    dim = oall.shape[2]
    hidden = wu.shape[2]
    tile = 256
    partner = index_of(side, y, x, 1 - c)

    def in_col(m):
        return index_of(side, m // CORES, x, m % CORES)

    def ring(at, p):
        back, fwd, far = (p + side - 1) % side, (p + 1) % side, (p + 2) % side
        return at(back), at(fwd), back, p, fwd, far

    along_y = ring(lambda p: index_of(side, p, x, c), y)
    along_x = ring(lambda p: index_of(side, y, p, c), x)

    def weights(layer, n, src, buf):
        rows = buf.shape[2] // 2

        def slot(pos, other):
            return buf.at[layer, pos * CORES + (c if other == 0 else 1 - c)]

        def half(pos, n):
            return buf.at[layer, pos * CORES + c, pl.ds(n * rows, rows)]

        return Gather(along_y, src.at[layer], slot, half, g_recv.at[layer, n], g_send.at[layer, n], partner)

    def w_out_y(layer):
        here = x * CORES + c

        def slot(pos, other):
            return go.at[layer, here, pl.ds(pl.multiple_of(pos * dim, dim), dim)]

        def half(pos, n):
            return go.at[layer, here, pl.ds(pl.multiple_of(pos * dim + n * (dim // 2), dim // 2), dim // 2)]

        return Gather(along_y, wo_in.at[layer], slot, half, g_recv.at[layer, 3], g_send.at[layer, 3], None)

    def w_out_x(layer):
        rows = go.shape[2] // 2

        def slot(pos, other):
            return go.at[layer, pos * CORES + (c if other == 0 else 1 - c)]

        def half(pos, n):
            return go.at[layer, pos * CORES + c, pl.ds(n * rows, rows)]

        return Gather(along_x, slot(x, 0), slot, half, g_recv.at[layer, 4], g_send.at[layer, 4], partner)

    q_job = [weights(layer, 0, wq_in, gq) for layer in range(layers)]
    u_job = [weights(layer, 1, wu_in, gu) for layer in range(layers)]
    d_job = [weights(layer, 2, wd_in, gd) for layer in range(layers)]
    oy_job = [w_out_y(layer) for layer in range(layers)]
    ox_job = [w_out_x(layer) for layer in range(layers)]

    def load_rest(buf, dst, layer, n):
        return [pltpu.make_async_copy(buf.at[layer, (mine + d) % col], dst.at[(mine + d) % col], l_sem.at[n, d]) for d in range(1, col)]

    def own_load(src, dst, layer, n):
        return pltpu.make_async_copy(src.at[layer], dst.at[mine], l_sem.at[n, 0])

    def begin(copies):
        for copy in copies:
            copy.start()

    def end(copies):
        for copy in copies:
            copy.wait()

    enter([(me + d) % tp for d in range(1, tp)])
    q_job[0].start()
    for layer in range(layers):
        out_copy(wo_in, oy_job, layer, y, l_sem).start()
    for d in range(1, col):
        remote(bu_ref, bup.at[mine], b_sem.at[0], b_sem.at[1], in_col((mine + d) % col)).start()
    bup[mine] = bu_ref[...]
    resid[...] = x_ref[...].astype(F32)

    def send_h(layer, which, buf):
        peers = [index_of(side, y, (x + off) % side, c) for off in offs]
        return [remote(buf.at[layer, x], buf.at[layer, x], h_send.at[layer, which, n], h_recv.at[layer, which, n], peers[n]) for n in range(near)]

    for layer in range(layers):
        first, final = layer == 0, layer == layers - 1
        row = slice(layer, layer + 1)
        h1[layer, x] = norm(resid[...], ln1g[row, :], ln1b[row, :])
        h_copies = send_h(layer, 0, h1)
        begin(h_copies)
        if first:
            loads = [own_load(wq_in, wq, layer, 0)] + load_rest(gq, wq, layer, 0)
            loads[0].start()
            oy_job[0].start()
            q_job[0].relay()
            q_job[0].last()
            q_job[0].finish()
            begin(loads[1:])
            end(loads)

        def q_copy(k, d, xk):
            return remote(qsend.at[k, d], qkv.at[layer, index_of(side, y, xk, c)], q_sem.at[layer, 0], q_sem.at[layer, 1], in_col((mine + d) % col))

        for k in range(side):
            xk = (x - ([0] + offs)[k] + side) % side
            if k:
                h_copies[k - 1].wait_recv()

            def q_part(n, _):
                d = (n + 1) % col
                part = lax.dot_general(wq[(mine + d) % col], h1[layer, xk], NT, preferred_element_type=F32).astype(BF16)

                @pl.when(d != 0)
                def _():
                    qsend[k, d] = part
                    q_copy(k, d, xk).start()

                @pl.when(d == 0)
                def _():
                    qkv[layer, index_of(side, y, xk, c)] = part

                return 0

            lax.fori_loop(0, col, q_part, 0)
        oy_job[layer].relay()
        oy_job[layer].last()
        out_copy(wo_in, oy_job, layer, y, l_sem).wait()
        ox_job[layer].start()
        if first:
            u_job[layer].start()
        else:
            u_job[layer].relay()
            d_job[layer].start()
        moved = qkv.at[layer, pl.ds(0, side * (col - 1))]
        everything_qkv = remote(moved, moved, q_sem.at[layer, 0], q_sem.at[layer, 1], me)
        everything_qkv.wait_recv()

        def hook():
            ox_job[layer].relay()
            if first:
                u_job[layer].relay()
            else:
                u_job[layer].last()

        attend(side, layer, me, c, x, y, qkv, oall, osend, o_sem, hook)

        if first:
            d_job[layer].start()
        ox_job[layer].last()
        if first:
            u_job[layer].last()
        else:
            d_job[layer].relay()
        moved = oall.at[layer, pl.ds(0, tp - 1)]
        everything_o = remote(moved, moved, o_sem.at[layer, 0], o_sem.at[layer, 1], me)
        ox_job[layer].finish()
        load_o = pltpu.make_async_copy(go.at[layer], wo, l_sem.at[1, 0])
        load_o.start()
        load_u = [own_load(wu_in, wu, layer, 2)] + load_rest(gu, wu, layer, 2)
        load_d = [own_load(wd_in, wd, layer, 3)] + load_rest(gd, wd, layer, 3)
        begin([load_u[0], load_d[0]])
        everything_o.wait_recv()
        load_o.wait()
        o_t = oall[layer].reshape(tp * dim, share)

        def out_step(n, _):
            cs = pl.ds(pl.multiple_of(n * tile, tile), tile)
            w = wo[:, :, cs].reshape(tp * dim, tile)
            resid[:, cs] = resid[:, cs] + (lax.dot_general(o_t, w, TN, preferred_element_type=F32) + bo_ref[row, cs])
            return 0

        lax.fori_loop(0, width // tile, out_step, 0)
        h2[layer, x] = norm(resid[...], ln2g[row, :], ln2b[row, :])
        g_copies = send_h(layer, 1, h2)
        begin(g_copies)
        u_job[layer].finish()
        begin(load_u[1:])
        if first:
            moved = bup.at[pl.ds(0, col - 1)]
            remote(moved, moved, b_sem.at[0], b_sem.at[1], me).wait()
        else:
            d_job[layer].last()
        end(load_u)

        def chunk(k):
            return (x - ([0] + offs)[k] + side) % side

        def up(k):
            if k:
                g_copies[k - 1].wait_recv()

            def up_step(g, _):
                pre = lax.dot_general(h2[layer, chunk(k)], wu[g], NN, preferred_element_type=F32) + bup[g, row, :]
                ubuf[k, :, pl.ds(pl.multiple_of(g * hidden, 128), hidden)] = jax.nn.gelu(pre, approximate=True).astype(BF16)
                return 0

            lax.fori_loop(0, col, up_step, 0)

        z_copies = [remote(zsend.at[n], zrecv.at[layer, n], z_send.at[layer, n], z_recv.at[layer, n], index_of(side, y, chunk(n + 1), c)) for n in range(near)]

        def down(k):
            def down_step(n, _):
                cs = pl.ds(pl.multiple_of(n * tile, tile), tile)
                w = wd[:, :, cs].reshape(col * hidden, tile)
                z = lax.dot_general(ubuf[k], w, NN, preferred_element_type=F32)
                if k:
                    zsend[k - 1, :, cs] = z.astype(BF16)
                else:
                    resid[:, cs] = resid[:, cs] + (z + bd_ref[row, cs])
                return 0

            lax.fori_loop(0, width // tile, down_step, 0)
            if k:
                z_copies[k - 1].start()

        up(0)
        if first:
            d_job[layer].relay()
            if not final:
                q_job[layer + 1].start()
                oy_job[layer + 1].start()
            for k in range(1, side):
                up(k)
                if k == near - 1:
                    d_job[layer].last()
            d_job[layer].finish()
            begin(load_d[1:])
            end(load_d)
            for k in range(1, side):
                down(k)
            if not final:
                q_job[layer + 1].relay()
                q_job[layer + 1].last()
                u_job[layer + 1].start()
            down(0)
        else:
            if not final:
                q_job[layer + 1].start()
                oy_job[layer + 1].start()
            d_job[layer].finish()
            begin(load_d[1:])
            end(load_d)
            down(0)
            for k in range(1, side):
                up(k)
                down(k)
            if not final:
                q_job[layer + 1].relay()
                q_job[layer + 1].last()
                u_job[layer + 1].start()
        if not final:
            q_job[layer + 1].finish()
            loads = [own_load(wq_in, wq, layer + 1, 0)] + load_rest(gq, wq, layer + 1, 0)
            begin(loads)
        for copy in z_copies:
            copy.wait_recv()
        total = resid[...]
        for n in range(near):
            total = total + zrecv[layer, n].astype(F32)
        if final:
            out_ref[...] = total.astype(BF16)
        else:
            resid[...] = total
            end(loads)
        everything_qkv.wait_send()
        everything_o.wait_send()
        for copy in h_copies + g_copies + z_copies:
            copy.wait_send()
    for layer in range(layers):
        q_job[layer].drain(lambda n: gq.at[layer, pl.ds(0, n)])
        u_job[layer].drain(lambda n: gu.at[layer, pl.ds(0, n)])
        d_job[layer].drain(lambda n: gd.at[layer, pl.ds(0, n)])
        ox_job[layer].drain(lambda n: go.at[layer, pl.ds(0, n)])
        oy_job[layer].drain(lambda n: go.at[layer, 0, pl.ds(0, n * dim)])


def out_copy(wo_in, oy_job, layer, y, l_sem):
    return pltpu.make_async_copy(wo_in.at[layer], oy_job[layer].slot(y, 0), l_sem.at[4, layer])


def attend(side, layer, me, c, x, y, qkv, oall, osend, o_sem, hook):
    _, tp, three_dim, share = qkv.shape
    dim = three_dim // 3
    per = 4
    block = per * share
    c2 = math.log2(math.e) / math.sqrt(dim)
    rows = lax.broadcasted_iota(jnp.int32, (block, block), 0)
    cols = lax.broadcasted_iota(jnp.int32, (block, block), 1)
    slot = (x * CORES + c) * side + y
    steps = tp // per

    def part(i, which):
        return jnp.concatenate([qkv[layer, i * per + n, which * dim : (which + 1) * dim, :] for n in range(per)], axis=1)

    def q_step(i, _):
        @pl.when(i == steps - 1)
        def _():
            hook()

        q = part(i, 0).T

        def scores(j):
            return lax.dot_general(q, part(j, 1), NN, preferred_element_type=F32)

        def update(s, j, carry):
            m, l, acc = carry
            m_new = jnp.maximum(m, jnp.max(s, axis=-1, keepdims=True))
            p = jnp.exp2(s * c2 - m_new * c2)
            alpha = jnp.exp2((m - m_new) * c2)
            acc = acc * alpha + lax.dot_general(p.astype(BF16), part(j, 2), NT, preferred_element_type=F32)
            return m_new, l * alpha + jnp.sum(p, axis=-1, keepdims=True), acc

        init = (jnp.full((block, 1), -1e30, F32), jnp.zeros((block, 1), F32), jnp.zeros((block, dim), F32))
        carry = lax.fori_loop(0, i, lambda j, carry: update(scores(j), j, carry), init)
        _, l, acc = update(jnp.where(rows >= cols, scores(i), -1e30), i, carry)
        o_t = (acc / l).T.astype(BF16)
        for n in range(per):
            d = (i * per + n - me + tp) % tp
            piece = o_t[:, n * share : (n + 1) * share]

            @pl.when(d != 0)
            def _():
                osend[d] = piece
                remote(osend.at[d], oall.at[layer, slot], o_sem.at[layer, 0], o_sem.at[layer, 1], i * per + n).start()

            @pl.when(d == 0)
            def _():
                oall[layer, slot] = piece

        return 0

    lax.fori_loop(0, steps, q_step, 0)


def solution(mesh):
    tp = mesh.shape["tp"]
    side = math.isqrt(tp // CORES)
    col = side * CORES
    near = side - 1

    def local_forward(x_local, ln1_gain, ln1_bias, ln2_gain, ln2_bias, w_qkv, w_out, b_out, w_up, b_up, w_down, b_down):
        _, share, width = x_local.shape
        layers, _, three, _, dim = w_qkv.shape
        hidden = w_up.shape[2]
        wq_t = jnp.transpose(w_qkv, (0, 2, 3, 4, 1)).reshape(layers, three * dim, width)
        hbm = lambda *shape: jax.ShapeDtypeStruct(shape, BF16)
        vmem = lambda *shape: pltpu.VMEM(shape, BF16)
        y = pl.pallas_call(
            functools.partial(decoder_kernel, side, layers),
            out_shape=(
                hbm(share, width), hbm(layers, col, three * dim, width), hbm(layers, col, side * dim, width),
                hbm(layers, col, width, hidden), hbm(layers, col, hidden, width),
            ),
            in_specs=[VMEM] * 8 + [HBM] * 4,
            out_specs=(VMEM, HBM, HBM, HBM, HBM),
            scratch_shapes=[
                vmem(col, three * dim, width), vmem(col, side * dim, width), vmem(col, width, hidden), vmem(col, hidden, width),
                vmem(layers, side, share, width), vmem(layers, side, share, width),
                vmem(layers, tp, three * dim, share), vmem(side, col, three * dim, share),
                vmem(layers, tp, dim, share), vmem(tp, dim, share),
                vmem(side, share, col * hidden),
                vmem(near, share, width), vmem(layers, near, share, width),
                pltpu.VMEM((share, width), F32), pltpu.VMEM((col, layers, hidden), F32),
                DMA((layers, 5, 8)), DMA((layers, 5)), DMA((layers, 2, near)), DMA((layers, 2, near)),
                DMA((layers, 2)), DMA((layers, 2)), DMA((layers, near)), DMA((layers, near)), DMA((2,)), DMA((5, 8)),
            ],
            compiler_params=pltpu.CompilerParams(collective_id=0, has_side_effects=True, vmem_limit_bytes=63 * 1024 * 1024),
            name="decoder",
        )(x_local[0], ln1_gain, ln1_bias, ln2_gain, ln2_bias, b_out, b_up, b_down, wq_t, w_out.reshape(layers, dim, width), w_up, w_down)[0]
        return y[None]

    rows_spec = P("dp", "tp", None)
    in_specs = (rows_spec, P(), P(), P(), P(), P(None, None, None, "tp", None), P(None, "tp", None, None), P(), P(None, None, "tp"), P(None, "tp"), P(None, "tp", None), P())
    return jax.shard_map(local_forward, mesh=mesh, in_specs=in_specs, out_specs=rows_spec, check_vma=False)
```

```python
import functools
import math
import jax
import jax.numpy as jnp
from jax import lax
from jax.experimental import pallas as pl
from jax.experimental.pallas import tpu as pltpu
from jax.sharding import PartitionSpec as P

F32 = jnp.float32
BF16 = jnp.bfloat16
CORES = 2
NN = (((1,), (0,)), ((), ()))
NT = (((1,), (1,)), ((), ()))
TN = (((0,), (0,)), ((), ()))
MESH = pl.DeviceIdType.MESH
VMEM = pl.BlockSpec(memory_space=pltpu.VMEM)
HBM = pl.BlockSpec(memory_space=pl.ANY)
DMA = pltpu.SemaphoreType.DMA


def index_of(side, y, x, c):
    return (y * side + x) * CORES + c


def dev(index):
    return {"tp": index}


def remote(src, dst, send_sem, recv_sem, index):
    return pltpu.make_async_remote_copy(src_ref=src, dst_ref=dst, send_sem=send_sem, recv_sem=recv_sem, device_id=dev(index), device_id_type=MESH)


def enter(indices):
    barrier = pltpu.get_barrier_semaphore()
    for index in indices:
        pl.semaphore_signal(barrier, inc=1, device_id=dev(index), device_id_type=MESH)
    pl.semaphore_wait(barrier, len(indices))


def norm(resid, gain, shift):
    row_mean = jnp.mean(resid, axis=-1, keepdims=True)
    centered = resid - row_mean
    variance = jnp.mean(centered * centered, axis=-1, keepdims=True)
    return (centered * lax.rsqrt(variance + 1e-5) * gain + shift).astype(BF16)


scope = jax.named_scope


class Gather:
    def __init__(self, name, ring, src, slot, half, recv, send, partner, dst=None, load_sem=None, number=None):
        self.name = name
        self.prev, self.next, self.back, self.here, self.fwd, self.far = ring
        self.src, self.slot, self.half, self.recv, self.send, self.partner = src, slot, half, recv, send, partner
        self.dst, self.load_sem, self.number = dst, load_sem, number

    def order(self):
        return (self.here, self.back, self.fwd, self.far)

    def start(self):
        dst = self.slot(self.here, 0)
        remote(self.src, dst, self.send, self.recv.at[0], self.next).start()
        remote(self.src, dst, self.send, self.recv.at[1], self.prev).start()
        if self.partner is not None:
            remote(self.src, dst, self.send, self.recv.at[4], self.partner).start()

    def landed(self, ref, n):
        remote(ref, ref, self.send, self.recv.at[n], self.next).wait_recv()

    def load(self, i, other):
        pos = self.order()[i]
        src = self.src if i == 0 and other == 0 else self.slot(pos, other)
        return pltpu.make_async_copy(src, self.dst.at[self.number(pos, other)], self.load_sem.at[2 * i + other])

    def share(self, pos, n):
        ref = self.slot(pos, 0)
        remote(ref, ref, self.send, self.recv.at[n], self.partner).start()

    def relay(self):
        with scope(self.name + "_relay"):
            for n, pos, to in ((0, self.back, self.next), (1, self.fwd, self.prev)):
                self.landed(self.slot(pos, 0), n)
                ref = self.half(pos, n)
                remote(ref, ref, self.send, self.recv.at[2 + n], to).start()
                if self.partner is not None:
                    self.share(pos, 5 + n)
                    self.load(1 + n, 0).start()

    def own(self):
        self.load(0, 0).start()

    def other(self, i):
        with scope(f"{self.name}_other{i}"):
            self.landed(self.slot(self.order()[i], 1), 4 + i)
            self.load(i, 1).start()

    def last(self):
        with scope(self.name + "_last"):
            self.landed(self.half(self.far, 0), 2)
            self.landed(self.half(self.far, 1), 3)
            if self.partner is not None:
                self.share(self.far, 7)
                self.load(3, 0).start()

    def ready(self, *which):
        with scope(self.name + "_ready"):
            for i in which:
                self.load(i, 0).wait()
                self.load(i, 1).wait()

    def drain(self, ref):
        remote(ref, ref, self.send, self.recv.at[0], self.next).wait_send()


class Layer:
    def __init__(self, side, layer, y, x, c):
        self.side, self.swap, self.c = side, layer % 2, c
        self.w, self.t = (x, y) if self.swap else (y, x)
        self.mine = self.w * CORES + c

    def at(self, w, t, c):
        return index_of(self.side, t, w, c) if self.swap else index_of(self.side, w, t, c)

    def in_w(self, m):
        return self.at(m // CORES, self.t, m % CORES)

    def ring(self, along_w):
        side, c = self.side, self.c
        p = self.w if along_w else self.t
        back, fwd, far = (p + side - 1) % side, (p + 1) % side, (p + 2) % side
        at = (lambda q: self.at(q, self.t, c)) if along_w else (lambda q: self.at(self.w, q, c))
        return at(back), at(fwd), back, p, fwd, far

    def owner(self, k):
        return self.at(self.w, (self.t + (0, self.side - 1, 1, 2)[k]) % self.side, self.c)


def decoder_kernel(side, layers, x_ref, ln1g, ln1b, ln2g, ln2b, bo_ref, bu_ref, bd_ref, wq_in, wo_in, wu_in, wd_in,
                   out_ref, gq, go, gu, gd,
                   wq, wo, wu, wd, h1, h2, qkv, qsend, oall, osend, ubuf, zsend, zrecv, resid, bup,
                   g_recv, g_send, h_send, h_recv, q_sem, o_sem, z_send, z_recv, b_sem, l_sem, c_sem):
    me = lax.axis_index("tp")
    y, x, c = me // (side * CORES), (me // CORES) % side, me % CORES
    col = side * CORES
    tp = side * col
    near = side - 1
    share, width = x_ref.shape
    dim = oall.shape[2]
    hidden = wu.shape[2]
    tile = 256
    partner = index_of(side, y, x, 1 - c)
    at = [Layer(side, layer, y, x, c) for layer in range(layers)]

    def number(pos, other):
        return pos * CORES + (c if other == 0 else 1 - c)

    def weights(layer, n, name, src, buf, dst):
        rows = buf.shape[2] // 2
        return Gather(
            f"L{layer}_{name}", at[layer].ring(True), src.at[layer],
            lambda pos, other: buf.at[layer, number(pos, other)],
            lambda pos, k: buf.at[layer, number(pos, 0), pl.ds(k * rows, rows)],
            g_recv.at[layer, n], g_send.at[layer, n], partner, dst, l_sem.at[layer, n], number)

    def out_w(layer):
        here = number(at[layer].t, 0)
        half = dim // 2
        return Gather(
            f"L{layer}_ow", at[layer].ring(True), wo_in.at[layer],
            lambda pos, other: go.at[layer, here, pl.ds(pl.multiple_of(pos * dim, dim), dim)],
            lambda pos, k: go.at[layer, here, pl.ds(pl.multiple_of(pos * dim + k * half, half), half)],
            g_recv.at[layer, 3], g_send.at[layer, 3], None)

    def out_t(layer):
        rows = go.shape[2] // 2
        return Gather(
            f"L{layer}_ot", at[layer].ring(False), go.at[layer, number(at[layer].t, 0)],
            lambda pos, other: go.at[layer, number(pos, other)],
            lambda pos, k: go.at[layer, number(pos, 0), pl.ds(k * rows, rows)],
            g_recv.at[layer, 4], g_send.at[layer, 4], partner, wo, l_sem.at[layer, 4], number)

    q_job = [weights(layer, 0, "q", wq_in, gq, wq) for layer in range(layers)]
    u_job = [weights(layer, 1, "u", wu_in, gu, wu) for layer in range(layers)]
    d_job = [weights(layer, 2, "d", wd_in, gd, wd) for layer in range(layers)]
    ow_job = [out_w(layer) for layer in range(layers)]
    ot_job = [out_t(layer) for layer in range(layers)]

    def own_out(layer):
        return pltpu.make_async_copy(wo_in.at[layer], ow_job[layer].slot(at[layer].w, 0), c_sem.at[layer])

    def all_bias(layer):
        moved = bup.at[layer, pl.ds(0, col - 1)]
        return remote(moved, moved, b_sem.at[layer, 0], b_sem.at[layer, 1], me)

    with scope("enter"):
        enter([(me + d) % tp for d in range(1, tp)])
    ow_job[0].start()
    q_job[0].start()
    for layer in range(layers):
        own_out(layer).start()
        mine = at[layer].mine
        for d in range(1, col):
            row = bu_ref.at[layer]
            remote(row, bup.at[layer, mine], b_sem.at[layer, 0], b_sem.at[layer, 1], at[layer].in_w((mine + d) % col)).start()
        bup[layer, mine] = bu_ref[layer]
    q_job[0].own()
    resid[...] = x_ref[...].astype(F32)

    class Spread:
        def __init__(self, layer, which, buf):
            self.buf, self.name = buf.at[layer], f"L{layer}_h{which}"
            self.send, self.recv = h_send.at[layer, which], h_recv.at[layer, which]
            self.prev, self.next = at[layer].ring(False)[:2]
            self.half = share // 2

        def full(self, k):
            return remote(self.buf.at[0], self.buf.at[k], self.send.at[k - 1], self.recv.at[k - 1], self.next if k == 1 else self.prev)

        def part(self, k):
            rows = pl.ds((k - 1) * self.half, self.half)
            return remote(self.buf.at[k, rows], self.buf.at[3, rows], self.send.at[k + 1], self.recv.at[k + 1], self.next if k == 1 else self.prev)

        def start(self):
            self.full(1).start()
            self.full(2).start()

        def relay(self, k):
            with scope(f"{self.name}_recv{k}"):
                self.full(k).wait_recv()
                self.part(k).start()

        def far(self):
            with scope(f"{self.name}_far"):
                self.part(1).wait_recv()
                self.part(2).wait_recv()

        def drain(self):
            for k in (1, 2):
                self.full(k).wait_send()
                self.part(k).wait_send()

    for layer in range(layers):
        first, final = layer == 0, layer == layers - 1
        row = slice(layer, layer + 1)
        lay = at[layer]
        tag = f"L{layer}_"
        h1[layer, 0] = norm(resid[...], ln1g[row, :], ln1b[row, :])
        spread1 = Spread(layer, 0, h1)
        spread1.start()

        def q_copy(k, m):
            return remote(qsend.at[k, m], qkv.at[layer, lay.owner(k)], q_sem.at[layer, 0], q_sem.at[layer, 1], lay.in_w(m))

        def put(k, m, part):
            @pl.when(m != lay.mine)
            def _():
                qsend[k, m] = part
                q_copy(k, m).start()

            @pl.when(m == lay.mine)
            def _():
                qkv[layer, lay.owner(k)] = part

        def q_parts(k0, count, start, slots):
            def step(n, _):
                m = (start + n) % col
                part = lax.dot_general(wq[m], h1[layer, k0 : k0 + count].reshape(count * share, width), NT, preferred_element_type=F32).astype(BF16)
                for k in range(count):
                    put(k0 + k, m, part[:, k * share : (k + 1) * share])
                return 0

            with scope(f"{tag}qkv{k0}"):
                lax.fori_loop(0, slots, step, 0)

        job = q_job[layer]
        if first:
            slots = [pos * CORES for pos in job.order()]
            job.other(0)
            job.ready(0)
            q_parts(0, 1, slots[0], CORES)
            spread1.relay(1)
            spread1.relay(2)
            if not final:
                q_job[layer + 1].start()
                ow_job[layer + 1].start()
            q_parts(1, 1, slots[0], CORES)
            q_parts(2, 1, slots[0], CORES)
            ow_job[layer].relay()
            job.relay()
            spread1.far()
            q_parts(3, 1, slots[0], CORES)
            job.other(1)
            job.other(2)
            job.ready(1, 2)
            for n in (1, 2):
                q_parts(0, 2, slots[n], CORES)
                q_parts(2, 2, slots[n], CORES)
            ow_job[layer].last()
            own_out(layer).wait()
            ot_job[layer].start()
            job.last()
            job.other(3)
            job.ready(3)
            q_parts(0, 2, slots[3], CORES)
            q_parts(2, 2, slots[3], CORES)
            u_job[layer].start()
            if not final:
                ow_job[layer + 1].relay()
                q_job[layer + 1].relay()
        else:
            q_parts(0, 1, lay.mine + 1, col)
            spread1.relay(1)
            spread1.relay(2)
            ot_job[layer].relay()
            q_parts(1, 1, lay.mine + 1, col)
            q_parts(2, 1, lay.mine + 1, col)
            spread1.far()
            q_parts(3, 1, lay.mine + 1, col)
            d_job[layer].start()
        moved = qkv.at[layer, pl.ds(0, side * (col - 1))]
        all_qkv = remote(moved, moved, q_sem.at[layer, 0], q_sem.at[layer, 1], me)
        with scope(tag + "qkv_recv"):
            all_qkv.wait_recv()
        with scope(tag + "attend"):
            attend(layer, me, (lay.t * CORES + c) * side + lay.w, qkv, oall, osend, o_sem)
        moved = oall.at[layer, pl.ds(0, tp - 1)]
        all_o = remote(moved, moved, o_sem.at[layer, 0], o_sem.at[layer, 1], me)
        ot, u, d = ot_job[layer], u_job[layer], d_job[layer]
        ot.own()
        u.own()
        if first:
            d.start()
            ot.relay()
            if not final:
                ow_job[layer + 1].last()
                own_out(layer + 1).wait()
                q_job[layer + 1].last()
        for i in range(3):
            ot.other(i)
        ot.last()
        if first:
            if not final:
                u_job[layer + 1].start()
            u.relay()
        else:
            u.last()
            for i in range(4):
                u.other(i)
        ot.other(3)
        ot.ready(0, 1, 2, 3)
        with scope(tag + "o_recv"):
            all_o.wait_recv()
        o_t = oall[layer].reshape(tp * dim, share)

        def out_step(n, _):
            cs = pl.ds(pl.multiple_of(n * tile, tile), tile)
            w = wo[:, :, cs].reshape(tp * dim, tile)
            resid[:, cs] = resid[:, cs] + (lax.dot_general(o_t, w, TN, preferred_element_type=F32) + bo_ref[row, cs])
            return 0

        with scope(tag + "outproj"):
            lax.fori_loop(0, width // tile, out_step, 0)
        h2[layer, 0] = norm(resid[...], ln2g[row, :], ln2b[row, :])
        spread2 = Spread(layer, 1, h2)
        spread2.start()
        all_bias(layer).wait()

        def up(k0, count):
            def up_step(g, _):
                h = h2[layer, k0 : k0 + count].reshape(count * share, width)
                pre = lax.dot_general(h, wu[g], NN, preferred_element_type=F32) + bup[layer, g]
                act = jax.nn.gelu(pre, approximate=True).astype(BF16)
                ubuf[k0 * share : (k0 + count) * share, pl.ds(pl.multiple_of(g * hidden, 128), hidden)] = act
                return 0

            with scope(f"{tag}up{k0}"):
                lax.fori_loop(0, col, up_step, 0)

        pieces = zsend.shape[0]
        piece = width // pieces

        def z_copy(p, k):
            return remote(zsend.at[p, k - 1], zrecv.at[layer, p, k - 1], z_send.at[layer, k - 1, p], z_recv.at[layer, k - 1, p], lay.owner(k))

        def down(k0, count):
            def piece_step(p, _):
                for n in range(piece // tile):
                    cs = pl.ds(pl.multiple_of(p * piece + n * tile, tile), tile)
                    w = wd[:, :, cs].reshape(col * hidden, tile)
                    z = lax.dot_general(ubuf[k0 * share : (k0 + count) * share, :], w, NN, preferred_element_type=F32)
                    for k in range(k0, k0 + count):
                        zk = z[(k - k0) * share : (k - k0 + 1) * share]
                        if k:
                            zsend[p, k - 1, :, n * tile : (n + 1) * tile] = zk.astype(BF16)
                        else:
                            resid[:, cs] = resid[:, cs] + (zk + bd_ref[row, cs])
                for k in range(max(k0, 1), k0 + count):
                    z_copy(p, k).start()
                return 0

            with scope(f"{tag}down{k0}"):
                lax.fori_loop(0, pieces, piece_step, 0)

        if first:
            spread2.relay(1)
            spread2.relay(2)
            d.own()
            d.relay()
            if not final:
                ot_job[layer + 1].start()
                for i in range(4):
                    q_job[layer + 1].other(i)
            for i in range(3):
                u.other(i)
            u.last()
            u.other(3)
            u.ready(0, 1, 2, 3)
            spread2.far()
            up(0, side)
            for i in range(3):
                d.other(i)
            d.last()
            d.other(3)
            d.ready(0, 1, 2, 3)
            down(0, side)
        else:
            u.ready(0, 1, 2, 3)
            up(0, 1)
            spread2.relay(1)
            spread2.relay(2)
            d.own()
            d.relay()
            up(1, 2)
            spread2.far()
            up(3, 1)
            for i in range(3):
                d.other(i)
            d.last()
            d.other(3)
            d.ready(0, 1, 2, 3)
            down(3, 1)
            down(1, 2)
            down(0, 1)
        if not final:
            q_job[layer + 1].own()
            u_job[layer + 1].relay()
            q_job[layer + 1].ready(0, 1, 2, 3)
        with scope(tag + "z_recv"):
            for p in range(pieces):
                cs = slice(p * piece, (p + 1) * piece)
                total = resid[:, cs]
                for k in (1, 2, 3):
                    z_copy(p, k).wait_recv()
                    total = total + zrecv[layer, p, k - 1].astype(F32)
                if final:
                    out_ref[:, cs] = total.astype(BF16)
                else:
                    resid[:, cs] = total
        with scope(tag + "sent"):
            all_qkv.wait_send()
            all_o.wait_send()
            spread1.drain()
            spread2.drain()
            for p in range(pieces):
                for k in (1, 2, 3):
                    z_copy(p, k).wait_send()
    with scope("drain"):
        for layer in range(layers):
            q_job[layer].drain(gq.at[layer, pl.ds(0, 7)])
            u_job[layer].drain(gu.at[layer, pl.ds(0, 7)])
            d_job[layer].drain(gd.at[layer, pl.ds(0, 7)])
            ot_job[layer].drain(go.at[layer, pl.ds(0, 7)])
            ow_job[layer].drain(go.at[layer, 0, pl.ds(0, 3 * dim)])


def attend(layer, me, slot, qkv, oall, osend, o_sem):
    _, tp, three_dim, share = qkv.shape
    dim = three_dim // 3
    per = 4
    block = per * share
    c2 = math.log2(math.e) / math.sqrt(dim)
    rows = lax.broadcasted_iota(jnp.int32, (block, block), 0)
    cols = lax.broadcasted_iota(jnp.int32, (block, block), 1)
    steps = tp // per

    def part(i, which):
        return jnp.concatenate([qkv[layer, i * per + n, which * dim : (which + 1) * dim, :] for n in range(per)], axis=1)

    def q_step(i, _):
        q = part(i, 0).T

        def scores(j):
            return lax.dot_general(q, part(j, 1), NN, preferred_element_type=F32)

        def update(s, j, carry):
            m, l, acc = carry
            m_new = jnp.maximum(m, jnp.max(s, axis=-1, keepdims=True))
            p = jnp.exp2(s * c2 - m_new * c2)
            alpha = jnp.exp2((m - m_new) * c2)
            acc = acc * alpha + lax.dot_general(p.astype(BF16), part(j, 2), NT, preferred_element_type=F32)
            return m_new, l * alpha + jnp.sum(p, axis=-1, keepdims=True), acc

        init = (jnp.full((block, 1), -1e30, F32), jnp.zeros((block, 1), F32), jnp.zeros((block, dim), F32))
        carry = lax.fori_loop(0, i, lambda j, carry: update(scores(j), j, carry), init)
        _, l, acc = update(jnp.where(rows >= cols, scores(i), -1e30), i, carry)
        o_t = (acc / l).T.astype(BF16)
        for n in range(per):
            d = (i * per + n - me + tp) % tp
            piece = o_t[:, n * share : (n + 1) * share]

            @pl.when(d != 0)
            def _():
                osend[d] = piece
                remote(osend.at[d], oall.at[layer, slot], o_sem.at[layer, 0], o_sem.at[layer, 1], i * per + n).start()

            @pl.when(d == 0)
            def _():
                oall[layer, slot] = piece

        return 0

    lax.fori_loop(0, steps, q_step, 0)


def solution(mesh):
    tp = mesh.shape["tp"]
    side = math.isqrt(tp // CORES)
    col = side * CORES
    near = side - 1
    pieces = 4

    def local_forward(x_local, ln1_gain, ln1_bias, ln2_gain, ln2_bias, w_qkv, w_out, b_out, w_up, b_up, w_down, b_down):
        _, share, width = x_local.shape
        layers, _, three, _, dim = w_qkv.shape
        hidden = w_up.shape[2]
        piece = width // pieces
        wq_t = jnp.transpose(w_qkv, (0, 2, 3, 4, 1)).reshape(layers, three * dim, width)
        hbm = lambda *shape: jax.ShapeDtypeStruct(shape, BF16)
        vmem = lambda *shape: pltpu.VMEM(shape, BF16)
        y = pl.pallas_call(
            functools.partial(decoder_kernel, side, layers),
            out_shape=(
                hbm(share, width), hbm(layers, col, three * dim, width), hbm(layers, col, side * dim, width),
                hbm(layers, col, width, hidden), hbm(layers, col, hidden, width),
            ),
            in_specs=[VMEM] * 8 + [HBM] * 4,
            out_specs=(VMEM, HBM, HBM, HBM, HBM),
            scratch_shapes=[
                vmem(col, three * dim, width), vmem(col, side * dim, width), vmem(col, width, hidden), vmem(col, hidden, width),
                vmem(layers, side, share, width), vmem(layers, side, share, width),
                vmem(layers, tp, three * dim, share), vmem(side, col, three * dim, share),
                vmem(layers, tp, dim, share), vmem(tp, dim, share),
                vmem(side * share, col * hidden),
                vmem(pieces, near, share, piece), vmem(layers, pieces, near, share, piece),
                pltpu.VMEM((share, width), F32), pltpu.VMEM((layers, col, 1, hidden), F32),
                DMA((layers, 5, 8)), DMA((layers, 5)), DMA((layers, 2, 4)), DMA((layers, 2, 4)),
                DMA((layers, 2)), DMA((layers, 2)), DMA((layers, near, pieces)), DMA((layers, near, pieces)),
                DMA((layers, 2)), DMA((layers, 5, 8)), DMA((layers,)),
            ],
            compiler_params=pltpu.CompilerParams(collective_id=0, has_side_effects=True, vmem_limit_bytes=63 * 1024 * 1024),
            name="decoder",
        )(x_local[0], ln1_gain, ln1_bias, ln2_gain, ln2_bias, b_out, b_up[:, None], b_down, wq_t, w_out.reshape(layers, dim, width), w_up, w_down)[0]
        return y[None]

    rows_spec = P("dp", "tp", None)
    in_specs = (rows_spec, P(), P(), P(), P(), P(None, None, None, "tp", None), P(None, "tp", None, None), P(), P(None, None, "tp"), P(None, "tp"), P(None, "tp", None), P())
    return jax.shard_map(local_forward, mesh=mesh, in_specs=in_specs, out_specs=rows_spec, check_vma=False)
```

```python
import functools
import math
import jax
import jax.numpy as jnp
from jax import lax
from jax.experimental import pallas as pl
from jax.experimental.pallas import tpu as pltpu
from jax.sharding import PartitionSpec as P

F32 = jnp.float32
BF16 = jnp.bfloat16
CORES = 2
NN = (((1,), (0,)), ((), ()))
NT = (((1,), (1,)), ((), ()))
TN = (((0,), (0,)), ((), ()))
MESH = pl.DeviceIdType.MESH
VMEM = pl.BlockSpec(memory_space=pltpu.VMEM)
HBM = pl.BlockSpec(memory_space=pl.ANY)
DMA = pltpu.SemaphoreType.DMA


def index_of(side, y, x, c):
    return (y * side + x) * CORES + c


def dev(index):
    return {"tp": index}


def remote(src, dst, send_sem, recv_sem, index):
    return pltpu.make_async_remote_copy(src_ref=src, dst_ref=dst, send_sem=send_sem, recv_sem=recv_sem, device_id=dev(index), device_id_type=MESH)


def enter(indices):
    barrier = pltpu.get_barrier_semaphore()
    for index in indices:
        pl.semaphore_signal(barrier, inc=1, device_id=dev(index), device_id_type=MESH)
    pl.semaphore_wait(barrier, len(indices))


def norm(resid, gain, shift):
    row_mean = jnp.mean(resid, axis=-1, keepdims=True)
    centered = resid - row_mean
    variance = jnp.mean(centered * centered, axis=-1, keepdims=True)
    return (centered * lax.rsqrt(variance + 1e-5) * gain + shift).astype(BF16)


scope = jax.named_scope


class Gather:
    def __init__(self, name, ring, src, slot, half, recv, send, partner, dst=None, load_sem=None, number=None):
        self.name = name
        self.prev, self.next, self.back, self.here, self.fwd, self.far = ring
        self.src, self.slot, self.half, self.recv, self.send, self.partner = src, slot, half, recv, send, partner
        self.dst, self.load_sem, self.number = dst, load_sem, number

    def order(self):
        return (self.here, self.back, self.fwd, self.far)

    def start(self):
        dst = self.slot(self.here, 0)
        remote(self.src, dst, self.send, self.recv.at[0], self.next).start()
        remote(self.src, dst, self.send, self.recv.at[1], self.prev).start()
        if self.partner is not None:
            remote(self.src, dst, self.send, self.recv.at[4], self.partner).start()

    def landed(self, ref, n):
        remote(ref, ref, self.send, self.recv.at[n], self.next).wait_recv()

    def load(self, i, other):
        pos = self.order()[i]
        src = self.src if i == 0 and other == 0 else self.slot(pos, other)
        return pltpu.make_async_copy(src, self.dst.at[self.number(pos, other)], self.load_sem.at[2 * i + other])

    def share(self, pos, n):
        ref = self.slot(pos, 0)
        remote(ref, ref, self.send, self.recv.at[n], self.partner).start()

    def relay(self):
        with scope(self.name + "_relay"):
            for n, pos, to in ((0, self.back, self.next), (1, self.fwd, self.prev)):
                self.landed(self.slot(pos, 0), n)
                ref = self.half(pos, n)
                remote(ref, ref, self.send, self.recv.at[2 + n], to).start()
                if self.partner is not None:
                    self.share(pos, 5 + n)
                    self.load(1 + n, 0).start()

    def own(self):
        self.load(0, 0).start()

    def other(self, i):
        with scope(f"{self.name}_other{i}"):
            self.landed(self.slot(self.order()[i], 1), 4 + i)
            self.load(i, 1).start()

    def last(self):
        with scope(self.name + "_last"):
            self.landed(self.half(self.far, 0), 2)
            self.landed(self.half(self.far, 1), 3)
            if self.partner is not None:
                self.share(self.far, 7)
                self.load(3, 0).start()

    def ready(self, *which):
        with scope(self.name + "_ready"):
            for i in which:
                self.load(i, 0).wait()
                self.load(i, 1).wait()

    def drain(self, ref):
        remote(ref, ref, self.send, self.recv.at[0], self.next).wait_send()


class Layer:
    def __init__(self, side, layer, y, x, c):
        self.side, self.swap, self.c = side, layer % 2, c
        self.w, self.t = (x, y) if self.swap else (y, x)
        self.mine = self.w * CORES + c

    def at(self, w, t, c):
        return index_of(self.side, t, w, c) if self.swap else index_of(self.side, w, t, c)

    def in_w(self, m):
        return self.at(m // CORES, self.t, m % CORES)

    def ring(self, along_w):
        side, c = self.side, self.c
        p = self.w if along_w else self.t
        back, fwd, far = (p + side - 1) % side, (p + 1) % side, (p + 2) % side
        at = (lambda q: self.at(q, self.t, c)) if along_w else (lambda q: self.at(self.w, q, c))
        return at(back), at(fwd), back, p, fwd, far

    def owner(self, k):
        return self.at(self.w, (self.t + (0, self.side - 1, 1, 2)[k]) % self.side, self.c)


def decoder_kernel(side, layers, x_ref, ln1g, ln1b, ln2g, ln2b, bo_ref, bu_ref, bd_ref, wq_in, wo_in, wu_in, wd_in,
                   out_ref, gq, go, gu, gd,
                   wq, wo, wu, wd, h1, h2, qkv, qsend, oall, osend, ubuf, zsend, zrecv, resid, bup,
                   g_recv, g_send, h_send, h_recv, q_sem, o_sem, z_send, z_recv, b_sem, l_sem, c_sem):
    me = lax.axis_index("tp")
    y, x, c = me // (side * CORES), (me // CORES) % side, me % CORES
    col = side * CORES
    tp = side * col
    near = side - 1
    share, width = x_ref.shape
    dim = oall.shape[2]
    hidden = wu.shape[2]
    tile = 256
    partner = index_of(side, y, x, 1 - c)
    at = [Layer(side, layer, y, x, c) for layer in range(layers)]

    def number(pos, other):
        return pos * CORES + (c if other == 0 else 1 - c)

    def weights(layer, n, name, src, buf, dst):
        rows = buf.shape[2] // 2
        return Gather(
            f"L{layer}_{name}", at[layer].ring(True), src.at[layer],
            lambda pos, other: buf.at[layer, number(pos, other)],
            lambda pos, k: buf.at[layer, number(pos, 0), pl.ds(k * rows, rows)],
            g_recv.at[layer, n], g_send.at[layer, n], partner, dst, l_sem.at[layer, n], number)

    def out_w(layer):
        here = number(at[layer].t, 0)
        half = dim // 2
        return Gather(
            f"L{layer}_ow", at[layer].ring(True), wo_in.at[layer],
            lambda pos, other: go.at[layer, here, pl.ds(pl.multiple_of(pos * dim, dim), dim)],
            lambda pos, k: go.at[layer, here, pl.ds(pl.multiple_of(pos * dim + k * half, half), half)],
            g_recv.at[layer, 3], g_send.at[layer, 3], None)

    def out_t(layer):
        rows = go.shape[2] // 2
        return Gather(
            f"L{layer}_ot", at[layer].ring(False), go.at[layer, number(at[layer].t, 0)],
            lambda pos, other: go.at[layer, number(pos, other)],
            lambda pos, k: go.at[layer, number(pos, 0), pl.ds(k * rows, rows)],
            g_recv.at[layer, 4], g_send.at[layer, 4], partner, wo, l_sem.at[layer, 4], number)

    q_job = [weights(layer, 0, "q", wq_in, gq, wq) for layer in range(layers)]
    u_job = [weights(layer, 1, "u", wu_in, gu, wu) for layer in range(layers)]
    d_job = [weights(layer, 2, "d", wd_in, gd, wd) for layer in range(layers)]
    ow_job = [out_w(layer) for layer in range(layers)]
    ot_job = [out_t(layer) for layer in range(layers)]

    def own_out(layer):
        return pltpu.make_async_copy(wo_in.at[layer], ow_job[layer].slot(at[layer].w, 0), c_sem.at[layer])

    def all_bias(layer):
        moved = bup.at[layer, pl.ds(0, col - 1)]
        return remote(moved, moved, b_sem.at[layer, 0], b_sem.at[layer, 1], me)

    with scope("enter"):
        enter([(me + d) % tp for d in range(1, tp)])
    ow_job[0].start()
    q_job[0].start()
    for layer in range(layers):
        own_out(layer).start()
        mine = at[layer].mine
        for d in range(1, col):
            row = bu_ref.at[pl.ds(layer, 1)]
            remote(row, bup.at[layer, mine], b_sem.at[layer, 0], b_sem.at[layer, 1], at[layer].in_w((mine + d) % col)).start()
        bup[layer, mine] = bu_ref[layer : layer + 1, :]
    q_job[0].own()
    resid[...] = x_ref[...].astype(F32)

    class Spread:
        def __init__(self, layer, which, buf):
            self.buf, self.name = buf.at[layer], f"L{layer}_h{which}"
            self.send, self.recv = h_send.at[layer, which], h_recv.at[layer, which]
            self.prev, self.next = at[layer].ring(False)[:2]
            self.half = share // 2

        def full(self, k):
            return remote(self.buf.at[0], self.buf.at[k], self.send.at[k - 1], self.recv.at[k - 1], self.next if k == 1 else self.prev)

        def part(self, k):
            rows = pl.ds((k - 1) * self.half, self.half)
            return remote(self.buf.at[k, rows], self.buf.at[3, rows], self.send.at[k + 1], self.recv.at[k + 1], self.next if k == 1 else self.prev)

        def start(self):
            self.full(1).start()
            self.full(2).start()

        def relay(self, k):
            with scope(f"{self.name}_recv{k}"):
                self.full(k).wait_recv()
                self.part(k).start()

        def far(self):
            with scope(f"{self.name}_far"):
                self.part(1).wait_recv()
                self.part(2).wait_recv()

        def drain(self):
            for k in (1, 2):
                self.full(k).wait_send()
                self.part(k).wait_send()

    for layer in range(layers):
        first, final = layer == 0, layer == layers - 1
        row = slice(layer, layer + 1)
        lay = at[layer]
        tag = f"L{layer}_"
        h1[layer, 0] = norm(resid[...], ln1g[row, :], ln1b[row, :])
        spread1 = Spread(layer, 0, h1)
        spread1.start()

        def q_copy(k, m):
            return remote(qsend.at[k, m], qkv.at[layer, lay.owner(k)], q_sem.at[layer, 0], q_sem.at[layer, 1], lay.in_w(m))

        def put(k, m, part):
            @pl.when(m != lay.mine)
            def _():
                qsend[k, m] = part
                q_copy(k, m).start()

            @pl.when(m == lay.mine)
            def _():
                qkv[layer, lay.owner(k)] = part

        def q_parts(k0, count, start, slots):
            def step(n, _):
                m = (start + n) % col
                part = lax.dot_general(wq[m], h1[layer, k0 : k0 + count].reshape(count * share, width), NT, preferred_element_type=F32).astype(BF16)
                for k in range(count):
                    put(k0 + k, m, part[:, k * share : (k + 1) * share])
                return 0

            with scope(f"{tag}qkv{k0}"):
                lax.fori_loop(0, slots, step, 0)

        job = q_job[layer]
        if first:
            slots = [pos * CORES for pos in job.order()]
            job.other(0)
            job.ready(0)
            q_parts(0, 1, slots[0], CORES)
            spread1.relay(1)
            spread1.relay(2)
            if not final:
                q_job[layer + 1].start()
                ow_job[layer + 1].start()
            q_parts(1, 1, slots[0], CORES)
            q_parts(2, 1, slots[0], CORES)
            ow_job[layer].relay()
            job.relay()
            spread1.far()
            q_parts(3, 1, slots[0], CORES)
            job.other(1)
            job.other(2)
            job.ready(1, 2)
            for n in (1, 2):
                q_parts(0, 2, slots[n], CORES)
                q_parts(2, 2, slots[n], CORES)
            ow_job[layer].last()
            own_out(layer).wait()
            ot_job[layer].start()
            job.last()
            job.other(3)
            job.ready(3)
            q_parts(0, 2, slots[3], CORES)
            q_parts(2, 2, slots[3], CORES)
            u_job[layer].start()
        else:
            q_parts(0, 1, lay.mine + 1, col)
            spread1.relay(1)
            spread1.relay(2)
            ot_job[layer].relay()
            q_parts(1, 2, lay.mine + 1, col)
            spread1.far()
            q_parts(3, 1, lay.mine + 1, col)
            d_job[layer].start()
            u_job[layer].own()
            u_job[layer].last()
        moved = qkv.at[layer, pl.ds(0, side * (col - 1))]
        all_qkv = remote(moved, moved, q_sem.at[layer, 0], q_sem.at[layer, 1], me)
        with scope(tag + "qkv_recv"):
            all_qkv.wait_recv()
        def hook_early():
            if not first:
                for i in range(4):
                    u_job[layer].other(i)

        def hook_middle():
            if first:
                ot_job[layer].relay()
                if not final:
                    ow_job[layer + 1].relay()
                    q_job[layer + 1].relay()

        def hook_late():
            if not first:
                d_job[layer].relay()

        hooks = {3: hook_early, 5: hook_middle, 7: hook_late}
        with scope(tag + "attend"):
            attend(layer, me, (lay.t * CORES + c) * side + lay.w, qkv, oall, osend, o_sem, hooks)
        moved = oall.at[layer, pl.ds(0, tp - 1)]
        all_o = remote(moved, moved, o_sem.at[layer, 0], o_sem.at[layer, 1], me)
        ot, u, d = ot_job[layer], u_job[layer], d_job[layer]
        ot.own()
        if first:
            u.own()
            d.start()
            u.relay()
        for i in range(3):
            ot.other(i)
        ot.last()
        ot.other(3)
        ot.ready(0, 1, 2, 3)
        with scope(tag + "o_recv"):
            all_o.wait_recv()
        o_t = oall[layer].reshape(tp * dim, share)

        def out_step(n, _):
            cs = pl.ds(pl.multiple_of(n * tile, tile), tile)
            w = wo[:, :, cs].reshape(tp * dim, tile)
            resid[:, cs] = resid[:, cs] + (lax.dot_general(o_t, w, TN, preferred_element_type=F32) + bo_ref[row, cs])
            return 0

        with scope(tag + "outproj"):
            lax.fori_loop(0, width // tile, out_step, 0)
        h2[layer, 0] = norm(resid[...], ln2g[row, :], ln2b[row, :])
        spread2 = Spread(layer, 1, h2)
        spread2.start()
        all_bias(layer).wait()

        def up(k0, count):
            def up_step(g, _):
                h = h2[layer, k0 : k0 + count].reshape(count * share, width)
                pre = lax.dot_general(h, wu[g], NN, preferred_element_type=F32) + bup[layer, g]
                act = jax.nn.gelu(pre, approximate=True).astype(BF16)
                ubuf[k0 * share : (k0 + count) * share, pl.ds(pl.multiple_of(g * hidden, 128), hidden)] = act
                return 0

            with scope(f"{tag}up{k0}"):
                lax.fori_loop(0, col, up_step, 0)

        pieces = zsend.shape[0]
        piece = width // pieces

        def z_copy(p, k):
            return remote(zsend.at[p, k - 1], zrecv.at[layer, p, k - 1], z_send.at[layer, k - 1, p], z_recv.at[layer, k - 1, p], lay.owner(k))

        def down(k0, count):
            def piece_step(p, _):
                for n in range(piece // tile):
                    cs = pl.ds(pl.multiple_of(p * piece + n * tile, tile), tile)
                    w = wd[:, :, cs].reshape(col * hidden, tile)
                    z = lax.dot_general(ubuf[k0 * share : (k0 + count) * share, :], w, NN, preferred_element_type=F32)
                    for k in range(k0, k0 + count):
                        zk = z[(k - k0) * share : (k - k0 + 1) * share]
                        if k:
                            zsend[p, k - 1, :, n * tile : (n + 1) * tile] = zk.astype(BF16)
                        else:
                            resid[:, cs] = resid[:, cs] + (zk + bd_ref[row, cs])
                for k in range(max(k0, 1), k0 + count):
                    z_copy(p, k).start()
                return 0

            with scope(f"{tag}down{k0}"):
                lax.fori_loop(0, pieces, piece_step, 0)

        if first:
            if not final:
                ow_job[layer + 1].last()
                own_out(layer + 1).wait()
                q_job[layer + 1].last()
            spread2.relay(1)
            spread2.relay(2)
            if not final:
                u_job[layer + 1].start()
            d.own()
            d.relay()
            if not final:
                ot_job[layer + 1].start()
                for i in range(4):
                    q_job[layer + 1].other(i)
            for i in range(3):
                u.other(i)
            u.last()
            u.other(3)
            u.ready(0, 1, 2, 3)
            spread2.far()
            up(0, side)
            for i in range(3):
                d.other(i)
            d.last()
            d.other(3)
            d.ready(0, 1, 2, 3)
            down(0, side)
        else:
            d.own()
            d.last()
            for i in range(4):
                d.other(i)
            u.ready(0, 1, 2, 3)
            up(0, 1)
            spread2.relay(1)
            spread2.relay(2)
            up(1, 2)
            d.ready(0, 1, 2, 3)
            down(1, 2)
            spread2.far()
            up(3, 1)
            down(3, 1)
            down(0, 1)
        if not final:
            q_job[layer + 1].own()
            u_job[layer + 1].relay()
            q_job[layer + 1].ready(0, 1, 2, 3)
        with scope(tag + "z_recv"):
            for p in range(pieces):
                cs = slice(p * piece, (p + 1) * piece)
                total = resid[:, cs]
                for k in (1, 2, 3):
                    z_copy(p, k).wait_recv()
                    total = total + zrecv[layer, p, k - 1].astype(F32)
                if final:
                    out_ref[:, cs] = total.astype(BF16)
                else:
                    resid[:, cs] = total
        with scope(tag + "sent"):
            all_qkv.wait_send()
            all_o.wait_send()
            spread1.drain()
            spread2.drain()
            for p in range(pieces):
                for k in (1, 2, 3):
                    z_copy(p, k).wait_send()
    with scope("drain"):
        for layer in range(layers):
            q_job[layer].drain(gq.at[layer, pl.ds(0, 7)])
            u_job[layer].drain(gu.at[layer, pl.ds(0, 7)])
            d_job[layer].drain(gd.at[layer, pl.ds(0, 7)])
            ot_job[layer].drain(go.at[layer, pl.ds(0, 7)])
            ow_job[layer].drain(go.at[layer, 0, pl.ds(0, 3 * dim)])


def attend(layer, me, slot, qkv, oall, osend, o_sem, hooks):
    _, tp, three_dim, share = qkv.shape
    dim = three_dim // 3
    per = 4
    block = per * share
    c2 = math.log2(math.e) / math.sqrt(dim)
    rows = lax.broadcasted_iota(jnp.int32, (block, block), 0)
    cols = lax.broadcasted_iota(jnp.int32, (block, block), 1)
    steps = tp // per

    def part(i, which):
        return jnp.concatenate([qkv[layer, i * per + n, which * dim : (which + 1) * dim, :] for n in range(per)], axis=1)

    def q_step(i, _):
        for when, hook in hooks.items():
            pl.when(i == when)(hook)
        q = part(i, 0).T

        def scores(j):
            return lax.dot_general(q, part(j, 1), NN, preferred_element_type=F32)

        def update(s, j, carry):
            m, l, acc = carry
            m_new = jnp.maximum(m, jnp.max(s, axis=-1, keepdims=True))
            p = jnp.exp2(s * c2 - m_new * c2)
            alpha = jnp.exp2((m - m_new) * c2)
            acc = acc * alpha + lax.dot_general(p.astype(BF16), part(j, 2), NT, preferred_element_type=F32)
            return m_new, l * alpha + jnp.sum(p, axis=-1, keepdims=True), acc

        init = (jnp.full((block, 1), -1e30, F32), jnp.zeros((block, 1), F32), jnp.zeros((block, dim), F32))
        carry = lax.fori_loop(0, i, lambda j, carry: update(scores(j), j, carry), init)
        _, l, acc = update(jnp.where(rows >= cols, scores(i), -1e30), i, carry)
        o_t = (acc / l).T.astype(BF16)
        for n in range(per):
            d = (i * per + n - me + tp) % tp
            piece = o_t[:, n * share : (n + 1) * share]

            @pl.when(d != 0)
            def _():
                osend[d] = piece
                remote(osend.at[d], oall.at[layer, slot], o_sem.at[layer, 0], o_sem.at[layer, 1], i * per + n).start()

            @pl.when(d == 0)
            def _():
                oall[layer, slot] = piece

        return 0

    lax.fori_loop(0, steps, q_step, 0)


def solution(mesh):
    tp = mesh.shape["tp"]
    side = math.isqrt(tp // CORES)
    col = side * CORES
    near = side - 1
    pieces = 4

    def local_forward(x_local, ln1_gain, ln1_bias, ln2_gain, ln2_bias, w_qkv, w_out, b_out, w_up, b_up, w_down, b_down):
        _, share, width = x_local.shape
        layers, _, three, _, dim = w_qkv.shape
        hidden = w_up.shape[2]
        piece = width // pieces
        wq_t = jnp.transpose(w_qkv, (0, 2, 3, 4, 1)).reshape(layers, three * dim, width)
        hbm = lambda *shape: jax.ShapeDtypeStruct(shape, BF16)
        vmem = lambda *shape: pltpu.VMEM(shape, BF16)
        y = pl.pallas_call(
            functools.partial(decoder_kernel, side, layers),
            out_shape=(
                hbm(share, width), hbm(layers, col, three * dim, width), hbm(layers, col, side * dim, width),
                hbm(layers, col, width, hidden), hbm(layers, col, hidden, width),
            ),
            in_specs=[VMEM] * 8 + [HBM] * 4,
            out_specs=(VMEM, HBM, HBM, HBM, HBM),
            scratch_shapes=[
                vmem(col, three * dim, width), vmem(col, side * dim, width), vmem(col, width, hidden), vmem(col, hidden, width),
                vmem(layers, side, share, width), vmem(layers, side, share, width),
                vmem(layers, tp, three * dim, share), vmem(side, col, three * dim, share),
                vmem(layers, tp, dim, share), vmem(tp, dim, share),
                vmem(side * share, col * hidden),
                vmem(pieces, near, share, piece), vmem(layers, pieces, near, share, piece),
                pltpu.VMEM((share, width), F32), pltpu.VMEM((layers, col, 1, hidden), F32),
                DMA((layers, 5, 8)), DMA((layers, 5)), DMA((layers, 2, 4)), DMA((layers, 2, 4)),
                DMA((layers, 2)), DMA((layers, 2)), DMA((layers, near, pieces)), DMA((layers, near, pieces)),
                DMA((layers, 2)), DMA((layers, 5, 8)), DMA((layers,)),
            ],
            compiler_params=pltpu.CompilerParams(collective_id=0, has_side_effects=True, vmem_limit_bytes=63 * 1024 * 1024),
            name="decoder",
        )(x_local[0], ln1_gain, ln1_bias, ln2_gain, ln2_bias, b_out, b_up, b_down, wq_t, w_out.reshape(layers, dim, width), w_up, w_down)[0]
        return y[None]

    rows_spec = P("dp", "tp", None)
    in_specs = (rows_spec, P(), P(), P(), P(), P(None, None, None, "tp", None), P(None, "tp", None, None), P(), P(None, None, "tp"), P(None, "tp"), P(None, "tp", None), P())
    return jax.shard_map(local_forward, mesh=mesh, in_specs=in_specs, out_specs=rows_spec, check_vma=False)
```

```python
import functools
import math
import jax
import jax.numpy as jnp
from jax import lax
from jax.experimental import pallas as pl
from jax.experimental.pallas import tpu as pltpu
from jax.sharding import PartitionSpec as P

F32 = jnp.float32
BF16 = jnp.bfloat16
CORES = 2
NN = (((1,), (0,)), ((), ()))
NT = (((1,), (1,)), ((), ()))
TN = (((0,), (0,)), ((), ()))
MESH = pl.DeviceIdType.MESH
VMEM = pl.BlockSpec(memory_space=pltpu.VMEM)
HBM = pl.BlockSpec(memory_space=pl.ANY)
DMA = pltpu.SemaphoreType.DMA


def index_of(side, y, x, c):
    return (y * side + x) * CORES + c


def dev(index):
    return {"tp": index}


def remote(src, dst, send_sem, recv_sem, index):
    return pltpu.make_async_remote_copy(src_ref=src, dst_ref=dst, send_sem=send_sem, recv_sem=recv_sem, device_id=dev(index), device_id_type=MESH)


def enter(indices):
    barrier = pltpu.get_barrier_semaphore()
    for index in indices:
        pl.semaphore_signal(barrier, inc=1, device_id=dev(index), device_id_type=MESH)
    pl.semaphore_wait(barrier, len(indices))


def norm(resid, gain, shift):
    row_mean = jnp.mean(resid, axis=-1, keepdims=True)
    centered = resid - row_mean
    variance = jnp.mean(centered * centered, axis=-1, keepdims=True)
    return (centered * lax.rsqrt(variance + 1e-5) * gain + shift).astype(BF16)


scope = jax.named_scope


class Gather:
    def __init__(self, name, ring, src, slot, half, recv, send, partner, dst=None, load_sem=None, number=None):
        self.name = name
        self.prev, self.next, self.back, self.here, self.fwd, self.far = ring
        self.src, self.slot, self.half, self.recv, self.send, self.partner = src, slot, half, recv, send, partner
        self.dst, self.load_sem, self.number = dst, load_sem, number

    def order(self):
        return (self.here, self.back, self.fwd, self.far)

    def start(self):
        dst = self.slot(self.here, 0)
        remote(self.src, dst, self.send, self.recv.at[0], self.next).start()
        remote(self.src, dst, self.send, self.recv.at[1], self.prev).start()
        if self.partner is not None:
            remote(self.src, dst, self.send, self.recv.at[4], self.partner).start()

    def landed(self, ref, n):
        remote(ref, ref, self.send, self.recv.at[n], self.next).wait_recv()

    def load(self, i, other):
        pos = self.order()[i]
        src = self.src if i == 0 and other == 0 else self.slot(pos, other)
        return pltpu.make_async_copy(src, self.dst.at[self.number(pos, other)], self.load_sem.at[2 * i + other])

    def share(self, pos, n):
        ref = self.slot(pos, 0)
        remote(ref, ref, self.send, self.recv.at[n], self.partner).start()

    def relay(self):
        with scope(self.name + "_relay"):
            for n, pos, to in ((0, self.back, self.next), (1, self.fwd, self.prev)):
                self.landed(self.slot(pos, 0), n)
                ref = self.half(pos, n)
                remote(ref, ref, self.send, self.recv.at[2 + n], to).start()
                if self.partner is not None:
                    self.share(pos, 5 + n)
                    self.load(1 + n, 0).start()

    def own(self):
        self.load(0, 0).start()

    def other(self, i):
        with scope(f"{self.name}_other{i}"):
            self.landed(self.slot(self.order()[i], 1), 4 + i)
            self.load(i, 1).start()

    def last(self):
        with scope(self.name + "_last"):
            self.landed(self.half(self.far, 0), 2)
            self.landed(self.half(self.far, 1), 3)
            if self.partner is not None:
                self.share(self.far, 7)
                self.load(3, 0).start()

    def ready(self, *which):
        with scope(self.name + "_ready"):
            for i in which:
                self.load(i, 0).wait()
                self.load(i, 1).wait()

    def drain(self, ref):
        remote(ref, ref, self.send, self.recv.at[0], self.next).wait_send()


class Layer:
    def __init__(self, side, layer, y, x, c):
        self.side, self.swap, self.c = side, layer % 2, c
        self.w, self.t = (x, y) if self.swap else (y, x)
        self.mine = self.w * CORES + c

    def at(self, w, t, c):
        return index_of(self.side, t, w, c) if self.swap else index_of(self.side, w, t, c)

    def in_w(self, m):
        return self.at(m // CORES, self.t, m % CORES)

    def ring(self, along_w):
        side, c = self.side, self.c
        p = self.w if along_w else self.t
        back, fwd, far = (p + side - 1) % side, (p + 1) % side, (p + 2) % side
        at = (lambda q: self.at(q, self.t, c)) if along_w else (lambda q: self.at(self.w, q, c))
        return at(back), at(fwd), back, p, fwd, far

    def owner(self, k):
        return self.at(self.w, (self.t + (0, self.side - 1, 1, 2)[k]) % self.side, self.c)


def decoder_kernel(side, layers, x_ref, ln1g, ln1b, ln2g, ln2b, bo_ref, bu_ref, bd_ref, wq_in, wo_in, wu_in, wd_in,
                   out_ref, gq, go, gu, gd,
                   wq, wo, wu, wd, h1, h2, qkv, qsend, oall, osend, ubuf, zsend, zrecv, resid, bup,
                   g_recv, g_send, h_send, h_recv, q_sem, o_sem, z_send, z_recv, b_sem, l_sem, c_sem):
    me = lax.axis_index("tp")
    y, x, c = me // (side * CORES), (me // CORES) % side, me % CORES
    col = side * CORES
    tp = side * col
    near = side - 1
    share, width = x_ref.shape
    dim = oall.shape[2]
    hidden = wu.shape[2]
    tile = 256
    partner = index_of(side, y, x, 1 - c)
    at = [Layer(side, layer, y, x, c) for layer in range(layers)]

    def number(pos, other):
        return pos * CORES + (c if other == 0 else 1 - c)

    def weights(layer, n, name, src, buf, dst):
        rows = buf.shape[2] // 2
        return Gather(
            f"L{layer}_{name}", at[layer].ring(True), src.at[layer],
            lambda pos, other: buf.at[layer, number(pos, other)],
            lambda pos, k: buf.at[layer, number(pos, 0), pl.ds(k * rows, rows)],
            g_recv.at[layer, n], g_send.at[layer, n], partner, dst, l_sem.at[layer, n], number)

    def out_w(layer):
        here = number(at[layer].t, 0)
        half = dim // 2
        return Gather(
            f"L{layer}_ow", at[layer].ring(True), wo_in.at[layer],
            lambda pos, other: go.at[layer, here, pl.ds(pl.multiple_of(pos * dim, dim), dim)],
            lambda pos, k: go.at[layer, here, pl.ds(pl.multiple_of(pos * dim + k * half, half), half)],
            g_recv.at[layer, 3], g_send.at[layer, 3], None)

    def out_t(layer):
        rows = go.shape[2] // 2
        return Gather(
            f"L{layer}_ot", at[layer].ring(False), go.at[layer, number(at[layer].t, 0)],
            lambda pos, other: go.at[layer, number(pos, other)],
            lambda pos, k: go.at[layer, number(pos, 0), pl.ds(k * rows, rows)],
            g_recv.at[layer, 4], g_send.at[layer, 4], partner, wo, l_sem.at[layer, 4], number)

    q_job = [weights(layer, 0, "q", wq_in, gq, wq) for layer in range(layers)]
    u_job = [weights(layer, 1, "u", wu_in, gu, wu) for layer in range(layers)]
    d_job = [weights(layer, 2, "d", wd_in, gd, wd) for layer in range(layers)]
    ow_job = [out_w(layer) for layer in range(layers)]
    ot_job = [out_t(layer) for layer in range(layers)]

    def own_out(layer):
        return pltpu.make_async_copy(wo_in.at[layer], ow_job[layer].slot(at[layer].w, 0), c_sem.at[layer])

    def all_bias(layer):
        moved = bup.at[layer, pl.ds(0, col - 1)]
        return remote(moved, moved, b_sem.at[layer, 0], b_sem.at[layer, 1], me)

    with scope("enter"):
        enter([(me + d) % tp for d in range(1, tp)])
    ow_job[0].start()
    q_job[0].start()
    for layer in range(layers):
        own_out(layer).start()
        mine = at[layer].mine
        for d in range(1, col):
            row = bu_ref.at[pl.ds(layer, 1)]
            remote(row, bup.at[layer, mine], b_sem.at[layer, 0], b_sem.at[layer, 1], at[layer].in_w((mine + d) % col)).start()
        bup[layer, mine] = bu_ref[layer : layer + 1, :]
    q_job[0].own()
    resid[...] = x_ref[...].astype(F32)

    class Spread:
        def __init__(self, layer, which, buf):
            self.buf, self.name = buf.at[layer], f"L{layer}_h{which}"
            self.send, self.recv = h_send.at[layer, which], h_recv.at[layer, which]
            self.prev, self.next = at[layer].ring(False)[:2]
            self.half = share // 2

        def full(self, k):
            return remote(self.buf.at[0], self.buf.at[k], self.send.at[k - 1], self.recv.at[k - 1], self.next if k == 1 else self.prev)

        def part(self, k):
            rows = pl.ds((k - 1) * self.half, self.half)
            return remote(self.buf.at[k, rows], self.buf.at[3, rows], self.send.at[k + 1], self.recv.at[k + 1], self.next if k == 1 else self.prev)

        def start(self):
            self.full(1).start()
            self.full(2).start()

        def relay(self, k):
            with scope(f"{self.name}_recv{k}"):
                self.full(k).wait_recv()
                self.part(k).start()

        def far(self):
            with scope(f"{self.name}_far"):
                self.part(1).wait_recv()
                self.part(2).wait_recv()

        def drain(self):
            for k in (1, 2):
                self.full(k).wait_send()
                self.part(k).wait_send()

    for layer in range(layers):
        first, final = layer == 0, layer == layers - 1
        row = slice(layer, layer + 1)
        lay = at[layer]
        tag = f"L{layer}_"
        h1[layer, 0] = norm(resid[...], ln1g[row, :], ln1b[row, :])
        spread1 = Spread(layer, 0, h1)
        spread1.start()

        def q_copy(k, m):
            return remote(qsend.at[k, m], qkv.at[layer, lay.owner(k)], q_sem.at[layer, 0], q_sem.at[layer, 1], lay.in_w(m))

        def put(k, m, part):
            @pl.when(m != lay.mine)
            def _():
                qsend[k, m] = part
                q_copy(k, m).start()

            @pl.when(m == lay.mine)
            def _():
                qkv[layer, lay.owner(k)] = part

        def q_parts(k0, count, start, slots):
            def step(n, _):
                m = (start + n) % col
                part = lax.dot_general(wq[m], h1[layer, k0 : k0 + count].reshape(count * share, width), NT, preferred_element_type=F32).astype(BF16)
                for k in range(count):
                    put(k0 + k, m, part[:, k * share : (k + 1) * share])
                return 0

            with scope(f"{tag}qkv{k0}"):
                lax.fori_loop(0, slots, step, 0)

        job = q_job[layer]
        if first:
            slots = [pos * CORES for pos in job.order()]
            job.other(0)
            job.ready(0)
            q_parts(0, 1, slots[0], CORES)
            spread1.relay(1)
            spread1.relay(2)
            if not final:
                q_job[layer + 1].start()
                ow_job[layer + 1].start()
            q_parts(1, 1, slots[0], CORES)
            q_parts(2, 1, slots[0], CORES)
            ow_job[layer].relay()
            job.relay()
            spread1.far()
            q_parts(3, 1, slots[0], CORES)
            job.other(1)
            job.other(2)
            job.ready(1, 2)
            for n in (1, 2):
                q_parts(0, 2, slots[n], CORES)
                q_parts(2, 2, slots[n], CORES)
            ow_job[layer].last()
            own_out(layer).wait()
            ot_job[layer].start()
            job.last()
            job.other(3)
            job.ready(3)
            q_parts(0, 2, slots[3], CORES)
            q_parts(2, 2, slots[3], CORES)
            u_job[layer].start()
        else:
            q_parts(0, 1, lay.mine + 1, col)
            spread1.relay(1)
            spread1.relay(2)
            ot_job[layer].relay()
            q_parts(1, 2, lay.mine + 1, col)
            spread1.far()
            q_parts(3, 1, lay.mine + 1, col)
            d_job[layer].start()
            u_job[layer].own()
            u_job[layer].last()
        moved = qkv.at[layer, pl.ds(0, side * (col - 1))]
        all_qkv = remote(moved, moved, q_sem.at[layer, 0], q_sem.at[layer, 1], me)
        with scope(tag + "qkv_recv"):
            all_qkv.wait_recv()
        def hook_early():
            if not first:
                for i in range(4):
                    u_job[layer].other(i)

        def hook_middle():
            if first:
                ot_job[layer].relay()
                if not final:
                    ow_job[layer + 1].relay()
                    q_job[layer + 1].relay()

        def hook_late():
            if first:
                u_job[layer].relay()

        hooks = {3: hook_early, 5: hook_middle, 7: hook_late}
        with scope(tag + "attend"):
            attend(layer, me, (lay.t * CORES + c) * side + lay.w, qkv, oall, osend, o_sem, hooks)
        moved = oall.at[layer, pl.ds(0, tp - 1)]
        all_o = remote(moved, moved, o_sem.at[layer, 0], o_sem.at[layer, 1], me)
        ot, u, d = ot_job[layer], u_job[layer], d_job[layer]
        ot.own()
        for i in range(3):
            ot.other(i)
        ot.last()
        ot.other(3)
        ot.ready(0, 1, 2, 3)
        if first:
            d.start()
        with scope(tag + "o_recv"):
            all_o.wait_recv()
        if not first:
            d.relay()
        o_t = oall[layer].reshape(tp * dim, share)

        def out_step(n, _):
            cs = pl.ds(pl.multiple_of(n * tile, tile), tile)
            w = wo[:, :, cs].reshape(tp * dim, tile)
            resid[:, cs] = resid[:, cs] + (lax.dot_general(o_t, w, TN, preferred_element_type=F32) + bo_ref[row, cs])
            return 0

        with scope(tag + "outproj"):
            lax.fori_loop(0, width // tile, out_step, 0)
        h2[layer, 0] = norm(resid[...], ln2g[row, :], ln2b[row, :])
        spread2 = Spread(layer, 1, h2)
        spread2.start()
        all_bias(layer).wait()

        def up(k0, count):
            def up_step(g, _):
                h = h2[layer, k0 : k0 + count].reshape(count * share, width)
                pre = lax.dot_general(h, wu[g], NN, preferred_element_type=F32) + bup[layer, g]
                act = jax.nn.gelu(pre, approximate=True).astype(BF16)
                ubuf[k0 * share : (k0 + count) * share, pl.ds(pl.multiple_of(g * hidden, 128), hidden)] = act
                return 0

            with scope(f"{tag}up{k0}"):
                lax.fori_loop(0, col, up_step, 0)

        pieces = zsend.shape[0]
        piece = width // pieces

        def z_copy(p, k):
            return remote(zsend.at[p, k - 1], zrecv.at[layer, p, k - 1], z_send.at[layer, k - 1, p], z_recv.at[layer, k - 1, p], lay.owner(k))

        def down(k0, count):
            def piece_step(p, _):
                for n in range(piece // tile):
                    cs = pl.ds(pl.multiple_of(p * piece + n * tile, tile), tile)
                    w = wd[:, :, cs].reshape(col * hidden, tile)
                    z = lax.dot_general(ubuf[k0 * share : (k0 + count) * share, :], w, NN, preferred_element_type=F32)
                    for k in range(k0, k0 + count):
                        zk = z[(k - k0) * share : (k - k0 + 1) * share]
                        if k:
                            zsend[p, k - 1, :, n * tile : (n + 1) * tile] = zk.astype(BF16)
                        else:
                            resid[:, cs] = resid[:, cs] + (zk + bd_ref[row, cs])
                for k in range(max(k0, 1), k0 + count):
                    z_copy(p, k).start()
                return 0

            with scope(f"{tag}down{k0}"):
                lax.fori_loop(0, pieces, piece_step, 0)

        if first:
            if not final:
                ow_job[layer + 1].last()
                own_out(layer + 1).wait()
                q_job[layer + 1].last()
            spread2.relay(1)
            spread2.relay(2)
            if not final:
                u_job[layer + 1].start()
            u.own()
            d.own()
            d.relay()
            if not final:
                ot_job[layer + 1].start()
                for i in range(4):
                    q_job[layer + 1].other(i)
            for i in range(3):
                u.other(i)
            u.last()
            u.other(3)
            u.ready(0, 1, 2, 3)
            spread2.far()
            up(0, side)
            for i in range(3):
                d.other(i)
            d.last()
            d.other(3)
            d.ready(0, 1, 2, 3)
            down(0, side)
        else:
            d.own()
            u.ready(0, 1, 2, 3)
            up(0, 1)
            spread2.relay(1)
            spread2.relay(2)
            d.last()
            up(1, 2)
            for i in range(4):
                d.other(i)
            d.ready(0, 1, 2, 3)
            down(1, 2)
            spread2.far()
            up(3, 1)
            down(3, 1)
            down(0, 1)
        if not final:
            q_job[layer + 1].own()
            q_job[layer + 1].ready(0, 1, 2, 3)
        with scope(tag + "z_recv"):
            for p in range(pieces):
                cs = slice(p * piece, (p + 1) * piece)
                total = resid[:, cs]
                for k in (1, 2, 3):
                    z_copy(p, k).wait_recv()
                    total = total + zrecv[layer, p, k - 1].astype(F32)
                if final:
                    out_ref[:, cs] = total.astype(BF16)
                else:
                    resid[:, cs] = total
        if not final:
            u_job[layer + 1].relay()
        with scope(tag + "sent"):
            all_qkv.wait_send()
            all_o.wait_send()
            spread1.drain()
            spread2.drain()
            for p in range(pieces):
                for k in (1, 2, 3):
                    z_copy(p, k).wait_send()
    with scope("drain"):
        for layer in range(layers):
            q_job[layer].drain(gq.at[layer, pl.ds(0, 7)])
            u_job[layer].drain(gu.at[layer, pl.ds(0, 7)])
            d_job[layer].drain(gd.at[layer, pl.ds(0, 7)])
            ot_job[layer].drain(go.at[layer, pl.ds(0, 7)])
            ow_job[layer].drain(go.at[layer, 0, pl.ds(0, 3 * dim)])


def attend(layer, me, slot, qkv, oall, osend, o_sem, hooks):
    _, tp, three_dim, share = qkv.shape
    dim = three_dim // 3
    per = 4
    block = per * share
    c2 = math.log2(math.e) / math.sqrt(dim)
    steps = tp // per

    def part(i, count, which):
        return jnp.concatenate([qkv[layer, i * per + n, which * dim : (which + 1) * dim, :] for n in range(count * per)], axis=1)

    def q_step(i, _):
        for when, hook in hooks.items():
            pl.when(i == when)(hook)
        q = part(i, 1, 0).T

        def update(j, count, carry, masked):
            m, l, acc = carry
            s = lax.dot_general(q, part(j, count, 1), NN, preferred_element_type=F32)
            if masked:
                rows = lax.broadcasted_iota(jnp.int32, (block, count * block), 0)
                cols = lax.broadcasted_iota(jnp.int32, (block, count * block), 1)
                s = jnp.where(rows + (count - 1) * block >= cols, s, -1e30)
            m_new = jnp.maximum(m, jnp.max(s, axis=-1, keepdims=True))
            p = jnp.exp2(s * c2 - m_new * c2)
            alpha = jnp.exp2((m - m_new) * c2)
            acc = acc * alpha + lax.dot_general(p.astype(BF16), part(j, count, 2), NT, preferred_element_type=F32)
            return m_new, l * alpha + jnp.sum(p, axis=-1, keepdims=True), acc

        init = (jnp.full((block, 1), -1e30, F32), jnp.zeros((block, 1), F32), jnp.zeros((block, dim), F32))
        carry = lax.fori_loop(0, i // 2, lambda j, carry: update(2 * j, 2, carry, False), init)
        _, l, acc = lax.cond(i % 2 == 1, lambda carry: update(i - 1, 2, carry, True), lambda carry: update(i, 1, carry, True), carry)
        o_t = (acc / l).T.astype(BF16)
        for n in range(per):
            d = (i * per + n - me + tp) % tp
            piece = o_t[:, n * share : (n + 1) * share]

            @pl.when(d != 0)
            def _():
                osend[d] = piece
                remote(osend.at[d], oall.at[layer, slot], o_sem.at[layer, 0], o_sem.at[layer, 1], i * per + n).start()

            @pl.when(d == 0)
            def _():
                oall[layer, slot] = piece

        return 0

    lax.fori_loop(0, steps, q_step, 0)


def solution(mesh):
    tp = mesh.shape["tp"]
    side = math.isqrt(tp // CORES)
    col = side * CORES
    near = side - 1
    pieces = 4

    def local_forward(x_local, ln1_gain, ln1_bias, ln2_gain, ln2_bias, w_qkv, w_out, b_out, w_up, b_up, w_down, b_down):
        _, share, width = x_local.shape
        layers, _, three, _, dim = w_qkv.shape
        hidden = w_up.shape[2]
        piece = width // pieces
        wq_t = jnp.transpose(w_qkv, (0, 2, 3, 4, 1)).reshape(layers, three * dim, width)
        hbm = lambda *shape: jax.ShapeDtypeStruct(shape, BF16)
        vmem = lambda *shape: pltpu.VMEM(shape, BF16)
        y = pl.pallas_call(
            functools.partial(decoder_kernel, side, layers),
            out_shape=(
                hbm(share, width), hbm(layers, col, three * dim, width), hbm(layers, col, side * dim, width),
                hbm(layers, col, width, hidden), hbm(layers, col, hidden, width),
            ),
            in_specs=[VMEM] * 8 + [HBM] * 4,
            out_specs=(VMEM, HBM, HBM, HBM, HBM),
            scratch_shapes=[
                vmem(col, three * dim, width), vmem(col, side * dim, width), vmem(col, width, hidden), vmem(col, hidden, width),
                vmem(layers, side, share, width), vmem(layers, side, share, width),
                vmem(layers, tp, three * dim, share), vmem(side, col, three * dim, share),
                vmem(layers, tp, dim, share), vmem(tp, dim, share),
                vmem(side * share, col * hidden),
                vmem(pieces, near, share, piece), vmem(layers, pieces, near, share, piece),
                pltpu.VMEM((share, width), F32), pltpu.VMEM((layers, col, 1, hidden), F32),
                DMA((layers, 5, 8)), DMA((layers, 5)), DMA((layers, 2, 4)), DMA((layers, 2, 4)),
                DMA((layers, 2)), DMA((layers, 2)), DMA((layers, near, pieces)), DMA((layers, near, pieces)),
                DMA((layers, 2)), DMA((layers, 5, 8)), DMA((layers,)),
            ],
            compiler_params=pltpu.CompilerParams(collective_id=0, has_side_effects=True, vmem_limit_bytes=63 * 1024 * 1024),
            name="decoder",
        )(x_local[0], ln1_gain, ln1_bias, ln2_gain, ln2_bias, b_out, b_up, b_down, wq_t, w_out.reshape(layers, dim, width), w_up, w_down)[0]
        return y[None]

    rows_spec = P("dp", "tp", None)
    in_specs = (rows_spec, P(), P(), P(), P(), P(None, None, None, "tp", None), P(None, "tp", None, None), P(), P(None, None, "tp"), P(None, "tp"), P(None, "tp", None), P())
    return jax.shard_map(local_forward, mesh=mesh, in_specs=in_specs, out_specs=rows_spec, check_vma=False)
```

```python
import functools
import math
import jax
import jax.numpy as jnp
from jax import lax
from jax.experimental import pallas as pl
from jax.experimental.pallas import tpu as pltpu
from jax.sharding import PartitionSpec as P

F32 = jnp.float32
BF16 = jnp.bfloat16
CORES = 2
NN = (((1,), (0,)), ((), ()))
NT = (((1,), (1,)), ((), ()))
TN = (((0,), (0,)), ((), ()))
MESH = pl.DeviceIdType.MESH
VMEM = pl.BlockSpec(memory_space=pltpu.VMEM)
HBM = pl.BlockSpec(memory_space=pl.ANY)
DMA = pltpu.SemaphoreType.DMA


def index_of(side, y, x, c):
    return (y * side + x) * CORES + c


def dev(index):
    return {"tp": index}


def remote(src, dst, send_sem, recv_sem, index):
    return pltpu.make_async_remote_copy(src_ref=src, dst_ref=dst, send_sem=send_sem, recv_sem=recv_sem, device_id=dev(index), device_id_type=MESH)


def enter(indices):
    barrier = pltpu.get_barrier_semaphore()
    for index in indices:
        pl.semaphore_signal(barrier, inc=1, device_id=dev(index), device_id_type=MESH)
    pl.semaphore_wait(barrier, len(indices))


def norm(resid, gain, shift):
    row_mean = jnp.mean(resid, axis=-1, keepdims=True)
    centered = resid - row_mean
    variance = jnp.mean(centered * centered, axis=-1, keepdims=True)
    return (centered * lax.rsqrt(variance + 1e-5) * gain + shift).astype(BF16)


scope = jax.named_scope


class Gather:
    def __init__(self, name, ring, src, slot, half, recv, send, partner, dst=None, load_sem=None, number=None):
        self.name = name
        self.prev, self.next, self.back, self.here, self.fwd, self.far = ring
        self.src, self.slot, self.half, self.recv, self.send, self.partner = src, slot, half, recv, send, partner
        self.dst, self.load_sem, self.number = dst, load_sem, number

    def order(self):
        return (self.here, self.back, self.fwd, self.far)

    def start(self):
        dst = self.slot(self.here, 0)
        remote(self.src, dst, self.send, self.recv.at[0], self.next).start()
        remote(self.src, dst, self.send, self.recv.at[1], self.prev).start()
        if self.partner is not None:
            remote(self.src, dst, self.send, self.recv.at[4], self.partner).start()

    def landed(self, ref, n):
        remote(ref, ref, self.send, self.recv.at[n], self.next).wait_recv()

    def load(self, i, other):
        pos = self.order()[i]
        src = self.src if i == 0 and other == 0 else self.slot(pos, other)
        return pltpu.make_async_copy(src, self.dst.at[self.number(pos, other)], self.load_sem.at[2 * i + other])

    def share(self, pos, n):
        ref = self.slot(pos, 0)
        remote(ref, ref, self.send, self.recv.at[n], self.partner).start()

    def relay(self):
        with scope(self.name + "_relay"):
            for n, pos, to in ((0, self.back, self.next), (1, self.fwd, self.prev)):
                self.landed(self.slot(pos, 0), n)
                ref = self.half(pos, n)
                remote(ref, ref, self.send, self.recv.at[2 + n], to).start()
                if self.partner is not None:
                    self.share(pos, 5 + n)
                    self.load(1 + n, 0).start()

    def own(self):
        self.load(0, 0).start()

    def other(self, i):
        with scope(f"{self.name}_other{i}"):
            self.landed(self.slot(self.order()[i], 1), 4 + i)
            self.load(i, 1).start()

    def last(self):
        with scope(self.name + "_last"):
            self.landed(self.half(self.far, 0), 2)
            self.landed(self.half(self.far, 1), 3)
            if self.partner is not None:
                self.share(self.far, 7)
                self.load(3, 0).start()

    def ready(self, *which):
        with scope(self.name + "_ready"):
            for i in which:
                self.load(i, 0).wait()
                self.load(i, 1).wait()

    def drain(self, ref):
        remote(ref, ref, self.send, self.recv.at[0], self.next).wait_send()


class Layer:
    def __init__(self, side, layer, y, x, c):
        self.side, self.swap, self.c = side, layer % 2, c
        self.w, self.t = (x, y) if self.swap else (y, x)
        self.mine = self.w * CORES + c

    def at(self, w, t, c):
        return index_of(self.side, t, w, c) if self.swap else index_of(self.side, w, t, c)

    def in_w(self, m):
        return self.at(m // CORES, self.t, m % CORES)

    def ring(self, along_w):
        side, c = self.side, self.c
        p = self.w if along_w else self.t
        back, fwd, far = (p + side - 1) % side, (p + 1) % side, (p + 2) % side
        at = (lambda q: self.at(q, self.t, c)) if along_w else (lambda q: self.at(self.w, q, c))
        return at(back), at(fwd), back, p, fwd, far

    def owner(self, k):
        return self.at(self.w, (self.t + (0, self.side - 1, 1, 2)[k]) % self.side, self.c)


def decoder_kernel(side, layers, x_ref, ln1g, ln1b, ln2g, ln2b, bo_ref, bu_ref, bd_ref, wq_in, wo_in, wu_in, wd_in,
                   out_ref, gq, go, gu, gd,
                   wq, wo, wu, wd, h1, h2, qkv, qsend, oall, osend, ubuf, zsend, zrecv, resid, bup,
                   g_recv, g_send, h_send, h_recv, q_sem, o_sem, z_send, z_recv, b_sem, l_sem, c_sem):
    me = lax.axis_index("tp")
    y, x, c = me // (side * CORES), (me // CORES) % side, me % CORES
    col = side * CORES
    tp = side * col
    near = side - 1
    share, width = x_ref.shape
    dim = oall.shape[2]
    hidden = wu.shape[2]
    tile = 256
    partner = index_of(side, y, x, 1 - c)
    at = [Layer(side, layer, y, x, c) for layer in range(layers)]

    def number(pos, other):
        return pos * CORES + (c if other == 0 else 1 - c)

    def weights(layer, n, name, src, buf, dst):
        rows = buf.shape[2] // 2
        return Gather(
            f"L{layer}_{name}", at[layer].ring(True), src.at[layer],
            lambda pos, other: buf.at[layer, number(pos, other)],
            lambda pos, k: buf.at[layer, number(pos, 0), pl.ds(k * rows, rows)],
            g_recv.at[layer, n], g_send.at[layer, n], partner, dst, l_sem.at[layer, n], number)

    def down_half(layer, h):
        rows, cols = hidden // 2, width // 2
        n = (2, 5)[h]
        return Gather(
            f"L{layer}_d{h}", at[layer].ring(True), wd_in.at[layer, :, pl.ds(h * cols, cols)],
            lambda pos, other: gd.at[layer, h, number(pos, other)],
            lambda pos, k: gd.at[layer, h, number(pos, 0), pl.ds(k * rows, rows)],
            g_recv.at[layer, n], g_send.at[layer, n], partner, wd.at[h], l_sem.at[layer, n], number)

    def out_w(layer):
        here = number(at[layer].t, 0)
        half = dim // 2
        return Gather(
            f"L{layer}_ow", at[layer].ring(True), wo_in.at[layer],
            lambda pos, other: go.at[layer, here, pl.ds(pl.multiple_of(pos * dim, dim), dim)],
            lambda pos, k: go.at[layer, here, pl.ds(pl.multiple_of(pos * dim + k * half, half), half)],
            g_recv.at[layer, 3], g_send.at[layer, 3], None)

    def out_t(layer):
        rows = go.shape[2] // 2
        return Gather(
            f"L{layer}_ot", at[layer].ring(False), go.at[layer, number(at[layer].t, 0)],
            lambda pos, other: go.at[layer, number(pos, other)],
            lambda pos, k: go.at[layer, number(pos, 0), pl.ds(k * rows, rows)],
            g_recv.at[layer, 4], g_send.at[layer, 4], partner, wo, l_sem.at[layer, 4], number)

    q_job = [weights(layer, 0, "q", wq_in, gq, wq) for layer in range(layers)]
    u_job = [weights(layer, 1, "u", wu_in, gu, wu) for layer in range(layers)]
    d_job = [[down_half(layer, h) for h in range(2)] for layer in range(layers)]
    ow_job = [out_w(layer) for layer in range(layers)]
    ot_job = [out_t(layer) for layer in range(layers)]

    def own_out(layer):
        return pltpu.make_async_copy(wo_in.at[layer], ow_job[layer].slot(at[layer].w, 0), c_sem.at[layer])

    def all_bias(layer):
        moved = bup.at[layer, pl.ds(0, col - 1)]
        return remote(moved, moved, b_sem.at[layer, 0], b_sem.at[layer, 1], me)

    with scope("enter"):
        enter([(me + d) % tp for d in range(1, tp)])
    ow_job[0].start()
    q_job[0].start()
    for layer in range(layers):
        own_out(layer).start()
        mine = at[layer].mine
        for d in range(1, col):
            row = bu_ref.at[pl.ds(layer, 1)]
            remote(row, bup.at[layer, mine], b_sem.at[layer, 0], b_sem.at[layer, 1], at[layer].in_w((mine + d) % col)).start()
        bup[layer, mine] = bu_ref[layer : layer + 1, :]
    q_job[0].own()
    resid[...] = x_ref[...].astype(F32)

    class Spread:
        def __init__(self, layer, which, buf):
            self.buf, self.name = buf.at[layer], f"L{layer}_h{which}"
            self.send, self.recv = h_send.at[layer, which], h_recv.at[layer, which]
            self.prev, self.next = at[layer].ring(False)[:2]
            self.half = share // 2

        def full(self, k):
            return remote(self.buf.at[0], self.buf.at[k], self.send.at[k - 1], self.recv.at[k - 1], self.next if k == 1 else self.prev)

        def part(self, k):
            rows = pl.ds((k - 1) * self.half, self.half)
            return remote(self.buf.at[k, rows], self.buf.at[3, rows], self.send.at[k + 1], self.recv.at[k + 1], self.next if k == 1 else self.prev)

        def start(self):
            self.full(1).start()
            self.full(2).start()

        def relay(self, k):
            with scope(f"{self.name}_recv{k}"):
                self.full(k).wait_recv()
                self.part(k).start()

        def far(self):
            with scope(f"{self.name}_far"):
                self.part(1).wait_recv()
                self.part(2).wait_recv()

        def drain(self):
            for k in (1, 2):
                self.full(k).wait_send()
                self.part(k).wait_send()

    for layer in range(layers):
        first, final = layer == 0, layer == layers - 1
        row = slice(layer, layer + 1)
        lay = at[layer]
        tag = f"L{layer}_"
        h1[layer, 0] = norm(resid[...], ln1g[row, :], ln1b[row, :])
        spread1 = Spread(layer, 0, h1)
        spread1.start()

        def q_copy(k, m):
            return remote(qsend.at[k, m], qkv.at[layer, lay.owner(k)], q_sem.at[layer, 0], q_sem.at[layer, 1], lay.in_w(m))

        def put(k, m, part):
            @pl.when(m != lay.mine)
            def _():
                qsend[k, m] = part
                q_copy(k, m).start()

            @pl.when(m == lay.mine)
            def _():
                qkv[layer, lay.owner(k)] = part

        def q_parts(k0, count, start, slots):
            def step(n, _):
                m = (start + n) % col
                part = lax.dot_general(wq[m], h1[layer, k0 : k0 + count].reshape(count * share, width), NT, preferred_element_type=F32).astype(BF16)
                for k in range(count):
                    put(k0 + k, m, part[:, k * share : (k + 1) * share])
                return 0

            with scope(f"{tag}qkv{k0}"):
                lax.fori_loop(0, slots, step, 0)

        job = q_job[layer]
        if first:
            slots = [pos * CORES for pos in job.order()]
            job.other(0)
            job.ready(0)
            q_parts(0, 1, slots[0], CORES)
            spread1.relay(1)
            spread1.relay(2)
            if not final:
                q_job[layer + 1].start()
                ow_job[layer + 1].start()
            q_parts(1, 1, slots[0], CORES)
            q_parts(2, 1, slots[0], CORES)
            ow_job[layer].relay()
            job.relay()
            spread1.far()
            q_parts(3, 1, slots[0], CORES)
            job.other(1)
            job.other(2)
            job.ready(1, 2)
            for n in (1, 2):
                q_parts(0, 2, slots[n], CORES)
                q_parts(2, 2, slots[n], CORES)
            ow_job[layer].last()
            own_out(layer).wait()
            ot_job[layer].start()
            job.last()
            job.other(3)
            job.ready(3)
            q_parts(0, 2, slots[3], CORES)
            q_parts(2, 2, slots[3], CORES)
        else:
            q_parts(0, 1, lay.mine + 1, col)
            spread1.relay(1)
            spread1.relay(2)
            ot_job[layer].relay()
            q_parts(1, 2, lay.mine + 1, col)
            spread1.far()
            q_parts(3, 1, lay.mine + 1, col)
            u_job[layer].own()
            u_job[layer].last()
        moved = qkv.at[layer, pl.ds(0, side * (col - 1))]
        all_qkv = remote(moved, moved, q_sem.at[layer, 0], q_sem.at[layer, 1], me)
        with scope(tag + "qkv_recv"):
            all_qkv.wait_recv()
        if first:
            u_job[layer].start()
        else:
            for d in d_job[layer]:
                d.start()
        def hook_early():
            if not first:
                for i in range(4):
                    u_job[layer].other(i)

        def hook_middle():
            if first:
                ot_job[layer].relay()
                if not final:
                    ow_job[layer + 1].relay()
                    q_job[layer + 1].relay()

        def hook_late():
            if first:
                u_job[layer].relay()

        hooks = {3: hook_early, 5: hook_middle, 7: hook_late}
        with scope(tag + "attend"):
            attend(layer, me, (lay.t * CORES + c) * side + lay.w, qkv, oall, osend, o_sem, hooks)
        moved = oall.at[layer, pl.ds(0, tp - 1)]
        all_o = remote(moved, moved, o_sem.at[layer, 0], o_sem.at[layer, 1], me)
        ot, u = ot_job[layer], u_job[layer]
        ot.own()
        for i in range(3):
            ot.other(i)
        ot.last()
        ot.other(3)
        ot.ready(0, 1, 2, 3)
        with scope(tag + "o_recv"):
            all_o.wait_recv()
        if not first:
            for d in d_job[layer]:
                d.own()
                d.relay()
        o_t = oall[layer].reshape(tp * dim, share)

        def out_step(n, _):
            cs = pl.ds(pl.multiple_of(n * tile, tile), tile)
            w = wo[:, :, cs].reshape(tp * dim, tile)
            resid[:, cs] = resid[:, cs] + (lax.dot_general(o_t, w, TN, preferred_element_type=F32) + bo_ref[row, cs])
            return 0

        with scope(tag + "outproj"):
            lax.fori_loop(0, width // tile, out_step, 0)
        h2[layer, 0] = norm(resid[...], ln2g[row, :], ln2b[row, :])
        spread2 = Spread(layer, 1, h2)
        spread2.start()
        if first:
            d_job[layer][0].start()
        all_bias(layer).wait()

        def up(k0, count):
            def up_step(g, _):
                h = h2[layer, k0 : k0 + count].reshape(count * share, width)
                pre = lax.dot_general(h, wu[g], NN, preferred_element_type=F32) + bup[layer, g]
                act = jax.nn.gelu(pre, approximate=True).astype(BF16)
                ubuf[k0 * share : (k0 + count) * share, pl.ds(pl.multiple_of(g * hidden, 128), hidden)] = act
                return 0

            with scope(f"{tag}up{k0}"):
                lax.fori_loop(0, col, up_step, 0)

        pieces = zsend.shape[0]
        piece = width // pieces

        def z_copy(p, k):
            return remote(zsend.at[p, k - 1], zrecv.at[layer, p, k - 1], z_send.at[layer, k - 1, p], z_recv.at[layer, k - 1, p], lay.owner(k))

        def down(k0, count, h):
            per_half = pieces // 2

            def piece_step(i, _):
                p = h * per_half + i
                for n in range(piece // tile):
                    cs = pl.ds(pl.multiple_of(p * piece + n * tile, tile), tile)
                    w = wd[h, :, :, pl.ds(pl.multiple_of(i * piece + n * tile, tile), tile)].reshape(col * hidden, tile)
                    z = lax.dot_general(ubuf[k0 * share : (k0 + count) * share, :], w, NN, preferred_element_type=F32)
                    for k in range(k0, k0 + count):
                        zk = z[(k - k0) * share : (k - k0 + 1) * share]
                        if k:
                            zsend[p, k - 1, :, n * tile : (n + 1) * tile] = zk.astype(BF16)
                        else:
                            resid[:, cs] = resid[:, cs] + (zk + bd_ref[row, cs])
                for k in range(max(k0, 1), k0 + count):
                    z_copy(p, k).start()
                return 0

            with scope(f"{tag}down{k0}_{h}"):
                lax.fori_loop(0, per_half, piece_step, 0)

        da, db = d_job[layer]
        if first:
            if not final:
                ow_job[layer + 1].last()
                own_out(layer + 1).wait()
                q_job[layer + 1].last()
            spread2.relay(1)
            spread2.relay(2)
            u.own()
            da.own()
            da.relay()
            db.start()
            if not final:
                u_job[layer + 1].start()
                for i in range(4):
                    q_job[layer + 1].other(i)
            for i in range(3):
                u.other(i)
            u.last()
            u.other(3)
            u.ready(0, 1, 2, 3)
            spread2.far()
            up(0, side)
            for i in range(3):
                da.other(i)
            da.last()
            da.other(3)
            da.ready(0, 1, 2, 3)
            down(0, side, 0)
            db.own()
            db.relay()
            if not final:
                ot_job[layer + 1].start()
            for i in range(3):
                db.other(i)
            db.last()
            db.other(3)
            db.ready(0, 1, 2, 3)
            down(0, side, 1)
        else:
            u.ready(0, 1, 2, 3)
            up(0, 1)
            spread2.relay(1)
            spread2.relay(2)
            da.last()
            db.last()
            up(1, 2)
            for d in (da, db):
                for i in range(4):
                    d.other(i)
                d.ready(0, 1, 2, 3)
            down(1, 2, 0)
            down(1, 2, 1)
            spread2.far()
            up(3, 1)
            down(3, 1, 0)
            down(3, 1, 1)
            down(0, 1, 0)
            down(0, 1, 1)
        if not final:
            q_job[layer + 1].own()
            q_job[layer + 1].ready(0, 1, 2, 3)
        with scope(tag + "z_recv"):
            for p in range(pieces):
                cs = slice(p * piece, (p + 1) * piece)
                total = resid[:, cs]
                for k in (1, 2, 3):
                    z_copy(p, k).wait_recv()
                    total = total + zrecv[layer, p, k - 1].astype(F32)
                if final:
                    out_ref[:, cs] = total.astype(BF16)
                else:
                    resid[:, cs] = total
        if not final:
            u_job[layer + 1].relay()
        with scope(tag + "sent"):
            all_qkv.wait_send()
            all_o.wait_send()
            spread1.drain()
            spread2.drain()
            for p in range(pieces):
                for k in (1, 2, 3):
                    z_copy(p, k).wait_send()
    with scope("drain"):
        for layer in range(layers):
            q_job[layer].drain(gq.at[layer, pl.ds(0, 7)])
            u_job[layer].drain(gu.at[layer, pl.ds(0, 7)])
            for h in range(2):
                d_job[layer][h].drain(gd.at[layer, h, pl.ds(0, 7)])
            ot_job[layer].drain(go.at[layer, pl.ds(0, 7)])
            ow_job[layer].drain(go.at[layer, 0, pl.ds(0, 3 * dim)])


def attend(layer, me, slot, qkv, oall, osend, o_sem, hooks):
    _, tp, three_dim, share = qkv.shape
    dim = three_dim // 3
    per = 4
    block = per * share
    c2 = math.log2(math.e) / math.sqrt(dim)
    steps = tp // per

    def part(i, count, which):
        return jnp.concatenate([qkv[layer, i * per + n, which * dim : (which + 1) * dim, :] for n in range(count * per)], axis=1)

    def q_step(i, _):
        for when, hook in hooks.items():
            pl.when(i == when)(hook)
        q = part(i, 1, 0).T

        def update(j, count, carry, masked):
            m, l, acc = carry
            s = lax.dot_general(q, part(j, count, 1), NN, preferred_element_type=F32)
            if masked:
                rows = lax.broadcasted_iota(jnp.int32, (block, count * block), 0)
                cols = lax.broadcasted_iota(jnp.int32, (block, count * block), 1)
                s = jnp.where(rows + (count - 1) * block >= cols, s, -1e30)
            m_new = jnp.maximum(m, jnp.max(s, axis=-1, keepdims=True))
            p = jnp.exp2(s * c2 - m_new * c2)
            alpha = jnp.exp2((m - m_new) * c2)
            acc = acc * alpha + lax.dot_general(p.astype(BF16), part(j, count, 2), NT, preferred_element_type=F32)
            return m_new, l * alpha + jnp.sum(p, axis=-1, keepdims=True), acc

        init = (jnp.full((block, 1), -1e30, F32), jnp.zeros((block, 1), F32), jnp.zeros((block, dim), F32))
        carry = lax.fori_loop(0, i // 2, lambda j, carry: update(2 * j, 2, carry, False), init)
        _, l, acc = lax.cond(i % 2 == 1, lambda carry: update(i - 1, 2, carry, True), lambda carry: update(i, 1, carry, True), carry)
        o_t = (acc / l).T.astype(BF16)
        for n in range(per):
            d = (i * per + n - me + tp) % tp
            piece = o_t[:, n * share : (n + 1) * share]

            @pl.when(d != 0)
            def _():
                osend[d] = piece
                remote(osend.at[d], oall.at[layer, slot], o_sem.at[layer, 0], o_sem.at[layer, 1], i * per + n).start()

            @pl.when(d == 0)
            def _():
                oall[layer, slot] = piece

        return 0

    lax.fori_loop(0, steps, q_step, 0)


def solution(mesh):
    tp = mesh.shape["tp"]
    side = math.isqrt(tp // CORES)
    col = side * CORES
    near = side - 1
    pieces = 4

    def local_forward(x_local, ln1_gain, ln1_bias, ln2_gain, ln2_bias, w_qkv, w_out, b_out, w_up, b_up, w_down, b_down):
        _, share, width = x_local.shape
        layers, _, three, _, dim = w_qkv.shape
        hidden = w_up.shape[2]
        piece = width // pieces
        wq_t = jnp.transpose(w_qkv, (0, 2, 3, 4, 1)).reshape(layers, three * dim, width)
        hbm = lambda *shape: jax.ShapeDtypeStruct(shape, BF16)
        vmem = lambda *shape: pltpu.VMEM(shape, BF16)
        y = pl.pallas_call(
            functools.partial(decoder_kernel, side, layers),
            out_shape=(
                hbm(share, width), hbm(layers, col, three * dim, width), hbm(layers, col, side * dim, width),
                hbm(layers, col, width, hidden), hbm(layers, 2, col, hidden, width // 2),
            ),
            in_specs=[VMEM] * 8 + [HBM] * 4,
            out_specs=(VMEM, HBM, HBM, HBM, HBM),
            scratch_shapes=[
                vmem(col, three * dim, width), vmem(col, side * dim, width), vmem(col, width, hidden), vmem(2, col, hidden, width // 2),
                vmem(layers, side, share, width), vmem(layers, side, share, width),
                vmem(layers, tp, three * dim, share), vmem(side, col, three * dim, share),
                vmem(layers, tp, dim, share), vmem(tp, dim, share),
                vmem(side * share, col * hidden),
                vmem(pieces, near, share, piece), vmem(layers, pieces, near, share, piece),
                pltpu.VMEM((share, width), F32), pltpu.VMEM((layers, col, 1, hidden), F32),
                DMA((layers, 6, 8)), DMA((layers, 6)), DMA((layers, 2, 4)), DMA((layers, 2, 4)),
                DMA((layers, 2)), DMA((layers, 2)), DMA((layers, near, pieces)), DMA((layers, near, pieces)),
                DMA((layers, 2)), DMA((layers, 6, 8)), DMA((layers,)),
            ],
            compiler_params=pltpu.CompilerParams(collective_id=0, has_side_effects=True, vmem_limit_bytes=63 * 1024 * 1024),
            name="decoder",
        )(x_local[0], ln1_gain, ln1_bias, ln2_gain, ln2_bias, b_out, b_up, b_down, wq_t, w_out.reshape(layers, dim, width), w_up, w_down)[0]
        return y[None]

    rows_spec = P("dp", "tp", None)
    in_specs = (rows_spec, P(), P(), P(), P(), P(None, None, None, "tp", None), P(None, "tp", None, None), P(), P(None, None, "tp"), P(None, "tp"), P(None, "tp", None), P())
    return jax.shard_map(local_forward, mesh=mesh, in_specs=in_specs, out_specs=rows_spec, check_vma=False)
```

```python
import functools
import math
import jax
import jax.numpy as jnp
from jax import lax
from jax.experimental import pallas as pl
from jax.experimental.pallas import tpu as pltpu
from jax.sharding import PartitionSpec as P

F32 = jnp.float32
BF16 = jnp.bfloat16
CORES = 2
NN = (((1,), (0,)), ((), ()))
NT = (((1,), (1,)), ((), ()))
TN = (((0,), (0,)), ((), ()))
MESH = pl.DeviceIdType.MESH
VMEM = pl.BlockSpec(memory_space=pltpu.VMEM)
HBM = pl.BlockSpec(memory_space=pl.ANY)
DMA = pltpu.SemaphoreType.DMA


def index_of(side, y, x, c):
    return (y * side + x) * CORES + c


def dev(index):
    return {"tp": index}


def remote(src, dst, send_sem, recv_sem, index):
    return pltpu.make_async_remote_copy(src_ref=src, dst_ref=dst, send_sem=send_sem, recv_sem=recv_sem, device_id=dev(index), device_id_type=MESH)


def enter(indices):
    barrier = pltpu.get_barrier_semaphore()
    for index in indices:
        pl.semaphore_signal(barrier, inc=1, device_id=dev(index), device_id_type=MESH)
    pl.semaphore_wait(barrier, len(indices))


def norm(resid, gain, shift):
    row_mean = jnp.mean(resid, axis=-1, keepdims=True)
    centered = resid - row_mean
    variance = jnp.mean(centered * centered, axis=-1, keepdims=True)
    return (centered * lax.rsqrt(variance + 1e-5) * gain + shift).astype(BF16)


scope = jax.named_scope


class Gather:
    def __init__(self, name, ring, src, slot, half, recv, send, partner, dst=None, load_sem=None, number=None):
        self.name = name
        self.prev, self.next, self.back, self.here, self.fwd, self.far = ring
        self.src, self.slot, self.half, self.recv, self.send, self.partner = src, slot, half, recv, send, partner
        self.dst, self.load_sem, self.number = dst, load_sem, number

    def order(self):
        return (self.here, self.back, self.fwd, self.far)

    def start(self):
        dst = self.slot(self.here, 0)
        remote(self.src, dst, self.send, self.recv.at[0], self.next).start()
        remote(self.src, dst, self.send, self.recv.at[1], self.prev).start()
        if self.partner is not None:
            remote(self.src, dst, self.send, self.recv.at[4], self.partner).start()

    def landed(self, ref, n):
        remote(ref, ref, self.send, self.recv.at[n], self.next).wait_recv()

    def load(self, i, other):
        pos = self.order()[i]
        src = self.src if i == 0 and other == 0 else self.slot(pos, other)
        return pltpu.make_async_copy(src, self.dst.at[self.number(pos, other)], self.load_sem.at[2 * i + other])

    def share(self, pos, n):
        ref = self.slot(pos, 0)
        remote(ref, ref, self.send, self.recv.at[n], self.partner).start()

    def relay(self):
        with scope(self.name + "_relay"):
            for n, pos, to in ((0, self.back, self.next), (1, self.fwd, self.prev)):
                self.landed(self.slot(pos, 0), n)
                ref = self.half(pos, n)
                remote(ref, ref, self.send, self.recv.at[2 + n], to).start()
                if self.partner is not None:
                    self.share(pos, 5 + n)
                    self.load(1 + n, 0).start()

    def own(self):
        self.load(0, 0).start()

    def other(self, i):
        with scope(f"{self.name}_other{i}"):
            self.landed(self.slot(self.order()[i], 1), 4 + i)
            self.load(i, 1).start()

    def last(self):
        with scope(self.name + "_last"):
            self.landed(self.half(self.far, 0), 2)
            self.landed(self.half(self.far, 1), 3)
            if self.partner is not None:
                self.share(self.far, 7)
                self.load(3, 0).start()

    def ready(self, *which):
        with scope(self.name + "_ready"):
            for i in which:
                self.load(i, 0).wait()
                self.load(i, 1).wait()

    def drain(self, ref):
        remote(ref, ref, self.send, self.recv.at[0], self.next).wait_send()


class Layer:
    def __init__(self, side, layer, y, x, c):
        self.side, self.swap, self.c = side, layer % 2, c
        self.w, self.t = (x, y) if self.swap else (y, x)
        self.mine = self.w * CORES + c

    def at(self, w, t, c):
        return index_of(self.side, t, w, c) if self.swap else index_of(self.side, w, t, c)

    def in_w(self, m):
        return self.at(m // CORES, self.t, m % CORES)

    def ring(self, along_w):
        side, c = self.side, self.c
        p = self.w if along_w else self.t
        back, fwd, far = (p + side - 1) % side, (p + 1) % side, (p + 2) % side
        at = (lambda q: self.at(q, self.t, c)) if along_w else (lambda q: self.at(self.w, q, c))
        return at(back), at(fwd), back, p, fwd, far

    def owner(self, k):
        return self.at(self.w, (self.t + (0, self.side - 1, 1, 2)[k]) % self.side, self.c)


def decoder_kernel(side, layers, x_ref, ln1g, ln1b, ln2g, ln2b, bo_ref, bu_ref, bd_ref, wq_in, wo_in, wu_in, wd_in,
                   out_ref, gq, go, gu, gd,
                   wq, wo, wu, wd, h1, h2, qkv, qsend, oall, osend, ubuf, zsend, zrecv, resid, bup,
                   g_recv, g_send, h_send, h_recv, q_sem, o_sem, z_send, z_recv, b_sem, l_sem, c_sem):
    me = lax.axis_index("tp")
    y, x, c = me // (side * CORES), (me // CORES) % side, me % CORES
    col = side * CORES
    tp = side * col
    near = side - 1
    share, width = x_ref.shape
    dim = oall.shape[2]
    hidden = wu.shape[2]
    tile = 256
    partner = index_of(side, y, x, 1 - c)
    at = [Layer(side, layer, y, x, c) for layer in range(layers)]

    def number(pos, other):
        return pos * CORES + (c if other == 0 else 1 - c)

    def weights(layer, n, name, src, buf, dst):
        rows = buf.shape[2] // 2
        return Gather(
            f"L{layer}_{name}", at[layer].ring(True), src.at[layer],
            lambda pos, other: buf.at[layer, number(pos, other)],
            lambda pos, k: buf.at[layer, number(pos, 0), pl.ds(k * rows, rows)],
            g_recv.at[layer, n], g_send.at[layer, n], partner, dst, l_sem.at[layer, n], number)

    def down_half(layer, h):
        rows, cols = hidden // 2, width // 2
        n = (2, 5)[h]
        return Gather(
            f"L{layer}_d{h}", at[layer].ring(True), wd_in.at[layer, :, pl.ds(h * cols, cols)],
            lambda pos, other: gd.at[layer, h, number(pos, other)],
            lambda pos, k: gd.at[layer, h, number(pos, 0), pl.ds(k * rows, rows)],
            g_recv.at[layer, n], g_send.at[layer, n], partner, wd.at[h], l_sem.at[layer, n], number)

    def out_w(layer):
        here = number(at[layer].t, 0)
        half = dim // 2
        return Gather(
            f"L{layer}_ow", at[layer].ring(True), wo_in.at[layer],
            lambda pos, other: go.at[layer, here, pl.ds(pl.multiple_of(pos * dim, dim), dim)],
            lambda pos, k: go.at[layer, here, pl.ds(pl.multiple_of(pos * dim + k * half, half), half)],
            g_recv.at[layer, 3], g_send.at[layer, 3], None)

    def out_t(layer):
        rows = go.shape[2] // 2
        return Gather(
            f"L{layer}_ot", at[layer].ring(False), go.at[layer, number(at[layer].t, 0)],
            lambda pos, other: go.at[layer, number(pos, other)],
            lambda pos, k: go.at[layer, number(pos, 0), pl.ds(k * rows, rows)],
            g_recv.at[layer, 4], g_send.at[layer, 4], partner, wo, l_sem.at[layer, 4], number)

    q_job = [weights(layer, 0, "q", wq_in, gq, wq) for layer in range(layers)]
    u_job = [weights(layer, 1, "u", wu_in, gu, wu) for layer in range(layers)]
    d_job = [[down_half(layer, h) for h in range(2)] for layer in range(layers)]
    ow_job = [out_w(layer) for layer in range(layers)]
    ot_job = [out_t(layer) for layer in range(layers)]

    def own_out(layer):
        return pltpu.make_async_copy(wo_in.at[layer], ow_job[layer].slot(at[layer].w, 0), c_sem.at[layer])

    def all_bias(layer):
        moved = bup.at[layer, pl.ds(0, col - 1)]
        return remote(moved, moved, b_sem.at[layer, 0], b_sem.at[layer, 1], me)

    with scope("enter"):
        enter([(me + d) % tp for d in range(1, tp)])
    ow_job[0].start()
    q_job[0].start()
    for layer in range(layers):
        own_out(layer).start()
        mine = at[layer].mine
        for d in range(1, col):
            row = bu_ref.at[pl.ds(layer, 1)]
            remote(row, bup.at[layer, mine], b_sem.at[layer, 0], b_sem.at[layer, 1], at[layer].in_w((mine + d) % col)).start()
        bup[layer, mine] = bu_ref[layer : layer + 1, :]
    q_job[0].own()
    resid[...] = x_ref[...].astype(F32)

    class Spread:
        def __init__(self, layer, which, buf):
            self.buf, self.name = buf.at[layer], f"L{layer}_h{which}"
            self.send, self.recv = h_send.at[layer, which], h_recv.at[layer, which]
            self.prev, self.next = at[layer].ring(False)[:2]
            self.half = share // 2

        def full(self, k):
            return remote(self.buf.at[0], self.buf.at[k], self.send.at[k - 1], self.recv.at[k - 1], self.next if k == 1 else self.prev)

        def part(self, k):
            rows = pl.ds((k - 1) * self.half, self.half)
            return remote(self.buf.at[k, rows], self.buf.at[3, rows], self.send.at[k + 1], self.recv.at[k + 1], self.next if k == 1 else self.prev)

        def start(self):
            self.full(1).start()
            self.full(2).start()

        def relay(self, k):
            with scope(f"{self.name}_recv{k}"):
                self.full(k).wait_recv()
                self.part(k).start()

        def far(self):
            with scope(f"{self.name}_far"):
                self.part(1).wait_recv()
                self.part(2).wait_recv()

        def drain(self):
            for k in (1, 2):
                self.full(k).wait_send()
                self.part(k).wait_send()

    for layer in range(layers):
        first, final = layer == 0, layer == layers - 1
        row = slice(layer, layer + 1)
        lay = at[layer]
        tag = f"L{layer}_"
        h1[layer, 0] = norm(resid[...], ln1g[row, :], ln1b[row, :])
        spread1 = Spread(layer, 0, h1)
        spread1.start()

        def q_copy(k, m):
            return remote(qsend.at[k, m], qkv.at[layer, lay.owner(k)], q_sem.at[layer, 0], q_sem.at[layer, 1], lay.in_w(m))

        def put(k, m, part):
            @pl.when(m != lay.mine)
            def _():
                qsend[k, m] = part
                q_copy(k, m).start()

            @pl.when(m == lay.mine)
            def _():
                qkv[layer, lay.owner(k)] = part

        def q_parts(k0, count, start, slots):
            def step(n, _):
                m = (start + n) % col
                part = lax.dot_general(wq[m], h1[layer, k0 : k0 + count].reshape(count * share, width), NT, preferred_element_type=F32).astype(BF16)
                for k in range(count):
                    put(k0 + k, m, part[:, k * share : (k + 1) * share])
                return 0

            with scope(f"{tag}qkv{k0}"):
                lax.fori_loop(0, slots, step, 0)

        job = q_job[layer]
        if first:
            slots = [pos * CORES for pos in job.order()]
            job.other(0)
            job.ready(0)
            q_parts(0, 1, slots[0], CORES)
            spread1.relay(1)
            spread1.relay(2)
            if not final:
                q_job[layer + 1].start()
                ow_job[layer + 1].start()
            q_parts(1, 1, slots[0], CORES)
            q_parts(2, 1, slots[0], CORES)
            ow_job[layer].relay()
            job.relay()
            spread1.far()
            q_parts(3, 1, slots[0], CORES)
            job.other(1)
            job.other(2)
            job.ready(1, 2)
            for n in (1, 2):
                q_parts(0, 2, slots[n], CORES)
                q_parts(2, 2, slots[n], CORES)
            ow_job[layer].last()
            own_out(layer).wait()
            ot_job[layer].start()
            job.last()
            job.other(3)
            job.ready(3)
            q_parts(0, 2, slots[3], CORES)
            q_parts(2, 2, slots[3], CORES)
            u_job[layer].start()
        else:
            q_parts(0, 1, lay.mine + 1, col)
            spread1.relay(1)
            spread1.relay(2)
            ot_job[layer].relay()
            q_parts(1, 2, lay.mine + 1, col)
            spread1.far()
            q_parts(3, 1, lay.mine + 1, col)
            u_job[layer].own()
            u_job[layer].last()
        moved = qkv.at[layer, pl.ds(0, side * (col - 1))]
        all_qkv = remote(moved, moved, q_sem.at[layer, 0], q_sem.at[layer, 1], me)
        with scope(tag + "qkv_recv"):
            all_qkv.wait_recv()
        if not first:
            for d in d_job[layer]:
                d.start()
        def hook_early():
            if not first:
                for i in range(4):
                    u_job[layer].other(i)

        def hook_middle():
            if first:
                ot_job[layer].relay()
                if not final:
                    ow_job[layer + 1].relay()
                    q_job[layer + 1].relay()

        def hook_late():
            if first:
                u_job[layer].relay()

        hooks = {3: hook_early, 5: hook_middle, 7: hook_late}
        with scope(tag + "attend"):
            attend(layer, me, (lay.t * CORES + c) * side + lay.w, qkv, oall, osend, o_sem, hooks)
        moved = oall.at[layer, pl.ds(0, tp - 1)]
        all_o = remote(moved, moved, o_sem.at[layer, 0], o_sem.at[layer, 1], me)
        ot, u = ot_job[layer], u_job[layer]
        ot.own()
        for i in range(3):
            ot.other(i)
        ot.last()
        ot.other(3)
        ot.ready(0, 1, 2, 3)
        if first:
            for d in d_job[layer]:
                d.start()
        with scope(tag + "o_recv"):
            all_o.wait_recv()
        if not first:
            for d in d_job[layer]:
                d.own()
                d.relay()
        o_t = oall[layer].reshape(tp * dim, share)

        def out_step(n, _):
            cs = pl.ds(pl.multiple_of(n * tile, tile), tile)
            w = wo[:, :, cs].reshape(tp * dim, tile)
            resid[:, cs] = resid[:, cs] + (lax.dot_general(o_t, w, TN, preferred_element_type=F32) + bo_ref[row, cs])
            return 0

        with scope(tag + "outproj"):
            lax.fori_loop(0, width // tile, out_step, 0)
        h2[layer, 0] = norm(resid[...], ln2g[row, :], ln2b[row, :])
        spread2 = Spread(layer, 1, h2)
        spread2.start()
        all_bias(layer).wait()

        def up(k0, count):
            def up_step(g, _):
                h = h2[layer, k0 : k0 + count].reshape(count * share, width)
                pre = lax.dot_general(h, wu[g], NN, preferred_element_type=F32) + bup[layer, g]
                act = jax.nn.gelu(pre, approximate=True).astype(BF16)
                ubuf[k0 * share : (k0 + count) * share, pl.ds(pl.multiple_of(g * hidden, 128), hidden)] = act
                return 0

            with scope(f"{tag}up{k0}"):
                lax.fori_loop(0, col, up_step, 0)

        pieces = zsend.shape[0]
        piece = width // pieces

        def z_copy(p, k):
            return remote(zsend.at[p, k - 1], zrecv.at[layer, p, k - 1], z_send.at[layer, k - 1, p], z_recv.at[layer, k - 1, p], lay.owner(k))

        def down(k0, count, h):
            per_half = pieces // 2

            def piece_step(i, _):
                p = h * per_half + i
                for n in range(piece // tile):
                    cs = pl.ds(pl.multiple_of(p * piece + n * tile, tile), tile)
                    w = wd[h, :, :, pl.ds(pl.multiple_of(i * piece + n * tile, tile), tile)].reshape(col * hidden, tile)
                    z = lax.dot_general(ubuf[k0 * share : (k0 + count) * share, :], w, NN, preferred_element_type=F32)
                    for k in range(k0, k0 + count):
                        zk = z[(k - k0) * share : (k - k0 + 1) * share]
                        if k:
                            zsend[p, k - 1, :, n * tile : (n + 1) * tile] = zk.astype(BF16)
                        else:
                            resid[:, cs] = resid[:, cs] + (zk + bd_ref[row, cs])
                for k in range(max(k0, 1), k0 + count):
                    z_copy(p, k).start()
                return 0

            with scope(f"{tag}down{k0}_{h}"):
                lax.fori_loop(0, per_half, piece_step, 0)

        da, db = d_job[layer]
        if first:
            if not final:
                ow_job[layer + 1].last()
                own_out(layer + 1).wait()
                q_job[layer + 1].last()
            spread2.relay(1)
            spread2.relay(2)
            u.own()
            da.own()
            da.relay()
            if not final:
                u_job[layer + 1].start()
                for i in range(4):
                    q_job[layer + 1].other(i)
            for i in range(3):
                u.other(i)
            u.last()
            u.other(3)
            u.ready(0, 1, 2, 3)
            spread2.far()
            up(0, side)
            db.own()
            db.relay()
            for i in range(3):
                da.other(i)
            da.last()
            da.other(3)
            da.ready(0, 1, 2, 3)
            down(0, side, 0)
            if not final:
                ot_job[layer + 1].start()
            for i in range(3):
                db.other(i)
            db.last()
            db.other(3)
            db.ready(0, 1, 2, 3)
            down(0, side, 1)
        else:
            u.ready(0, 1, 2, 3)
            up(0, 1)
            da.last()
            db.last()
            for d in (da, db):
                for i in range(4):
                    d.other(i)
            spread2.relay(1)
            spread2.relay(2)
            up(1, 2)
            da.ready(0, 1, 2, 3)
            db.ready(0, 1, 2, 3)
            down(1, 2, 0)
            down(1, 2, 1)
            spread2.far()
            up(3, 1)
            down(3, 1, 0)
            down(3, 1, 1)
            down(0, 1, 0)
            down(0, 1, 1)
        if not final:
            q_job[layer + 1].own()
            q_job[layer + 1].ready(0, 1, 2, 3)
        with scope(tag + "z_recv"):
            for p in range(pieces):
                cs = slice(p * piece, (p + 1) * piece)
                total = resid[:, cs]
                for k in (1, 2, 3):
                    z_copy(p, k).wait_recv()
                    total = total + zrecv[layer, p, k - 1].astype(F32)
                if final:
                    out_ref[:, cs] = total.astype(BF16)
                else:
                    resid[:, cs] = total
        if not final:
            u_job[layer + 1].relay()
        with scope(tag + "sent"):
            all_qkv.wait_send()
            all_o.wait_send()
            spread1.drain()
            spread2.drain()
            for p in range(pieces):
                for k in (1, 2, 3):
                    z_copy(p, k).wait_send()
    with scope("drain"):
        for layer in range(layers):
            q_job[layer].drain(gq.at[layer, pl.ds(0, 7)])
            u_job[layer].drain(gu.at[layer, pl.ds(0, 7)])
            for h in range(2):
                d_job[layer][h].drain(gd.at[layer, h, pl.ds(0, 7)])
            ot_job[layer].drain(go.at[layer, pl.ds(0, 7)])
            ow_job[layer].drain(go.at[layer, 0, pl.ds(0, 3 * dim)])


def attend(layer, me, slot, qkv, oall, osend, o_sem, hooks):
    _, tp, three_dim, share = qkv.shape
    dim = three_dim // 3
    per = 4
    block = per * share
    c2 = math.log2(math.e) / math.sqrt(dim)
    steps = tp // per

    def part(i, count, which):
        return jnp.concatenate([qkv[layer, i * per + n, which * dim : (which + 1) * dim, :] for n in range(count * per)], axis=1)

    def q_step(i, _):
        for when, hook in hooks.items():
            pl.when(i == when)(hook)
        q = part(i, 1, 0).T

        def update(j, count, carry, masked):
            m, l, acc = carry
            s = lax.dot_general(q, part(j, count, 1), NN, preferred_element_type=F32)
            if masked:
                rows = lax.broadcasted_iota(jnp.int32, (block, count * block), 0)
                cols = lax.broadcasted_iota(jnp.int32, (block, count * block), 1)
                s = jnp.where(rows + (count - 1) * block >= cols, s, -1e30)
            m_new = jnp.maximum(m, jnp.max(s, axis=-1, keepdims=True))
            p = jnp.exp2(s * c2 - m_new * c2)
            alpha = jnp.exp2((m - m_new) * c2)
            acc = acc * alpha + lax.dot_general(p.astype(BF16), part(j, count, 2), NT, preferred_element_type=F32)
            return m_new, l * alpha + jnp.sum(p, axis=-1, keepdims=True), acc

        init = (jnp.full((block, 1), -1e30, F32), jnp.zeros((block, 1), F32), jnp.zeros((block, dim), F32))
        carry = lax.fori_loop(0, i // 2, lambda j, carry: update(2 * j, 2, carry, False), init)
        _, l, acc = lax.cond(i % 2 == 1, lambda carry: update(i - 1, 2, carry, True), lambda carry: update(i, 1, carry, True), carry)
        o_t = (acc / l).T.astype(BF16)
        for n in range(per):
            d = (i * per + n - me + tp) % tp
            piece = o_t[:, n * share : (n + 1) * share]

            @pl.when(d != 0)
            def _():
                osend[d] = piece
                remote(osend.at[d], oall.at[layer, slot], o_sem.at[layer, 0], o_sem.at[layer, 1], i * per + n).start()

            @pl.when(d == 0)
            def _():
                oall[layer, slot] = piece

        return 0

    lax.fori_loop(0, steps, q_step, 0)


def solution(mesh):
    tp = mesh.shape["tp"]
    side = math.isqrt(tp // CORES)
    col = side * CORES
    near = side - 1
    pieces = 4

    def local_forward(x_local, ln1_gain, ln1_bias, ln2_gain, ln2_bias, w_qkv, w_out, b_out, w_up, b_up, w_down, b_down):
        _, share, width = x_local.shape
        layers, _, three, _, dim = w_qkv.shape
        hidden = w_up.shape[2]
        piece = width // pieces
        wq_t = jnp.transpose(w_qkv, (0, 2, 3, 4, 1)).reshape(layers, three * dim, width)
        hbm = lambda *shape: jax.ShapeDtypeStruct(shape, BF16)
        vmem = lambda *shape: pltpu.VMEM(shape, BF16)
        y = pl.pallas_call(
            functools.partial(decoder_kernel, side, layers),
            out_shape=(
                hbm(share, width), hbm(layers, col, three * dim, width), hbm(layers, col, side * dim, width),
                hbm(layers, col, width, hidden), hbm(layers, 2, col, hidden, width // 2),
            ),
            in_specs=[VMEM] * 8 + [HBM] * 4,
            out_specs=(VMEM, HBM, HBM, HBM, HBM),
            scratch_shapes=[
                vmem(col, three * dim, width), vmem(col, side * dim, width), vmem(col, width, hidden), vmem(2, col, hidden, width // 2),
                vmem(layers, side, share, width), vmem(layers, side, share, width),
                vmem(layers, tp, three * dim, share), vmem(side, col, three * dim, share),
                vmem(layers, tp, dim, share), vmem(tp, dim, share),
                vmem(side * share, col * hidden),
                vmem(pieces, near, share, piece), vmem(layers, pieces, near, share, piece),
                pltpu.VMEM((share, width), F32), pltpu.VMEM((layers, col, 1, hidden), F32),
                DMA((layers, 6, 8)), DMA((layers, 6)), DMA((layers, 2, 4)), DMA((layers, 2, 4)),
                DMA((layers, 2)), DMA((layers, 2)), DMA((layers, near, pieces)), DMA((layers, near, pieces)),
                DMA((layers, 2)), DMA((layers, 6, 8)), DMA((layers,)),
            ],
            compiler_params=pltpu.CompilerParams(collective_id=0, has_side_effects=True, vmem_limit_bytes=63 * 1024 * 1024),
            name="decoder",
        )(x_local[0], ln1_gain, ln1_bias, ln2_gain, ln2_bias, b_out, b_up, b_down, wq_t, w_out.reshape(layers, dim, width), w_up, w_down)[0]
        return y[None]

    rows_spec = P("dp", "tp", None)
    in_specs = (rows_spec, P(), P(), P(), P(), P(None, None, None, "tp", None), P(None, "tp", None, None), P(), P(None, None, "tp"), P(None, "tp"), P(None, "tp", None), P())
    return jax.shard_map(local_forward, mesh=mesh, in_specs=in_specs, out_specs=rows_spec, check_vma=False)
```

```python
import functools
import math
import jax
import jax.numpy as jnp
from jax import lax
from jax.experimental import pallas as pl
from jax.experimental.pallas import tpu as pltpu
from jax.sharding import PartitionSpec as P

F32 = jnp.float32
BF16 = jnp.bfloat16
CORES = 2
NN = (((1,), (0,)), ((), ()))
NT = (((1,), (1,)), ((), ()))
TN = (((0,), (0,)), ((), ()))
MESH = pl.DeviceIdType.MESH
VMEM = pl.BlockSpec(memory_space=pltpu.VMEM)
HBM = pl.BlockSpec(memory_space=pl.ANY)
DMA = pltpu.SemaphoreType.DMA


def index_of(side, y, x, c):
    return (y * side + x) * CORES + c


def dev(index):
    return {"tp": index}


def remote(src, dst, send_sem, recv_sem, index):
    return pltpu.make_async_remote_copy(src_ref=src, dst_ref=dst, send_sem=send_sem, recv_sem=recv_sem, device_id=dev(index), device_id_type=MESH)


def enter(indices):
    barrier = pltpu.get_barrier_semaphore()
    for index in indices:
        pl.semaphore_signal(barrier, inc=1, device_id=dev(index), device_id_type=MESH)
    pl.semaphore_wait(barrier, len(indices))


def norm(resid, gain, shift):
    row_mean = jnp.mean(resid, axis=-1, keepdims=True)
    centered = resid - row_mean
    variance = jnp.mean(centered * centered, axis=-1, keepdims=True)
    return (centered * lax.rsqrt(variance + 1e-5) * gain + shift).astype(BF16)


scope = jax.named_scope


class Gather:
    def __init__(self, name, ring, src, slot, half, recv, send, partner, dst=None, load_sem=None, number=None):
        self.name = name
        self.prev, self.next, self.back, self.here, self.fwd, self.far = ring
        self.src, self.slot, self.half, self.recv, self.send, self.partner = src, slot, half, recv, send, partner
        self.dst, self.load_sem, self.number = dst, load_sem, number

    def order(self):
        return (self.here, self.back, self.fwd, self.far)

    def start(self):
        dst = self.slot(self.here, 0)
        remote(self.src, dst, self.send, self.recv.at[0], self.next).start()
        remote(self.src, dst, self.send, self.recv.at[1], self.prev).start()
        if self.partner is not None:
            remote(self.src, dst, self.send, self.recv.at[4], self.partner).start()

    def landed(self, ref, n):
        remote(ref, ref, self.send, self.recv.at[n], self.next).wait_recv()

    def load(self, i, other):
        pos = self.order()[i]
        src = self.src if i == 0 and other == 0 else self.slot(pos, other)
        return pltpu.make_async_copy(src, self.dst.at[self.number(pos, other)], self.load_sem.at[2 * i + other])

    def share(self, pos, n):
        ref = self.slot(pos, 0)
        remote(ref, ref, self.send, self.recv.at[n], self.partner).start()

    def relay(self):
        with scope(self.name + "_relay"):
            for n, pos, to in ((0, self.back, self.next), (1, self.fwd, self.prev)):
                self.landed(self.slot(pos, 0), n)
                ref = self.half(pos, n)
                remote(ref, ref, self.send, self.recv.at[2 + n], to).start()
                if self.partner is not None:
                    self.share(pos, 5 + n)
                    self.load(1 + n, 0).start()

    def own(self):
        self.load(0, 0).start()

    def other(self, i):
        with scope(f"{self.name}_other{i}"):
            self.landed(self.slot(self.order()[i], 1), 4 + i)
            self.load(i, 1).start()

    def last(self):
        with scope(self.name + "_last"):
            self.landed(self.half(self.far, 0), 2)
            self.landed(self.half(self.far, 1), 3)
            if self.partner is not None:
                self.share(self.far, 7)
                self.load(3, 0).start()

    def ready(self, *which):
        with scope(self.name + "_ready"):
            for i in which:
                self.load(i, 0).wait()
                self.load(i, 1).wait()

    def drain(self, ref):
        remote(ref, ref, self.send, self.recv.at[0], self.next).wait_send()


class Layer:
    def __init__(self, side, layer, y, x, c):
        self.side, self.swap, self.c = side, layer % 2, c
        self.w, self.t = (x, y) if self.swap else (y, x)
        self.mine = self.w * CORES + c

    def at(self, w, t, c):
        return index_of(self.side, t, w, c) if self.swap else index_of(self.side, w, t, c)

    def in_w(self, m):
        return self.at(m // CORES, self.t, m % CORES)

    def ring(self, along_w):
        side, c = self.side, self.c
        p = self.w if along_w else self.t
        back, fwd, far = (p + side - 1) % side, (p + 1) % side, (p + 2) % side
        at = (lambda q: self.at(q, self.t, c)) if along_w else (lambda q: self.at(self.w, q, c))
        return at(back), at(fwd), back, p, fwd, far

    def owner(self, k):
        return self.at(self.w, (self.t + (0, self.side - 1, 1, 2)[k]) % self.side, self.c)


def decoder_kernel(side, layers, x_ref, ln1g, ln1b, ln2g, ln2b, bo_ref, bu_ref, bd_ref, wq_in, wo_in, wu_in, wd_in,
                   out_ref, gq, go, gu, gd,
                   wq, wo, wu, wd, h1, h2, qkv, qsend, oall, osend, ubuf, zsend, zrecv, resid, bup,
                   g_recv, g_send, h_send, h_recv, q_sem, o_sem, z_send, z_recv, b_sem, l_sem, c_sem):
    me = lax.axis_index("tp")
    y, x, c = me // (side * CORES), (me // CORES) % side, me % CORES
    col = side * CORES
    tp = side * col
    near = side - 1
    share, width = x_ref.shape
    dim = oall.shape[2]
    hidden = wu.shape[2]
    tile = 256
    partner = index_of(side, y, x, 1 - c)
    at = [Layer(side, layer, y, x, c) for layer in range(layers)]

    def number(pos, other):
        return pos * CORES + (c if other == 0 else 1 - c)

    def weights(layer, n, name, src, buf, dst):
        rows = buf.shape[2] // 2
        return Gather(
            f"L{layer}_{name}", at[layer].ring(True), src.at[layer],
            lambda pos, other: buf.at[layer, number(pos, other)],
            lambda pos, k: buf.at[layer, number(pos, 0), pl.ds(k * rows, rows)],
            g_recv.at[layer, n], g_send.at[layer, n], partner, dst, l_sem.at[layer, n], number)

    def down_half(layer, h):
        rows, cols = hidden // 2, width // 2
        n = (2, 5)[h]
        return Gather(
            f"L{layer}_d{h}", at[layer].ring(True), wd_in.at[layer, :, pl.ds(h * cols, cols)],
            lambda pos, other: gd.at[layer, h, number(pos, other)],
            lambda pos, k: gd.at[layer, h, number(pos, 0), pl.ds(k * rows, rows)],
            g_recv.at[layer, n], g_send.at[layer, n], partner, wd.at[h], l_sem.at[layer, n], number)

    def out_w(layer):
        here = number(at[layer].t, 0)
        half = dim // 2
        return Gather(
            f"L{layer}_ow", at[layer].ring(True), wo_in.at[layer],
            lambda pos, other: go.at[layer, here, pl.ds(pl.multiple_of(pos * dim, dim), dim)],
            lambda pos, k: go.at[layer, here, pl.ds(pl.multiple_of(pos * dim + k * half, half), half)],
            g_recv.at[layer, 3], g_send.at[layer, 3], None)

    def out_t(layer):
        rows = go.shape[2] // 2
        return Gather(
            f"L{layer}_ot", at[layer].ring(False), go.at[layer, number(at[layer].t, 0)],
            lambda pos, other: go.at[layer, number(pos, other)],
            lambda pos, k: go.at[layer, number(pos, 0), pl.ds(k * rows, rows)],
            g_recv.at[layer, 4], g_send.at[layer, 4], partner, wo, l_sem.at[layer, 4], number)

    q_job = [weights(layer, 0, "q", wq_in, gq, wq) for layer in range(layers)]
    u_job = [weights(layer, 1, "u", wu_in, gu, wu) for layer in range(layers)]
    d_job = [[down_half(layer, h) for h in range(2)] for layer in range(layers)]
    ow_job = [out_w(layer) for layer in range(layers)]
    ot_job = [out_t(layer) for layer in range(layers)]

    def own_out(layer):
        return pltpu.make_async_copy(wo_in.at[layer], ow_job[layer].slot(at[layer].w, 0), c_sem.at[layer])

    def all_bias(layer):
        moved = bup.at[layer, pl.ds(0, col - 1)]
        return remote(moved, moved, b_sem.at[layer, 0], b_sem.at[layer, 1], me)

    with scope("enter"):
        enter([(me + d) % tp for d in range(1, tp)])
    ow_job[0].start()
    q_job[0].start()
    for layer in range(layers):
        own_out(layer).start()
        mine = at[layer].mine
        for d in range(1, col):
            row = bu_ref.at[pl.ds(layer, 1)]
            remote(row, bup.at[layer, mine], b_sem.at[layer, 0], b_sem.at[layer, 1], at[layer].in_w((mine + d) % col)).start()
        bup[layer, mine] = bu_ref[layer : layer + 1, :]
    q_job[0].own()
    resid[...] = x_ref[...].astype(F32)

    class Spread:
        def __init__(self, layer, which, buf):
            self.buf, self.name = buf.at[layer], f"L{layer}_h{which}"
            self.send, self.recv = h_send.at[layer, which], h_recv.at[layer, which]
            self.prev, self.next = at[layer].ring(False)[:2]
            self.half = share // 2

        def full(self, k):
            return remote(self.buf.at[0], self.buf.at[k], self.send.at[k - 1], self.recv.at[k - 1], self.next if k == 1 else self.prev)

        def part(self, k):
            rows = pl.ds((k - 1) * self.half, self.half)
            return remote(self.buf.at[k, rows], self.buf.at[3, rows], self.send.at[k + 1], self.recv.at[k + 1], self.next if k == 1 else self.prev)

        def start(self):
            self.full(1).start()
            self.full(2).start()

        def relay(self, k):
            with scope(f"{self.name}_recv{k}"):
                self.full(k).wait_recv()
                self.part(k).start()

        def far(self):
            with scope(f"{self.name}_far"):
                self.part(1).wait_recv()
                self.part(2).wait_recv()

        def drain(self):
            for k in (1, 2):
                self.full(k).wait_send()
                self.part(k).wait_send()

    for layer in range(layers):
        first, final = layer == 0, layer == layers - 1
        row = slice(layer, layer + 1)
        lay = at[layer]
        tag = f"L{layer}_"
        h1[layer, 0] = norm(resid[...], ln1g[row, :], ln1b[row, :])
        spread1 = Spread(layer, 0, h1)
        spread1.start()

        def q_copy(k, m):
            return remote(qsend.at[k, m], qkv.at[layer, lay.owner(k)], q_sem.at[layer, 0], q_sem.at[layer, 1], lay.in_w(m))

        def put(k, m, part):
            @pl.when(m != lay.mine)
            def _():
                qsend[k, m] = part
                q_copy(k, m).start()

            @pl.when(m == lay.mine)
            def _():
                qkv[layer, lay.owner(k)] = part

        def q_parts(k0, count, start, slots):
            def step(n, _):
                m = (start + n) % col
                part = lax.dot_general(wq[m], h1[layer, k0 : k0 + count].reshape(count * share, width), NT, preferred_element_type=F32).astype(BF16)
                for k in range(count):
                    put(k0 + k, m, part[:, k * share : (k + 1) * share])
                return 0

            with scope(f"{tag}qkv{k0}"):
                lax.fori_loop(0, slots, step, 0)

        job = q_job[layer]
        if first:
            slots = [pos * CORES for pos in job.order()]
            job.other(0)
            job.ready(0)
            q_parts(0, 1, slots[0], CORES)
            spread1.relay(1)
            spread1.relay(2)
            if not final:
                q_job[layer + 1].start()
                ow_job[layer + 1].start()
            q_parts(1, 1, slots[0], CORES)
            q_parts(2, 1, slots[0], CORES)
            ow_job[layer].relay()
            job.relay()
            spread1.far()
            q_parts(3, 1, slots[0], CORES)
            job.other(1)
            job.other(2)
            job.ready(1, 2)
            for n in (1, 2):
                q_parts(0, 2, slots[n], CORES)
                q_parts(2, 2, slots[n], CORES)
            ow_job[layer].last()
            own_out(layer).wait()
            ot_job[layer].start()
            job.last()
            job.other(3)
            job.ready(3)
            q_parts(0, 2, slots[3], CORES)
            q_parts(2, 2, slots[3], CORES)
            u_job[layer].start()
        else:
            q_parts(0, 1, lay.mine + 1, col)
            spread1.relay(1)
            spread1.relay(2)
            ot_job[layer].relay()
            q_parts(1, 2, lay.mine + 1, col)
            spread1.far()
            q_parts(3, 1, lay.mine + 1, col)
        moved = qkv.at[layer, pl.ds(0, side * (col - 1))]
        all_qkv = remote(moved, moved, q_sem.at[layer, 0], q_sem.at[layer, 1], me)
        with scope(tag + "qkv_recv"):
            all_qkv.wait_recv()
        if not first:
            u_job[layer].own()
            u_job[layer].relay()
            for d in d_job[layer]:
                d.start()
        def hook_middle():
            if first:
                ot_job[layer].relay()
                if not final:
                    ow_job[layer + 1].relay()
                    q_job[layer + 1].relay()

        def hook_late():
            if first:
                u_job[layer].relay()
            else:
                u_job[layer].last()
                for i in range(3):
                    u_job[layer].other(i)

        hooks = {5: hook_middle, 7: hook_late}
        with scope(tag + "attend"):
            attend(layer, me, (lay.t * CORES + c) * side + lay.w, qkv, oall, osend, o_sem, hooks)
        moved = oall.at[layer, pl.ds(0, tp - 1)]
        all_o = remote(moved, moved, o_sem.at[layer, 0], o_sem.at[layer, 1], me)
        ot, u = ot_job[layer], u_job[layer]
        ot.own()
        for i in range(3):
            ot.other(i)
        ot.last()
        ot.other(3)
        ot.ready(0, 1, 2, 3)
        if first:
            for d in d_job[layer]:
                d.start()
        with scope(tag + "o_recv"):
            all_o.wait_recv()
        if not first:
            for d in d_job[layer]:
                d.own()
                d.relay()
        o_t = oall[layer].reshape(tp * dim, share)

        def out_step(n, _):
            cs = pl.ds(pl.multiple_of(n * tile, tile), tile)
            w = wo[:, :, cs].reshape(tp * dim, tile)
            resid[:, cs] = resid[:, cs] + (lax.dot_general(o_t, w, TN, preferred_element_type=F32) + bo_ref[row, cs])
            return 0

        with scope(tag + "outproj"):
            lax.fori_loop(0, width // tile, out_step, 0)
        h2[layer, 0] = norm(resid[...], ln2g[row, :], ln2b[row, :])
        spread2 = Spread(layer, 1, h2)
        spread2.start()
        all_bias(layer).wait()

        def up(k0, count):
            def up_step(g, _):
                h = h2[layer, k0 : k0 + count].reshape(count * share, width)
                pre = lax.dot_general(h, wu[g], NN, preferred_element_type=F32) + bup[layer, g]
                act = jax.nn.gelu(pre, approximate=True).astype(BF16)
                ubuf[k0 * share : (k0 + count) * share, pl.ds(pl.multiple_of(g * hidden, 128), hidden)] = act
                return 0

            with scope(f"{tag}up{k0}"):
                lax.fori_loop(0, col, up_step, 0)

        pieces = zsend.shape[0]
        piece = width // pieces

        def z_copy(p, k):
            return remote(zsend.at[p, k - 1], zrecv.at[layer, p, k - 1], z_send.at[layer, k - 1, p], z_recv.at[layer, k - 1, p], lay.owner(k))

        def down(k0, count, h):
            per_half = pieces // 2

            def piece_step(i, _):
                p = h * per_half + i
                for n in range(piece // tile):
                    cs = pl.ds(pl.multiple_of(p * piece + n * tile, tile), tile)
                    w = wd[h, :, :, pl.ds(pl.multiple_of(i * piece + n * tile, tile), tile)].reshape(col * hidden, tile)
                    z = lax.dot_general(ubuf[k0 * share : (k0 + count) * share, :], w, NN, preferred_element_type=F32)
                    for k in range(k0, k0 + count):
                        zk = z[(k - k0) * share : (k - k0 + 1) * share]
                        if k:
                            zsend[p, k - 1, :, n * tile : (n + 1) * tile] = zk.astype(BF16)
                        else:
                            resid[:, cs] = resid[:, cs] + (zk + bd_ref[row, cs])
                for k in range(max(k0, 1), k0 + count):
                    z_copy(p, k).start()
                return 0

            with scope(f"{tag}down{k0}_{h}"):
                lax.fori_loop(0, per_half, piece_step, 0)

        da, db = d_job[layer]
        if first:
            if not final:
                ow_job[layer + 1].last()
                own_out(layer + 1).wait()
                q_job[layer + 1].last()
            spread2.relay(1)
            spread2.relay(2)
            u.own()
            da.own()
            da.relay()
            if not final:
                for i in range(4):
                    q_job[layer + 1].other(i)
            for i in range(3):
                u.other(i)
            u.last()
            u.other(3)
            u.ready(0, 1, 2, 3)
            spread2.far()
            up(0, side)
            db.own()
            db.relay()
            for i in range(3):
                da.other(i)
            da.last()
            da.other(3)
            da.ready(0, 1, 2, 3)
            down(0, side, 0)
            if not final:
                ot_job[layer + 1].start()
            for i in range(3):
                db.other(i)
            db.last()
            db.other(3)
            db.ready(0, 1, 2, 3)
            down(0, side, 1)
        else:
            u.other(3)
            u.ready(0, 1, 2, 3)
            up(0, 1)
            da.last()
            db.last()
            for d in (da, db):
                for i in range(4):
                    d.other(i)
            spread2.relay(1)
            spread2.relay(2)
            up(1, 2)
            da.ready(0, 1, 2, 3)
            db.ready(0, 1, 2, 3)
            down(1, 2, 0)
            down(1, 2, 1)
            spread2.far()
            up(3, 1)
            down(3, 1, 0)
            down(3, 1, 1)
            down(0, 1, 0)
            down(0, 1, 1)
        if not final:
            q_job[layer + 1].own()
            q_job[layer + 1].ready(0, 1, 2, 3)
        with scope(tag + "z_recv"):
            for p in range(pieces):
                cs = slice(p * piece, (p + 1) * piece)
                total = resid[:, cs]
                for k in (1, 2, 3):
                    z_copy(p, k).wait_recv()
                    total = total + zrecv[layer, p, k - 1].astype(F32)
                if final:
                    out_ref[:, cs] = total
                else:
                    resid[:, cs] = total
        if not final:
            u_job[layer + 1].start()
        with scope(tag + "sent"):
            all_qkv.wait_send()
            all_o.wait_send()
            spread1.drain()
            spread2.drain()
            for p in range(pieces):
                for k in (1, 2, 3):
                    z_copy(p, k).wait_send()
    with scope("drain"):
        for layer in range(layers):
            q_job[layer].drain(gq.at[layer, pl.ds(0, 7)])
            u_job[layer].drain(gu.at[layer, pl.ds(0, 7)])
            for h in range(2):
                d_job[layer][h].drain(gd.at[layer, h, pl.ds(0, 7)])
            ot_job[layer].drain(go.at[layer, pl.ds(0, 7)])
            ow_job[layer].drain(go.at[layer, 0, pl.ds(0, 3 * dim)])


def attend(layer, me, slot, qkv, oall, osend, o_sem, hooks):
    _, tp, three_dim, share = qkv.shape
    dim = three_dim // 3
    per = 4
    block = per * share
    c2 = math.log2(math.e) / math.sqrt(dim)
    steps = tp // per

    def part(i, count, which):
        return jnp.concatenate([qkv[layer, i * per + n, which * dim : (which + 1) * dim, :] for n in range(count * per)], axis=1)

    def q_step(i, _):
        for when, hook in hooks.items():
            pl.when(i == when)(hook)
        q = part(i, 1, 0).T

        def update(j, count, carry, masked):
            m, l, acc = carry
            s = lax.dot_general(q, part(j, count, 1), NN, preferred_element_type=F32)
            if masked:
                rows = lax.broadcasted_iota(jnp.int32, (block, count * block), 0)
                cols = lax.broadcasted_iota(jnp.int32, (block, count * block), 1)
                s = jnp.where(rows + (count - 1) * block >= cols, s, -1e30)
            m_new = jnp.maximum(m, jnp.max(s, axis=-1, keepdims=True))
            p = jnp.exp2(s * c2 - m_new * c2)
            alpha = jnp.exp2((m - m_new) * c2)
            acc = acc * alpha + lax.dot_general(p.astype(BF16), part(j, count, 2), NT, preferred_element_type=F32)
            return m_new, l * alpha + jnp.sum(p, axis=-1, keepdims=True), acc

        init = (jnp.full((block, 1), -1e30, F32), jnp.zeros((block, 1), F32), jnp.zeros((block, dim), F32))
        carry = lax.fori_loop(0, i // 2, lambda j, carry: update(2 * j, 2, carry, False), init)
        _, l, acc = lax.cond(i % 2 == 1, lambda carry: update(i - 1, 2, carry, True), lambda carry: update(i, 1, carry, True), carry)
        o_t = (acc / l).T.astype(BF16)
        for n in range(per):
            d = (i * per + n - me + tp) % tp
            piece = o_t[:, n * share : (n + 1) * share]

            @pl.when(d != 0)
            def _():
                osend[d] = piece
                remote(osend.at[d], oall.at[layer, slot], o_sem.at[layer, 0], o_sem.at[layer, 1], i * per + n).start()

            @pl.when(d == 0)
            def _():
                oall[layer, slot] = piece

        return 0

    lax.fori_loop(0, steps, q_step, 0)


def solution(mesh):
    tp = mesh.shape["tp"]
    side = math.isqrt(tp // CORES)
    col = side * CORES
    near = side - 1
    pieces = 4

    def local_forward(x_local, ln1_gain, ln1_bias, ln2_gain, ln2_bias, w_qkv, w_out, b_out, w_up, b_up, w_down, b_down):
        _, share, width = x_local.shape
        layers, _, three, _, dim = w_qkv.shape
        hidden = w_up.shape[2]
        piece = width // pieces
        wq_t = jnp.transpose(w_qkv, (0, 2, 3, 4, 1)).reshape(layers, three * dim, width)
        hbm = lambda *shape: jax.ShapeDtypeStruct(shape, BF16)
        vmem = lambda *shape: pltpu.VMEM(shape, BF16)
        y = pl.pallas_call(
            functools.partial(decoder_kernel, side, layers),
            out_shape=(
                jax.ShapeDtypeStruct((share, width), F32), hbm(layers, col, three * dim, width), hbm(layers, col, side * dim, width),
                hbm(layers, col, width, hidden), hbm(layers, 2, col, hidden, width // 2),
            ),
            in_specs=[VMEM] * 8 + [HBM] * 4,
            out_specs=(VMEM, HBM, HBM, HBM, HBM),
            scratch_shapes=[
                vmem(col, three * dim, width), vmem(col, side * dim, width), vmem(col, width, hidden), vmem(2, col, hidden, width // 2),
                vmem(layers, side, share, width), vmem(layers, side, share, width),
                vmem(layers, tp, three * dim, share), vmem(side, col, three * dim, share),
                vmem(layers, tp, dim, share), vmem(tp, dim, share),
                vmem(side * share, col * hidden),
                vmem(pieces, near, share, piece), vmem(layers, pieces, near, share, piece),
                pltpu.VMEM((share, width), F32), pltpu.VMEM((layers, col, 1, hidden), F32),
                DMA((layers, 6, 8)), DMA((layers, 6)), DMA((layers, 2, 4)), DMA((layers, 2, 4)),
                DMA((layers, 2)), DMA((layers, 2)), DMA((layers, near, pieces)), DMA((layers, near, pieces)),
                DMA((layers, 2)), DMA((layers, 6, 8)), DMA((layers,)),
            ],
            compiler_params=pltpu.CompilerParams(collective_id=0, has_side_effects=True, vmem_limit_bytes=63 * 1024 * 1024),
            name="decoder",
        )(x_local[0], ln1_gain, ln1_bias, ln2_gain, ln2_bias, b_out, b_up, b_down, wq_t, w_out.reshape(layers, dim, width), w_up, w_down)[0]
        return y.astype(BF16)[None]

    rows_spec = P("dp", "tp", None)
    in_specs = (rows_spec, P(), P(), P(), P(), P(None, None, None, "tp", None), P(None, "tp", None, None), P(), P(None, None, "tp"), P(None, "tp"), P(None, "tp", None), P())
    return jax.shard_map(local_forward, mesh=mesh, in_specs=in_specs, out_specs=rows_spec, check_vma=False)
```

```python
import functools
import math
import jax
import jax.numpy as jnp
from jax import lax
from jax.experimental import pallas as pl
from jax.experimental.pallas import tpu as pltpu
from jax.sharding import PartitionSpec as P

F32 = jnp.float32
BF16 = jnp.bfloat16
CORES = 2
NN = (((1,), (0,)), ((), ()))
NT = (((1,), (1,)), ((), ()))
TN = (((0,), (0,)), ((), ()))
MESH = pl.DeviceIdType.MESH
VMEM = pl.BlockSpec(memory_space=pltpu.VMEM)
HBM = pl.BlockSpec(memory_space=pl.ANY)
DMA = pltpu.SemaphoreType.DMA


def index_of(side, y, x, c):
    return (y * side + x) * CORES + c


def dev(index):
    return {"tp": index}


def remote(src, dst, send_sem, recv_sem, index):
    return pltpu.make_async_remote_copy(src_ref=src, dst_ref=dst, send_sem=send_sem, recv_sem=recv_sem, device_id=dev(index), device_id_type=MESH)


def enter(indices):
    barrier = pltpu.get_barrier_semaphore()
    for index in indices:
        pl.semaphore_signal(barrier, inc=1, device_id=dev(index), device_id_type=MESH)
    pl.semaphore_wait(barrier, len(indices))


def norm(resid, gain, shift):
    row_mean = jnp.mean(resid, axis=-1, keepdims=True)
    centered = resid - row_mean
    variance = jnp.mean(centered * centered, axis=-1, keepdims=True)
    return (centered * lax.rsqrt(variance + 1e-5) * gain + shift).astype(BF16)


scope = jax.named_scope


class Gather:
    def __init__(self, name, ring, src, slot, half, recv, send, partner, dst=None, load_sem=None, number=None):
        self.name = name
        self.prev, self.next, self.back, self.here, self.fwd, self.far = ring
        self.src, self.slot, self.half, self.recv, self.send, self.partner = src, slot, half, recv, send, partner
        self.dst, self.load_sem, self.number = dst, load_sem, number

    def order(self):
        return (self.here, self.back, self.fwd, self.far)

    def start(self):
        dst = self.slot(self.here, 0)
        remote(self.src, dst, self.send, self.recv.at[0], self.next).start()
        remote(self.src, dst, self.send, self.recv.at[1], self.prev).start()
        if self.partner is not None:
            remote(self.src, dst, self.send, self.recv.at[4], self.partner).start()

    def landed(self, ref, n):
        remote(ref, ref, self.send, self.recv.at[n], self.next).wait_recv()

    def load(self, i, other):
        pos = self.order()[i]
        src = self.src if i == 0 and other == 0 else self.slot(pos, other)
        return pltpu.make_async_copy(src, self.dst.at[self.number(pos, other)], self.load_sem.at[2 * i + other])

    def share(self, pos, n):
        ref = self.slot(pos, 0)
        remote(ref, ref, self.send, self.recv.at[n], self.partner).start()

    def relay(self):
        with scope(self.name + "_relay"):
            for n, pos, to in ((0, self.back, self.next), (1, self.fwd, self.prev)):
                self.landed(self.slot(pos, 0), n)
                ref = self.half(pos, n)
                remote(ref, ref, self.send, self.recv.at[2 + n], to).start()
                if self.partner is not None:
                    self.share(pos, 5 + n)
                    self.load(1 + n, 0).start()

    def own(self):
        self.load(0, 0).start()

    def other(self, i):
        with scope(f"{self.name}_other{i}"):
            self.landed(self.slot(self.order()[i], 1), 4 + i)
            self.load(i, 1).start()

    def last(self):
        with scope(self.name + "_last"):
            self.landed(self.half(self.far, 0), 2)
            self.landed(self.half(self.far, 1), 3)
            if self.partner is not None:
                self.share(self.far, 7)
                self.load(3, 0).start()

    def ready(self, *which):
        with scope(self.name + "_ready"):
            for i in which:
                self.load(i, 0).wait()
                self.load(i, 1).wait()

    def drain(self, ref):
        remote(ref, ref, self.send, self.recv.at[0], self.next).wait_send()


class Layer:
    def __init__(self, side, layer, y, x, c):
        self.side, self.swap, self.c = side, layer % 2, c
        self.w, self.t = (x, y) if self.swap else (y, x)
        self.mine = self.w * CORES + c

    def at(self, w, t, c):
        return index_of(self.side, t, w, c) if self.swap else index_of(self.side, w, t, c)

    def in_w(self, m):
        return self.at(m // CORES, self.t, m % CORES)

    def ring(self, along_w):
        side, c = self.side, self.c
        p = self.w if along_w else self.t
        back, fwd, far = (p + side - 1) % side, (p + 1) % side, (p + 2) % side
        at = (lambda q: self.at(q, self.t, c)) if along_w else (lambda q: self.at(self.w, q, c))
        return at(back), at(fwd), back, p, fwd, far

    def owner(self, k):
        return self.at(self.w, (self.t + (0, self.side - 1, 1, 2)[k]) % self.side, self.c)


def decoder_kernel(side, layers, x_ref, ln1g, ln1b, ln2g, ln2b, bo_ref, bu_ref, bd_ref, wq_in, wo_in, wu_in, wd_in,
                   out_ref, gq, go, gu, gd,
                   wq, wo, wu, wd, h1, h2, qkv, qsend, oall, osend, ubuf, zsend, zrecv, resid, bup,
                   g_recv, g_send, h_send, h_recv, q_sem, o_sem, z_send, z_recv, b_sem, l_sem, c_sem):
    me = lax.axis_index("tp")
    y, x, c = me // (side * CORES), (me // CORES) % side, me % CORES
    col = side * CORES
    tp = side * col
    near = side - 1
    share, width = x_ref.shape
    dim = oall.shape[2]
    hidden = wu.shape[2]
    tile = 256
    partner = index_of(side, y, x, 1 - c)
    at = [Layer(side, layer, y, x, c) for layer in range(layers)]

    def number(pos, other):
        return pos * CORES + (c if other == 0 else 1 - c)

    def weights(layer, n, name, src, buf, dst):
        rows = buf.shape[2] // 2
        return Gather(
            f"L{layer}_{name}", at[layer].ring(True), src.at[layer],
            lambda pos, other: buf.at[layer, number(pos, other)],
            lambda pos, k: buf.at[layer, number(pos, 0), pl.ds(k * rows, rows)],
            g_recv.at[layer, n], g_send.at[layer, n], partner, dst, l_sem.at[layer, n], number)

    def down_half(layer, h):
        rows, cols = hidden // 2, width // 2
        n = (2, 5)[h]
        return Gather(
            f"L{layer}_d{h}", at[layer].ring(True), wd_in.at[layer, :, pl.ds(h * cols, cols)],
            lambda pos, other: gd.at[layer, h, number(pos, other)],
            lambda pos, k: gd.at[layer, h, number(pos, 0), pl.ds(k * rows, rows)],
            g_recv.at[layer, n], g_send.at[layer, n], partner, wd.at[h], l_sem.at[layer, n], number)

    def out_w(layer):
        here = number(at[layer].t, 0)
        half = dim // 2
        return Gather(
            f"L{layer}_ow", at[layer].ring(True), wo_in.at[layer],
            lambda pos, other: go.at[layer, here, pl.ds(pl.multiple_of(pos * dim, dim), dim)],
            lambda pos, k: go.at[layer, here, pl.ds(pl.multiple_of(pos * dim + k * half, half), half)],
            g_recv.at[layer, 3], g_send.at[layer, 3], None)

    def out_t(layer):
        rows = go.shape[2] // 2
        return Gather(
            f"L{layer}_ot", at[layer].ring(False), go.at[layer, number(at[layer].t, 0)],
            lambda pos, other: go.at[layer, number(pos, other)],
            lambda pos, k: go.at[layer, number(pos, 0), pl.ds(k * rows, rows)],
            g_recv.at[layer, 4], g_send.at[layer, 4], partner, wo, l_sem.at[layer, 4], number)

    q_job = [weights(layer, 0, "q", wq_in, gq, wq) for layer in range(layers)]
    u_job = [weights(layer, 1, "u", wu_in, gu, wu) for layer in range(layers)]
    d_job = [[down_half(layer, h) for h in range(2)] for layer in range(layers)]
    ow_job = [out_w(layer) for layer in range(layers)]
    ot_job = [out_t(layer) for layer in range(layers)]

    def own_out(layer):
        return pltpu.make_async_copy(wo_in.at[layer], ow_job[layer].slot(at[layer].w, 0), c_sem.at[layer])

    def all_bias(layer):
        moved = bup.at[layer, pl.ds(0, col - 1)]
        return remote(moved, moved, b_sem.at[layer, 0], b_sem.at[layer, 1], me)

    with scope("enter"):
        enter([(me + d) % tp for d in range(1, tp)])
    ow_job[0].start()
    q_job[0].start()
    for layer in range(layers):
        own_out(layer).start()
        mine = at[layer].mine
        for d in range(1, col):
            row = bu_ref.at[pl.ds(layer, 1)]
            remote(row, bup.at[layer, mine], b_sem.at[layer, 0], b_sem.at[layer, 1], at[layer].in_w((mine + d) % col)).start()
        bup[layer, mine] = bu_ref[layer : layer + 1, :]
    q_job[0].own()
    resid[...] = x_ref[...].astype(F32)

    class Spread:
        def __init__(self, layer, which, buf):
            self.buf, self.name = buf.at[layer], f"L{layer}_h{which}"
            self.send, self.recv = h_send.at[layer, which], h_recv.at[layer, which]
            self.prev, self.next = at[layer].ring(False)[:2]
            self.half = share // 2

        def full(self, k):
            return remote(self.buf.at[0], self.buf.at[k], self.send.at[k - 1], self.recv.at[k - 1], self.next if k == 1 else self.prev)

        def part(self, k):
            rows = pl.ds((k - 1) * self.half, self.half)
            return remote(self.buf.at[k, rows], self.buf.at[3, rows], self.send.at[k + 1], self.recv.at[k + 1], self.next if k == 1 else self.prev)

        def start(self):
            self.full(1).start()
            self.full(2).start()

        def relay(self, k):
            with scope(f"{self.name}_recv{k}"):
                self.full(k).wait_recv()
                self.part(k).start()

        def far(self):
            with scope(f"{self.name}_far"):
                self.part(1).wait_recv()
                self.part(2).wait_recv()

        def drain(self):
            for k in (1, 2):
                self.full(k).wait_send()
                self.part(k).wait_send()

    for layer in range(layers):
        first, final = layer == 0, layer == layers - 1
        row = slice(layer, layer + 1)
        lay = at[layer]
        tag = f"L{layer}_"
        h1[layer, 0] = norm(resid[...], ln1g[row, :], ln1b[row, :])
        spread1 = Spread(layer, 0, h1)
        spread1.start()

        def q_copy(k, m):
            return remote(qsend.at[k, m], qkv.at[layer, lay.owner(k)], q_sem.at[layer, 0], q_sem.at[layer, 1], lay.in_w(m))

        def put(k, m, part):
            @pl.when(m != lay.mine)
            def _():
                qsend[k, m] = part
                q_copy(k, m).start()

            @pl.when(m == lay.mine)
            def _():
                qkv[layer, lay.owner(k)] = part

        def q_parts(k0, count, start, slots):
            def step(n, _):
                m = (start + n) % col
                part = lax.dot_general(wq[m], h1[layer, k0 : k0 + count].reshape(count * share, width), NT, preferred_element_type=F32).astype(BF16)
                for k in range(count):
                    put(k0 + k, m, part[:, k * share : (k + 1) * share])
                return 0

            with scope(f"{tag}qkv{k0}"):
                lax.fori_loop(0, slots, step, 0)

        job = q_job[layer]
        if first:
            slots = [pos * CORES for pos in job.order()]
            job.other(0)
            job.ready(0)
            q_parts(0, 1, slots[0], CORES)
            spread1.relay(1)
            spread1.relay(2)
            if not final:
                q_job[layer + 1].start()
                ow_job[layer + 1].start()
            q_parts(1, 1, slots[0], CORES)
            q_parts(2, 1, slots[0], CORES)
            ow_job[layer].relay()
            job.relay()
            spread1.far()
            q_parts(3, 1, slots[0], CORES)
            job.other(1)
            job.other(2)
            job.ready(1, 2)
            for n in (1, 2):
                q_parts(0, 2, slots[n], CORES)
                q_parts(2, 2, slots[n], CORES)
            ow_job[layer].last()
            own_out(layer).wait()
            ot_job[layer].start()
            job.last()
            job.other(3)
            job.ready(3)
            q_parts(0, 2, slots[3], CORES)
            q_parts(2, 2, slots[3], CORES)
            u_job[layer].start()
        else:
            q_parts(0, 1, lay.mine + 1, col)
            spread1.relay(1)
            spread1.relay(2)
            ot_job[layer].relay()
            q_parts(1, 2, lay.mine + 1, col)
            spread1.far()
            q_parts(3, 1, lay.mine + 1, col)
            u_job[layer].own()
            u_job[layer].last()
        moved = qkv.at[layer, pl.ds(0, side * (col - 1))]
        all_qkv = remote(moved, moved, q_sem.at[layer, 0], q_sem.at[layer, 1], me)
        with scope(tag + "qkv_recv"):
            all_qkv.wait_recv()
        if not first:
            for d in d_job[layer]:
                d.start()
        def hook_early():
            if not first:
                for i in range(4):
                    u_job[layer].other(i)

        def hook_middle():
            if first:
                ot_job[layer].relay()
                if not final:
                    ow_job[layer + 1].relay()
                    q_job[layer + 1].relay()

        def hook_late():
            if first:
                u_job[layer].relay()

        hooks = {3: hook_early, 5: hook_middle, 7: hook_late}
        with scope(tag + "attend"):
            attend(layer, me, (lay.t * CORES + c) * side + lay.w, qkv, oall, osend, o_sem, hooks)
        moved = oall.at[layer, pl.ds(0, tp - 1)]
        all_o = remote(moved, moved, o_sem.at[layer, 0], o_sem.at[layer, 1], me)
        ot, u = ot_job[layer], u_job[layer]
        ot.own()
        for i in range(3):
            ot.other(i)
        ot.last()
        ot.other(3)
        ot.ready(0, 1, 2, 3)
        if first:
            for d in d_job[layer]:
                d.start()
        with scope(tag + "o_recv"):
            all_o.wait_recv()
        if not first:
            for d in d_job[layer]:
                d.own()
                d.relay()
        o_t = oall[layer].reshape(tp * dim, share)

        def out_step(n, _):
            cs = pl.ds(pl.multiple_of(n * tile, tile), tile)
            w = wo[:, :, cs].reshape(tp * dim, tile)
            resid[:, cs] = resid[:, cs] + (lax.dot_general(o_t, w, TN, preferred_element_type=F32) + bo_ref[row, cs])
            return 0

        with scope(tag + "outproj"):
            lax.fori_loop(0, width // tile, out_step, 0)
        h2[layer, 0] = norm(resid[...], ln2g[row, :], ln2b[row, :])
        spread2 = Spread(layer, 1, h2)
        spread2.start()
        all_bias(layer).wait()

        def up(k0, count):
            def up_step(g, _):
                h = h2[layer, k0 : k0 + count].reshape(count * share, width)
                pre = lax.dot_general(h, wu[g], NN, preferred_element_type=F32) + bup[layer, g]
                act = jax.nn.gelu(pre, approximate=True).astype(BF16)
                ubuf[k0 * share : (k0 + count) * share, pl.ds(pl.multiple_of(g * hidden, 128), hidden)] = act
                return 0

            with scope(f"{tag}up{k0}"):
                lax.fori_loop(0, col, up_step, 0)

        pieces = zsend.shape[0]
        piece = width // pieces

        def z_copy(p, k):
            return remote(zsend.at[p, k - 1], zrecv.at[layer, p, k - 1], z_send.at[layer, k - 1, p], z_recv.at[layer, k - 1, p], lay.owner(k))

        def down(k0, count, h):
            per_half = pieces // 2

            def piece_step(i, _):
                p = h * per_half + i
                for n in range(piece // tile):
                    cs = pl.ds(pl.multiple_of(p * piece + n * tile, tile), tile)
                    w = wd[h, :, :, pl.ds(pl.multiple_of(i * piece + n * tile, tile), tile)].reshape(col * hidden, tile)
                    z = lax.dot_general(ubuf[k0 * share : (k0 + count) * share, :], w, NN, preferred_element_type=F32)
                    for k in range(k0, k0 + count):
                        zk = z[(k - k0) * share : (k - k0 + 1) * share]
                        if k:
                            zsend[p, k - 1, :, n * tile : (n + 1) * tile] = zk.astype(BF16)
                        else:
                            resid[:, cs] = resid[:, cs] + (zk + bd_ref[row, cs])
                for k in range(max(k0, 1), k0 + count):
                    z_copy(p, k).start()
                return 0

            with scope(f"{tag}down{k0}_{h}"):
                lax.fori_loop(0, per_half, piece_step, 0)

        da, db = d_job[layer]
        if first:
            if not final:
                ow_job[layer + 1].last()
                own_out(layer + 1).wait()
                q_job[layer + 1].last()
            spread2.relay(1)
            spread2.relay(2)
            u.own()
            da.own()
            da.relay()
            if not final:
                u_job[layer + 1].start()
                for i in range(4):
                    q_job[layer + 1].other(i)
            for i in range(3):
                u.other(i)
            u.last()
            u.other(3)
            u.ready(0, 1, 2, 3)
            spread2.far()
            up(0, side)
            db.own()
            db.relay()
            for i in range(3):
                da.other(i)
            da.last()
            da.other(3)
            da.ready(0, 1, 2, 3)
            down(0, side, 0)
            if not final:
                ot_job[layer + 1].start()
            for i in range(3):
                db.other(i)
            db.last()
            db.other(3)
            db.ready(0, 1, 2, 3)
            down(0, side, 1)
        else:
            u.ready(0, 1, 2, 3)
            up(0, 1)
            for d in (da, db):
                for i in range(3):
                    d.other(i)
            spread2.relay(1)
            spread2.relay(2)
            da.last()
            db.last()
            up(1, 2)
            da.other(3)
            db.other(3)
            da.ready(0, 1, 2, 3)
            db.ready(0, 1, 2, 3)
            down(1, 2, 0)
            down(1, 2, 1)
            spread2.far()
            up(3, 1)
            down(3, 1, 0)
            down(3, 1, 1)
            down(0, 1, 0)
            down(0, 1, 1)
        if not final:
            q_job[layer + 1].own()
            q_job[layer + 1].ready(0, 1, 2, 3)
        with scope(tag + "z_recv"):
            for p in range(pieces):
                cs = slice(p * piece, (p + 1) * piece)
                total = resid[:, cs]
                for k in (1, 2, 3):
                    z_copy(p, k).wait_recv()
                    total = total + zrecv[layer, p, k - 1].astype(F32)
                if final:
                    out_ref[:, cs] = total.astype(BF16)
                else:
                    resid[:, cs] = total
        if not final:
            u_job[layer + 1].relay()
        with scope(tag + "sent"):
            all_qkv.wait_send()
            all_o.wait_send()
            spread1.drain()
            spread2.drain()
            for p in range(pieces):
                for k in (1, 2, 3):
                    z_copy(p, k).wait_send()
    with scope("drain"):
        for layer in range(layers):
            q_job[layer].drain(gq.at[layer, pl.ds(0, 7)])
            u_job[layer].drain(gu.at[layer, pl.ds(0, 7)])
            for h in range(2):
                d_job[layer][h].drain(gd.at[layer, h, pl.ds(0, 7)])
            ot_job[layer].drain(go.at[layer, pl.ds(0, 7)])
            ow_job[layer].drain(go.at[layer, 0, pl.ds(0, 3 * dim)])


def attend(layer, me, slot, qkv, oall, osend, o_sem, hooks):
    _, tp, three_dim, share = qkv.shape
    dim = three_dim // 3
    per = 4
    block = per * share
    c2 = math.log2(math.e) / math.sqrt(dim)
    steps = tp // per

    def part(i, count, which):
        return jnp.concatenate([qkv[layer, i * per + n, which * dim : (which + 1) * dim, :] for n in range(count * per)], axis=1)

    def q_step(i, _):
        for when, hook in hooks.items():
            pl.when(i == when)(hook)
        q = part(i, 1, 0).T

        def update(j, count, carry, masked):
            m, l, acc = carry
            s = lax.dot_general(q, part(j, count, 1), NN, preferred_element_type=F32)
            if masked:
                rows = lax.broadcasted_iota(jnp.int32, (block, count * block), 0)
                cols = lax.broadcasted_iota(jnp.int32, (block, count * block), 1)
                s = jnp.where(rows + (count - 1) * block >= cols, s, -1e30)
            m_new = jnp.maximum(m, jnp.max(s, axis=-1, keepdims=True))
            p = jnp.exp2(s * c2 - m_new * c2)
            alpha = jnp.exp2((m - m_new) * c2)
            acc = acc * alpha + lax.dot_general(p.astype(BF16), part(j, count, 2), NT, preferred_element_type=F32)
            return m_new, l * alpha + jnp.sum(p, axis=-1, keepdims=True), acc

        init = (jnp.full((block, 1), -1e30, F32), jnp.zeros((block, 1), F32), jnp.zeros((block, dim), F32))
        carry = lax.fori_loop(0, i // 2, lambda j, carry: update(2 * j, 2, carry, False), init)
        _, l, acc = lax.cond(i % 2 == 1, lambda carry: update(i - 1, 2, carry, True), lambda carry: update(i, 1, carry, True), carry)
        o_t = (acc / l).T.astype(BF16)
        for n in range(per):
            d = (i * per + n - me + tp) % tp
            piece = o_t[:, n * share : (n + 1) * share]

            @pl.when(d != 0)
            def _():
                osend[d] = piece
                remote(osend.at[d], oall.at[layer, slot], o_sem.at[layer, 0], o_sem.at[layer, 1], i * per + n).start()

            @pl.when(d == 0)
            def _():
                oall[layer, slot] = piece

        return 0

    lax.fori_loop(0, steps, q_step, 0)


def solution(mesh):
    tp = mesh.shape["tp"]
    side = math.isqrt(tp // CORES)
    col = side * CORES
    near = side - 1
    pieces = 4

    def local_forward(x_local, ln1_gain, ln1_bias, ln2_gain, ln2_bias, w_qkv, w_out, b_out, w_up, b_up, w_down, b_down):
        _, share, width = x_local.shape
        layers, _, three, _, dim = w_qkv.shape
        hidden = w_up.shape[2]
        piece = width // pieces
        wq_t = jnp.transpose(w_qkv, (0, 2, 3, 4, 1)).reshape(layers, three * dim, width)
        hbm = lambda *shape: jax.ShapeDtypeStruct(shape, BF16)
        vmem = lambda *shape: pltpu.VMEM(shape, BF16)
        y = pl.pallas_call(
            functools.partial(decoder_kernel, side, layers),
            out_shape=(
                hbm(share, width), hbm(layers, col, three * dim, width), hbm(layers, col, side * dim, width),
                hbm(layers, col, width, hidden), hbm(layers, 2, col, hidden, width // 2),
            ),
            in_specs=[VMEM] * 8 + [HBM] * 4,
            out_specs=(VMEM, HBM, HBM, HBM, HBM),
            scratch_shapes=[
                vmem(col, three * dim, width), vmem(col, side * dim, width), vmem(col, width, hidden), vmem(2, col, hidden, width // 2),
                vmem(layers, side, share, width), vmem(layers, side, share, width),
                vmem(layers, tp, three * dim, share), vmem(side, col, three * dim, share),
                vmem(layers, tp, dim, share), vmem(tp, dim, share),
                vmem(side * share, col * hidden),
                vmem(pieces, near, share, piece), vmem(layers, pieces, near, share, piece),
                pltpu.VMEM((share, width), F32), pltpu.VMEM((layers, col, 1, hidden), F32),
                DMA((layers, 6, 8)), DMA((layers, 6)), DMA((layers, 2, 4)), DMA((layers, 2, 4)),
                DMA((layers, 2)), DMA((layers, 2)), DMA((layers, near, pieces)), DMA((layers, near, pieces)),
                DMA((layers, 2)), DMA((layers, 6, 8)), DMA((layers,)),
            ],
            compiler_params=pltpu.CompilerParams(collective_id=0, has_side_effects=True, vmem_limit_bytes=63 * 1024 * 1024),
            name="decoder",
        )(x_local[0], ln1_gain, ln1_bias, ln2_gain, ln2_bias, b_out, b_up, b_down, wq_t, w_out.reshape(layers, dim, width), w_up, w_down)[0]
        return y[None]

    rows_spec = P("dp", "tp", None)
    in_specs = (rows_spec, P(), P(), P(), P(), P(None, None, None, "tp", None), P(None, "tp", None, None), P(), P(None, None, "tp"), P(None, "tp"), P(None, "tp", None), P())
    return jax.shard_map(local_forward, mesh=mesh, in_specs=in_specs, out_specs=rows_spec, check_vma=False)
```
